256 devices in a mesh: grp: 8 (over x_lo, y), smp: 32 (over x_hi, z, core).
Axes of the slice: x: 4 (x_hi: 2, x_lo: 2; x = x_hi * 2 + x_lo), y: 4, z: 8, core: 2. Of those that a mesh axis runs over, the one named last changes fastest.
Arguments:
- spins_packed: int32 [32, 32768], P(None, 'smp'), may hold values from -2147483648 to 2147483646
- weight: bfloat16 [1024, 8192], P(None, 'grp'), may hold values from -0.1875 to 0.1875
- hidden_bias: float32 [8192], P('grp'), may hold values from -1.5 to 1.5
- force_w: float32 [1024, 8192], P('smp', 'grp'), may hold values from -6 to 6
- force_b: float32 [8192], P('grp'), may hold values from -6 to 6
Outputs:
- update_w: float32 [1024, 8192], P('smp', 'grp')
- update_b: float32 [8192], P('grp')
The draws below stay inside these ranges and needn't reach their ends.
All inputs are finite; a program needn't handle non-finite values.
Results may differ from the reference program's by a relative error of at most 0.0003.
Values sent between devices are 32-bit elements; how exact they have to be, the bound alone decides.
A program may use at most 64 MiB of HBM per device.

```python
import jax
import jax.numpy as jnp
from jax import lax

NV = 1024
NH = 8192
TOK_DEV = 1024
ITERS = 2
WORDS = 32
TOKENS = 32768


def with_ends(entries, stream_key, low, high):
    dims = entries.shape
    spot = [jax.random.randint(jax.random.fold_in(stream_key, axis), (), 0, dims[axis]) for axis in range(len(dims))]
    entries = entries.at[tuple(spot)].set(low)
    longest = dims.index(max(dims))
    spot[longest] = (spot[longest] + 1) % dims[longest]
    return entries.at[tuple(spot)].set(high)


def block_levels(stream_key, dims, split, smallest, top_value):
    level = 1.0
    for axis_at, shards_of in split:
        heights = jax.random.uniform(jax.random.fold_in(jax.random.fold_in(stream_key, 6), axis_at), (shards_of,), jnp.float32, smallest / len(split), top_value / len(split))
        level = level * jnp.repeat(jnp.exp(heights), dims[axis_at] // shards_of).reshape((-1,) + (1,) * (len(dims) - 1 - axis_at))
    return level


def bell_draw(rng, shape, width, reach, shards=(), kind=jnp.bfloat16):
    array = width * jax.random.normal(rng, shape, jnp.float32)
    if shards:
        array = array * block_levels(rng, shape, shards, -0.22, 0.18)
    return jnp.clip(array, -reach, reach).astype(kind)


def setup_inputs(seed: int = 0) -> dict:
    key_of = jax.random.split(jax.random.key(seed), 6)
    spins_packed = with_ends(jax.random.randint(key_of[0], (WORDS, TOKENS), -2147483648, 2147483647), jax.random.fold_in(key_of[0], 1), -2147483648, 2147483646).astype(jnp.int32)
    weight = bell_draw(key_of[1], (NV, NH), NV ** -0.5, 0.1875, ((1, 8),))
    hidden_bias = jnp.clip(jax.random.uniform(key_of[2], (NH,), jnp.float32, -1.5, 1.5) * block_levels(key_of[2], (NH,), ((0, 8),), -0.4, 0.0), -1.5, 1.5)
    force_w = bell_draw(key_of[3], (NV, NH), 1.0, 6.0, ((0, 32), (1, 8)), jnp.float32)
    force_b = bell_draw(key_of[4], (NH,), 1.0, 6.0, ((0, 8),), jnp.float32)
    return dict(spins_packed=spins_packed, weight=weight, hidden_bias=hidden_bias, force_w=force_w, force_b=force_b)


diag_shift = 0.01


def unpack(packed):
    shifts = jnp.arange(32, dtype=jnp.int32)
    bit_values = jnp.bitwise_and(jnp.right_shift(packed[:, None, :], shifts[None, :, None]), 1)
    signs = 2 * bit_values - 1
    return signs.reshape(packed.shape[0] * 32, packed.shape[1]).astype(jnp.bfloat16)


def reference(spins_packed, weight, hidden_bias, force_w, force_b):
    spins = unpack(spins_packed)
    tile_count = TOKENS // TOK_DEV
    tiles = spins.reshape(NV, tile_count, TOK_DEV).transpose(1, 0, 2)

    def activations(sample_tile):
        pre_activation = jnp.einsum("it,ih->th", sample_tile, weight, preferred_element_type=jnp.float32)
        return jnp.tanh(pre_activation + hidden_bias)

    def forward(direction_w, direction_b):
        def scan_step(running, sample_tile):
            hidden = activations(sample_tile)
            projected = jnp.einsum("it,ih->th", sample_tile, direction_w, precision=lax.Precision.HIGHEST, preferred_element_type=jnp.float32)
            return running, jnp.sum(hidden * (projected + direction_b), axis=1)

        _, sample_values = lax.scan(scan_step, jnp.zeros((), jnp.float32), tiles)
        sample_values = sample_values.reshape(TOKENS)
        return sample_values - jnp.sum(sample_values) / TOKENS

    def metric(centred, direction_w, direction_b):
        scaled = (centred / TOKENS).reshape(tile_count, TOK_DEV)

        def scan_step(running, inputs):
            sample_tile, weights_now = inputs
            hidden = activations(sample_tile)
            weighted = weights_now[:, None] * hidden
            grad_w = running[0] + jnp.einsum("it,th->ih", sample_tile, weighted, precision=lax.Precision.HIGHEST, preferred_element_type=jnp.float32)
            grad_b = running[1] + jnp.dot(weights_now, hidden, precision=lax.Precision.HIGHEST, preferred_element_type=jnp.float32)
            return (grad_w, grad_b), None

        zeros_pair = (jnp.zeros((NV, NH), jnp.float32), jnp.zeros((NH,), jnp.float32))
        (grad_w, grad_b), _ = lax.scan(scan_step, zeros_pair, (tiles, scaled))
        return grad_w + diag_shift * direction_w, grad_b + diag_shift * direction_b

    solution_w = jnp.zeros_like(force_w)
    solution_b = jnp.zeros_like(force_b)
    residual_w, residual_b = force_w, force_b
    direction_w, direction_b = force_w, force_b
    norm_now = jnp.sum(residual_w * residual_w) + jnp.sum(residual_b * residual_b)
    for iteration in range(ITERS):
        centred = forward(direction_w, direction_b)
        curvature = jnp.sum(centred * centred) / TOKENS + diag_shift * (jnp.sum(direction_w * direction_w) + jnp.sum(direction_b * direction_b))
        step_size = norm_now / curvature
        solution_w = solution_w + step_size * direction_w
        solution_b = solution_b + step_size * direction_b
        if iteration + 1 < ITERS:
            image_w, image_b = metric(centred, direction_w, direction_b)
            residual_w = residual_w - step_size * image_w
            residual_b = residual_b - step_size * image_b
            norm_next = jnp.sum(residual_w * residual_w) + jnp.sum(residual_b * residual_b)
            direction_w = residual_w + (norm_next / norm_now) * direction_w
            direction_b = residual_b + (norm_next / norm_now) * direction_b
            norm_now = norm_next
    return solution_w, solution_b
```

```python
import functools

import jax
import jax.numpy as jnp
from jax import lax
from jax.experimental import pallas as pl
from jax.experimental.pallas import tpu as pltpu
from jax.sharding import PartitionSpec as P

MESH = pl.DeviceIdType.MESH
F32, BF16 = jnp.float32, jnp.bfloat16
diag_shift = 0.01
SETS = 8
EXTRA = 256
PAD = 16
PART = 256


def total(x):
    return jnp.sum(jnp.sum(x, axis=0, keepdims=True), axis=1, keepdims=True)


def kernel(
    groups, ranks,
    packed_ref, weight_ref, bias_ref, force_ref, force_b_ref,
    out_ref, out_b_ref,
    packed, weight_t, bias_t, tile, spins, hidden, force_all, lhs, scaled,
    image, image_core, image_z, image_x, image_all, image_b, by_group, by_rank, by_set,
    spin_send, spin_recv, force_send, force_recv, image_send, image_recv, sum_send, sum_recv,
    group_send, group_recv, rank_send, rank_recv, set_send, set_recv, bias_send, bias_recv,
):
    grp, smp = lax.axis_index("grp"), lax.axis_index("smp")
    words, here = packed_ref.shape
    inputs, units = weight_ref.shape
    rows = force_ref.shape[0]
    pair = SETS * rows
    samples = ranks * here
    count = samples * SETS
    block = min(512, here)
    parts = units // PART
    depth = 2 * ranks

    core, z, half = lax.rem(smp, 2), lax.rem(smp // 2, depth), smp // (2 * depth)
    parity, rank = lax.rem(z, 2), z // 2
    member = (core * 2 + parity) * 2 + half

    def device(half_at, z_at, core_at):
        return {"smp": (half_at * depth + z_at) * 2 + core_at}

    sibling = device(half, z, 1 - core)
    z_partner = device(half, z + 1 - 2 * parity, core)
    x_partner = device(1 - half, z, core)

    def group_device(at):
        return {"grp": at}

    def rank_device(at):
        return device(half, 2 * at + parity, core)

    def set_device(at):
        return device(lax.rem(at, 2), 2 * rank + lax.rem(at // 2, 2), at // 4)

    def remote(source, target, send, recv, where):
        return pltpu.make_async_remote_copy(
            source, target, send, recv, device_id=where, device_id_type=MESH
        )

    with jax.named_scope("barrier"):
        barrier = pltpu.get_barrier_semaphore()
        for size, me, peer in ((groups, grp, group_device), (ranks, rank, rank_device), (SETS, member, set_device)):
            for step in range(1, size):
                pl.semaphore_signal(barrier, device_id=peer(lax.rem(me + step, size)), device_id_type=MESH)
        pl.semaphore_wait(barrier, groups + ranks + SETS - 3)

    after, before, across = lax.rem(rank + 1, ranks), lax.rem(rank + ranks - 1, ranks), lax.rem(rank + 2, ranks)
    split = words // 2

    def spin_copy(which):
        source, target, where = (
            (packed_ref, packed.at[rank], after),
            (packed_ref, packed.at[rank], before),
            (packed.at[before, pl.ds(0, split)], packed.at[before, pl.ds(0, split)], after),
            (packed.at[after, pl.ds(split, split)], packed.at[after, pl.ds(split, split)], before),
        )[which]
        return remote(source, target, spin_send.at[which], spin_recv.at[which], rank_device(where))

    def spin_arrival(which):
        target = (
            packed.at[before], packed.at[after],
            packed.at[across, pl.ds(0, split)], packed.at[across, pl.ds(split, split)],
        )[which]
        return remote(target, target, spin_send.at[which], spin_recv.at[which], sibling)

    def share(slots, send, recv):
        def own(at, source):
            for which, where in ((1, x_partner), (0, z_partner)):
                remote(source, slots.at[at, core, parity, half], send.at[at, which], recv.at[at, which], where).start()

        def arrived(at, which):
            target = (
                slots.at[at, core, 1 - parity, half],
                slots.at[at, core, parity, 1 - half],
                slots.at[at, core, 1 - parity, 1 - half],
                slots.at[at, 1 - core, parity],
                slots.at[at, 1 - core, 1 - parity],
            )[which]
            remote(target, target, send.at[at, which], recv.at[at, which], sibling).wait_recv()

        def after_x(at):
            arrived(at, 1)
            block_x = slots.at[at, core, parity, 1 - half]
            remote(block_x, block_x, send.at[at, 2], recv.at[at, 2], z_partner).start()
            ours = slots.at[at, core, parity]
            remote(ours, ours, send.at[at, 3], recv.at[at, 3], sibling).start()

        def after_z(at):
            arrived(at, 0)
            arrived(at, 2)
            theirs = slots.at[at, core, 1 - parity]
            remote(theirs, theirs, send.at[at, 4], recv.at[at, 4], sibling).start()

        def whole(at):
            arrived(at, 3)
            arrived(at, 4)

        def sent(at):
            for which in range(3):
                target = slots.at[at, core, parity, half]
                remote(target, target, send.at[at, which], recv.at[at, which], sibling).wait_send()
            for which in range(3, 5):
                target = slots.at[at, core, parity]
                remote(target, target, send.at[at, which], recv.at[at, which], sibling).wait_send()

        return own, after_x, after_z, whole, sent

    def each_part(step):
        def run(at, carry):
            step(at)
            return carry

        lax.fori_loop(0, parts, run, 0)

    def cols_of(at):
        return pl.ds(pl.multiple_of(at * PART, PART), PART)

    force_own, force_x, force_z, force_whole, force_sent = share(force_all, force_send, force_recv)
    for at in range(parts):
        force_own(at, force_ref.at[:, pl.ds(at * PART, PART)])
    spin_copy(0).start()
    spin_copy(1).start()

    packed[rank] = packed_ref[...]
    for at in range(parts):
        force_all[at, core, parity, half] = force_ref[:, at * PART : (at + 1) * PART]

    def turn(at, carry):
        cols = pl.ds(pl.multiple_of(at * 256, 256), 256)
        weight_t[cols, :] = weight_ref[:, cols].T
        bias_t[cols, :] = jnp.broadcast_to(bias_ref[:, cols], (128, 256)).T
        return carry

    with jax.named_scope("turn"):
        lax.fori_loop(0, units // 256, turn, 0)

    masks = jnp.left_shift(1, lax.broadcasted_iota(jnp.int32, (32, block), 0))

    def hidden_block(at_rank, at, carry):
        local = pl.ds(pl.multiple_of(at * block, block), block)
        cols = pl.ds(pl.multiple_of(at_rank * here + at * block, block), block)
        for word in range(words):
            bits = jnp.bitwise_and(jnp.broadcast_to(packed[at_rank, word : word + 1, local], (32, block)), masks)
            tile[word * 32 : word * 32 + 32, :] = jnp.where(bits != 0, 1.0, -1.0).astype(BF16)
        for to in range(SETS):
            word = (to % 2) * 2 * depth + 4 * rank + 2 * (to // 2 % 2) + to // 4
            spins[to * rows : (to + 1) * rows, cols] = tile[pl.ds(pl.multiple_of(word * rows, rows), rows), :]
        for unit in range(0, units, 512):
            these = pl.ds(unit, 512)
            pre = jnp.dot(weight_t[these, :], tile[...], preferred_element_type=F32)
            pre = pre + jnp.concatenate([bias_t[these, :]] * (block // 128), axis=1)
            hidden[these, cols] = jnp.tanh(pre).astype(BF16)
        return carry

    def hidden_of(at_rank):
        lax.fori_loop(0, here // block, functools.partial(hidden_block, at_rank), 0)

    with jax.named_scope("hidden0"):
        hidden_of(rank)
    with jax.named_scope("spinwait"):
        spin_arrival(0).wait_recv()
        spin_copy(2).start()
        spin_arrival(1).wait_recv()
        spin_copy(3).start()
    with jax.named_scope("hidden1"):
        hidden_of(before)
    with jax.named_scope("forcex"):
        each_part(force_x)
    with jax.named_scope("hidden2"):
        hidden_of(after)
    with jax.named_scope("forcez"):
        each_part(force_z)
        spin_arrival(2).wait_recv()
        spin_arrival(3).wait_recv()
    with jax.named_scope("hidden3"):
        hidden_of(across)
    with jax.named_scope("forcew"):
        each_part(force_whole)

    def fill_lhs(at, slots, row):
        cols = cols_of(at)
        for to in range(SETS):
            lhs[to * rows : (to + 1) * rows, cols] = slots[at, to // 4, to // 2 % 2, to % 2].astype(BF16)
        lhs[pair:, cols] = jnp.concatenate([row / ranks, jnp.zeros((PAD - 1, PART), F32)], axis=0).astype(BF16)

    each_part(lambda at: fill_lhs(at, force_all, force_b_ref[:, cols_of(at)]))

    def weighed(projected, cols):
        value = jnp.sum(projected[:pair] * spins[:, cols].astype(F32), axis=0, keepdims=True)
        return value + projected[pair : pair + 1]

    def first_values(at, carry):
        cols = pl.ds(pl.multiple_of(at * block, block), block)
        by_group[0, grp, :, cols] = weighed(jnp.dot(lhs[...], hidden[:, cols], preferred_element_type=F32), cols)
        return carry

    with jax.named_scope("values0"):
        lax.fori_loop(0, samples // block, first_values, 0)

    def gather(slot, size, me, peer, send, recv):
        copies = []
        for step in range(1, size):
            copies.append(remote(slot(me), slot(me), send.at[step], recv.at[me], peer(lax.rem(me + step, size))))
            copies[-1].start()

        def finish():
            for step in range(1, size):
                source = lax.rem(me + size - step, size)
                remote(slot(source), slot(source), send.at[step], recv.at[source], sibling).wait_recv()
            for copy in copies:
                copy.wait_send()

        return finish

    def wide(x, lanes):
        return jnp.broadcast_to(x, (1, lanes))

    def reduce_values(which, first, second):
        by_group[which, grp, :, samples:] = jnp.concatenate([wide(first, 128), wide(second, 128)], axis=1)
        with jax.named_scope("redg"):
            gather(lambda at: by_group.at[which, at], groups, grp, group_device, group_send.at[which], group_recv.at[which])()
            mine = by_group[which, 0]
            for source in range(1, groups):
                mine = mine + by_group[which, source]
        by_rank[which, rank] = mine
        with jax.named_scope("redr"):
            gather(lambda at: by_rank.at[which, at], ranks, rank, rank_device, rank_send.at[which], rank_recv.at[which])()
            whole = by_rank[which, 0]
            for source in range(1, ranks):
                whole = whole + by_rank[which, source]
        return whole[:, :samples], whole[:, samples : samples + 1], whole[:, samples + 128 : samples + 129]

    def gather_sets(which, values):
        fill = jnp.zeros((8 - len(values), 128), F32)
        by_set[which, member] = jnp.concatenate([wide(value, 128) for value in values] + [fill], axis=0)
        return gather(lambda at: by_set.at[which, at], SETS, member, set_device, set_send.at[which], set_recv.at[which])

    def set_sum(which, row):
        value = by_set[which, 0, row : row + 1, :]
        for source in range(1, SETS):
            value = value + by_set[which, source, row : row + 1, :]
        return value[:, :1]

    def moments(which, values, others):
        mean = total(values) / samples
        apart = values - mean
        with jax.named_scope("sets"):
            gather_sets(which, [mean, total(apart * apart)] + others)()
        middle = set_sum(which, 0) / SETS
        spread = jnp.zeros((1, 1), F32)
        for source in range(SETS):
            shift = by_set[which, source, 0:1, :1] - middle
            spread = spread + shift * shift
        return middle, (set_sum(which, 1) + samples * spread) / count

    force_dot = total(force_ref[...] * force_ref[...]) + total(force_b_ref[...] * force_b_ref[...]) / (ranks * SETS)
    values0, own_dot, _ = reduce_values(0, force_dot, jnp.zeros((1, 1), F32))
    mean0, variance0 = moments(0, values0, [own_dot])
    norm0 = set_sum(0, 2)
    step0 = norm0 / (variance0 + diag_shift * norm0)

    centred = values0 - mean0
    with jax.named_scope("scaled"):
        for at in range(0, samples, block):
            weights = centred[:, at : at + block]
            scaled[:pair, at : at + block] = (spins[:, at : at + block].astype(F32) * weights).astype(BF16)
            scaled[pair:, at : at + block] = jnp.concatenate(
                [weights, jnp.zeros((PAD - 1, block), F32)], axis=0
            ).astype(BF16)

    def core_copy(at):
        return remote(image.at[at, 1 - core], image_core.at[at], sum_send.at[at, 0], sum_recv.at[at, 0], sibling)

    def z_copy(at):
        return remote(image.at[at, core, 1 - parity], image_z.at[at], sum_send.at[at, 1], sum_recv.at[at, 1], z_partner)

    def x_copy(at):
        return remote(
            image.at[at, core, parity, 1 - half], image_x.at[at], sum_send.at[at, 2], sum_recv.at[at, 2], x_partner
        )

    def image_part(at):
        part = lax.dot_general(
            scaled[...], hidden[cols_of(at), :], (((1,), (1,)), ((), ())), preferred_element_type=F32
        )
        for to in range(SETS):
            image[at, to // 4, to // 2 % 2, to % 2] = part[to * rows : (to + 1) * rows]
        core_copy(at).start()
        image_b[member, :, cols_of(at)] = part[pair : pair + 1]

    image_own, gather_x, gather_z, gather_whole, gather_sent = share(image_all, image_send, image_recv)

    def sum_core(at):
        core_copy(at).wait_recv()
        image[at, core, 1 - parity] = image[at, core, 1 - parity] + image_core[at, 1 - parity]
        z_copy(at).start()
        image[at, core, parity] = image[at, core, parity] + image_core[at, parity]

    def sum_z(at):
        z_copy(at).wait_recv()
        image[at, core, parity, 1 - half] = image[at, core, parity, 1 - half] + image_z[at, 1 - half]
        x_copy(at).start()
        image[at, core, parity, half] = image[at, core, parity, half] + image_z[at, half]

    def sum_x(at):
        x_copy(at).wait_recv()
        image_all[at, core, parity, half] = image[at, core, parity, half] + image_x[at]
        image_own(at, image_all.at[at, core, parity, half])

    with jax.named_scope("image"):
        each_part(image_part)
    finish_bias = gather(lambda at: image_b.at[at], SETS, member, set_device, bias_send, bias_recv)
    with jax.named_scope("sumcore"):
        each_part(sum_core)
    with jax.named_scope("sumz"):
        each_part(sum_z)
    with jax.named_scope("sumx"):
        each_part(sum_x)

    keep = 1.0 - diag_shift * step0
    pull = step0 / count
    with jax.named_scope("bias"):
        finish_bias()
        whole_b = image_b[0]
        for source in range(1, SETS):
            whole_b = whole_b + image_b[source]
        residual_b = keep * force_b_ref[...] - pull * whole_b
        own_norm = total(residual_b * residual_b) / (ranks * SETS)
        own_cross = total(residual_b * force_b_ref[...]) / (ranks * SETS)
        for at in range(parts):
            force = force_ref[:, at * PART : (at + 1) * PART]
            residual = keep * force - pull * image_all[at, core, parity, half]
            own_norm = own_norm + total(residual * residual)
            own_cross = own_cross + total(residual * force)
        finish_norm = gather_sets(1, [own_norm, own_cross])
        image_b[0] = whole_b

    with jax.named_scope("gatherx"):
        each_part(gather_x)
    with jax.named_scope("gatherz"):
        each_part(gather_z)

    def second_values(at):
        gather_whole(at)
        fill_lhs(at, image_all, image_b[0, :, cols_of(at)])

        def run(to, carry):
            cols = pl.ds(pl.multiple_of(to * block, block), block)
            product = jnp.dot(lhs[:, cols_of(at)], hidden[cols_of(at), cols], preferred_element_type=F32)
            before_it = jnp.where(at == 0, 0.0, by_group[1, grp, :, cols])
            by_group[1, grp, :, cols] = before_it + weighed(product, cols)
            return carry

        lax.fori_loop(0, samples // block, run, 0)

    by_group[1, grp, :, :samples] = jnp.zeros((1, samples), F32)
    with jax.named_scope("values1"):
        each_part(second_values)
        finish_norm()
    image_values, norm1, cross = reduce_values(1, set_sum(1, 0), set_sum(1, 1))
    beta = norm1 / norm0
    _, variance1 = moments(2, (keep + beta) * values0 - pull * image_values, [])
    direction_dot = norm1 + 2.0 * beta * cross + beta * beta * norm0
    step1 = norm1 / (variance1 + diag_shift * direction_dot)

    for_force = step0 + step1 * (keep + beta)
    for_image = step1 * pull
    with jax.named_scope("out"):
        for at in range(parts):
            cols = slice(at * PART, (at + 1) * PART)
            out_ref[:, cols] = for_force * force_ref[:, cols] - for_image * image_all[at, core, parity, half]
        out_b_ref[...] = for_force * force_b_ref[...] - for_image * image_b[0]

        for which in range(4):
            spin_copy(which).wait_send()
        each_part(force_sent)
        each_part(gather_sent)

        def sums_sent(at):
            core_copy(at).wait_send()
            z_copy(at).wait_send()
            x_copy(at).wait_send()

        each_part(sums_sent)


def body(groups, shards, spins_packed, weight, hidden_bias, force_w, force_b):
    words, here = spins_packed.shape
    inputs, units = weight.shape
    rows = force_w.shape[0]
    ranks = shards // SETS
    samples, pair = ranks * here, SETS * rows
    parts = units // PART
    vmem = pl.BlockSpec(memory_space=pltpu.VMEM)
    dma = pltpu.SemaphoreType.DMA
    update_w, update_b = pl.pallas_call(
        functools.partial(kernel, groups, ranks),
        out_shape=(jax.ShapeDtypeStruct((rows, units), F32), jax.ShapeDtypeStruct((1, units), F32)),
        in_specs=[vmem] * 5,
        out_specs=(vmem, vmem),
        scratch_shapes=[
            pltpu.VMEM((ranks, words, here), jnp.int32),
            pltpu.VMEM((units, inputs), BF16),
            pltpu.VMEM((units, 128), F32),
            pltpu.VMEM((inputs, min(512, here)), BF16),
            pltpu.VMEM((pair, samples), BF16),
            pltpu.VMEM((units, samples), BF16),
            pltpu.VMEM((parts, 2, 2, 2, rows, PART), F32),
            pltpu.VMEM((pair + PAD, units), BF16),
            pltpu.VMEM((pair + PAD, samples), BF16),
            pltpu.VMEM((parts, 2, 2, 2, rows, PART), F32),
            pltpu.VMEM((parts, 2, 2, rows, PART), F32),
            pltpu.VMEM((parts, 2, rows, PART), F32),
            pltpu.VMEM((parts, rows, PART), F32),
            pltpu.VMEM((parts, 2, 2, 2, rows, PART), F32),
            pltpu.VMEM((SETS, 1, units), F32),
            pltpu.VMEM((2, groups, 1, samples + EXTRA), F32),
            pltpu.VMEM((2, ranks, 1, samples + EXTRA), F32),
            pltpu.VMEM((3, SETS, 8, 128), F32),
            dma((4,)),
            dma((4,)),
            dma((parts, 5)),
            dma((parts, 5)),
            dma((parts, 5)),
            dma((parts, 5)),
            dma((parts, 3)),
            dma((parts, 3)),
            dma((2, groups)),
            dma((2, groups)),
            dma((2, ranks)),
            dma((2, ranks)),
            dma((3, SETS)),
            dma((3, SETS)),
            dma((SETS,)),
            dma((SETS,)),
        ],
        compiler_params=pltpu.CompilerParams(
            collective_id=0, has_side_effects=True, vmem_limit_bytes=62 * 1024 * 1024
        ),
    )(spins_packed, weight, hidden_bias.reshape(1, -1), force_w, force_b.reshape(1, -1))
    return update_w, update_b.reshape(-1)


def solution(mesh):
    placed = (P(None, "smp"), P(None, "grp"), P("grp"), P("smp", "grp"), P("grp"))
    return jax.shard_map(
        functools.partial(body, mesh.shape["grp"], mesh.shape["smp"]),
        mesh=mesh, in_specs=placed, out_specs=(P("smp", "grp"), P("grp")), check_vma=False,
    )
```

```python
import functools

import jax
import jax.numpy as jnp
from jax import lax
from jax.experimental import pallas as pl
from jax.experimental.pallas import tpu as pltpu
from jax.sharding import PartitionSpec as P

MESH = pl.DeviceIdType.MESH
F32, BF16 = jnp.float32, jnp.bfloat16
diag_shift = 0.01
SETS = 8
EXTRA = 256
PAD = 16
PART = 256
LINE = 4


def total(x):
    return jnp.sum(jnp.sum(x, axis=0, keepdims=True), axis=1, keepdims=True)


def kernel(
    groups, shards,
    packed_in, weight_in, bias_in, force_in, force_b_in,
    out_ref, out_b_ref,
    packed, weight, weight_t, bias_ref, bias_t, force_b_ref, tile, spins, hidden, force_all, lhs, scaled,
    image, image_core, image_z, image_x, image_all, image_b, by_group, by_rank, by_set, by_shard,
    load, spin_send, spin_recv, pass_send, pass_recv, force_send, force_recv, image_send, image_recv,
    group_send, group_recv, rank_send, rank_recv, set_send, set_recv, bias_send, bias_recv, shard_send, shard_recv,
):
    grp, smp = lax.axis_index("grp"), lax.axis_index("smp")
    words, here = packed_in.shape
    inputs, units = weight.shape
    rows = force_in.shape[0]
    ranks = shards // SETS
    pair = SETS * rows
    samples = ranks * here
    count = samples * SETS
    quarter = here // LINE
    parts = units // PART
    depth = 2 * ranks

    core, z, half = lax.rem(smp, 2), lax.rem(smp // 2, depth), smp // (2 * depth)
    parity, rank = lax.rem(z, 2), z // 2
    member = (core * 2 + parity) * 2 + half
    y, column = lax.rem(grp, LINE), grp // LINE

    def device(half_at, z_at, core_at):
        return {"smp": (half_at * depth + z_at) * 2 + core_at}

    sibling = device(half, z, 1 - core)
    z_partner = device(half, z + 1 - 2 * parity, core)
    x_partner = device(1 - half, z, core)

    def group_device(at):
        return {"grp": at}

    def line_device(at):
        return {"grp": column * LINE + at}

    def rank_device(at):
        return device(half, 2 * at + parity, core)

    def set_device(at):
        return device(lax.rem(at, 2), 2 * rank + lax.rem(at // 2, 2), at // 4)

    def shard_device(at):
        return {"smp": at}

    def remote(source, target, send, recv, where):
        return pltpu.make_async_remote_copy(
            source, target, send, recv, device_id=where, device_id_type=MESH
        )

    barrier = pltpu.get_barrier_semaphore()
    for size, me, peer in ((groups, grp, group_device), (ranks, rank, rank_device)):
        for step in range(1, size):
            pl.semaphore_signal(barrier, device_id=peer(lax.rem(me + step, size)), device_id_type=MESH)
    for where in (sibling, z_partner, x_partner):
        pl.semaphore_signal(barrier, device_id=where, device_id_type=MESH)

    def cols_of(at):
        return slice(at * PART, (at + 1) * PART)

    loads = [
        pltpu.make_async_copy(weight_in, weight, load.at[0]),
        pltpu.make_async_copy(bias_in, bias_ref, load.at[1]),
        pltpu.make_async_copy(force_b_in, force_b_ref, load.at[2]),
    ]
    for at in range(LINE):
        loads.append(
            pltpu.make_async_copy(packed_in.at[:, pl.ds(at * quarter, quarter)], packed.at[rank, at], load.at[3 + at])
        )
    for at in range(parts):
        loads.append(
            pltpu.make_async_copy(
                force_in.at[:, pl.ds(at * PART, PART)], force_all.at[at, core, parity, half], load.at[3 + LINE + at]
            )
        )
    for copy in loads:
        copy.start()
    for copy in loads:
        copy.wait()

    def turn(at, carry):
        cols = pl.ds(pl.multiple_of(at * 256, 256), 256)
        weight_t[cols, :] = weight[:, cols].T
        bias_t[cols, :] = jnp.broadcast_to(bias_ref[:, cols], (128, 256)).T
        return carry

    with jax.named_scope("turn"):
        lax.fori_loop(0, units // 256, turn, 0)
    with jax.named_scope("barrier"):
        pl.semaphore_wait(barrier, groups + ranks + 1)

    after, before, across = lax.rem(rank + 1, ranks), lax.rem(rank + ranks - 1, ranks), lax.rem(rank + 2, ranks)

    def force_send_own(at, which, where):
        own = force_all.at[at, core, parity, half]
        remote(own, own, force_send.at[at, which], force_recv.at[at, which], where).start()

    def force_arrived(at, which):
        target = (
            force_all.at[at, core, 1 - parity, half],
            force_all.at[at, core, parity, 1 - half],
            force_all.at[at, core, 1 - parity, 1 - half],
            force_all.at[at, 1 - core, parity],
            force_all.at[at, 1 - core, 1 - parity],
        )[which]
        remote(target, target, force_send.at[at, which], force_recv.at[at, which], sibling).wait_recv()

    def force_x(at):
        force_arrived(at, 1)
        block_x = force_all.at[at, core, parity, 1 - half]
        remote(block_x, block_x, force_send.at[at, 2], force_recv.at[at, 2], z_partner).start()
        ours = force_all.at[at, core, parity]
        remote(ours, ours, force_send.at[at, 3], force_recv.at[at, 3], sibling).start()

    def force_z(at):
        force_arrived(at, 0)
        force_arrived(at, 2)
        theirs = force_all.at[at, core, 1 - parity]
        remote(theirs, theirs, force_send.at[at, 4], force_recv.at[at, 4], sibling).start()

    def force_whole(at):
        force_arrived(at, 3)
        force_arrived(at, 4)

    def spin_send_to(step):
        own = packed.at[rank, y]
        return remote(own, own, spin_send.at[step], spin_recv.at[rank], rank_device(lax.rem(rank + step, ranks)))

    def spin_arrived(source):
        target = packed.at[source, y]
        remote(target, target, spin_send.at[0], spin_recv.at[source], sibling).wait_recv()

    def hand_on(source, slot):
        copies = []
        for step in range(1, LINE):
            piece = packed.at[source, y]
            copies.append(
                remote(
                    piece, piece, pass_send.at[slot, step], pass_recv.at[source, y],
                    line_device(lax.rem(y + step, LINE)),
                )
            )
            copies[-1].start()
        return copies

    def handed(source, step):
        from_y = lax.rem(y + step, LINE)
        target = packed.at[source, from_y]
        remote(target, target, pass_send.at[0, 0], pass_recv.at[source, from_y], sibling).wait_recv()
        return source, from_y

    for at in range(parts):
        force_send_own(at, 1, x_partner)
    spin_copies = [spin_send_to(step) for step in (1, ranks - 1, 2)]
    for copy in spin_copies:
        copy.start()
    for at in range(parts):
        force_send_own(at, 0, z_partner)

    masks = jnp.left_shift(1, lax.broadcasted_iota(jnp.int32, (32, quarter), 0))

    def hidden_pair(*pieces):
        cols = [pl.ds(pl.multiple_of(source * here + at * quarter, quarter), quarter) for source, at in pieces]
        for which, (source, at) in enumerate(pieces):
            to = slice(which * quarter, (which + 1) * quarter)
            for word in range(words):
                bits = jnp.bitwise_and(jnp.broadcast_to(packed[source, at, word : word + 1, :], (32, quarter)), masks)
                tile[word * 32 : word * 32 + 32, to] = jnp.where(bits != 0, 1.0, -1.0).astype(BF16)
        for to in range(SETS):
            word = (to % 2) * 2 * depth + 4 * rank + 2 * (to // 2 % 2) + to // 4
            from_rows = pl.ds(pl.multiple_of(word * rows, rows), rows)
            for which in range(2):
                spins[to * rows : (to + 1) * rows, cols[which]] = tile[
                    from_rows, which * quarter : (which + 1) * quarter
                ]
        for unit in range(0, units, 512):
            these = pl.ds(unit, 512)
            pre = jnp.dot(weight_t[these, :], tile[...], preferred_element_type=F32)
            pre = pre + jnp.concatenate([bias_t[these, :]] * (2 * quarter // 128), axis=1)
            result = jnp.tanh(pre).astype(BF16)
            for which in range(2):
                hidden[these, cols[which]] = result[:, which * quarter : (which + 1) * quarter]

    def own_pair(at, carry):
        hidden_pair((rank, 2 * at), (rank, 2 * at + 1))
        return carry

    with jax.named_scope("hidden0"):
        lax.fori_loop(0, LINE // 2, own_pair, 0)
    with jax.named_scope("spinab"):
        spin_arrived(before)
        passed = hand_on(before, 0)
        spin_arrived(after)
        passed += hand_on(after, 1)
    with jax.named_scope("hidden1"):
        hidden_pair((before, y), (after, y))
    with jax.named_scope("spinc"):
        spin_arrived(across)
        passed += hand_on(across, 2)
        piece = handed(before, 1)
    with jax.named_scope("hidden2"):
        hidden_pair((across, y), piece)

    def third(at, carry):
        first = jnp.where(at == 0, before, after)
        second = jnp.where(at == 0, after, before)
        with jax.named_scope("w3"):
            force_x(2 * at)
            force_x(2 * at + 1)
            pieces = handed(first, 3), handed(second, 1 + at)
        hidden_pair(*pieces)
        return carry

    def fourth(at, carry):
        first = jnp.where(at == 0, after, across)
        with jax.named_scope("w4"):
            pieces = handed(first, 2 + at), handed(across, 1 + at)
            force_z(2 * at)
            force_z(2 * at + 1)
        hidden_pair(*pieces)
        return carry

    with jax.named_scope("hidden3"):
        lax.fori_loop(0, 2, third, 0)
    with jax.named_scope("hidden4"):
        lax.fori_loop(0, 2, fourth, 0)

    wide_block = min(2048, samples)

    def values_part(which, at, slots, row):
        for to in range(SETS):
            lhs[to * rows : (to + 1) * rows, cols_of(at)] = slots[at, to // 4, to // 2 % 2, to % 2].astype(BF16)
        lhs[pair:, cols_of(at)] = jnp.concatenate(
            [row[:, cols_of(at)] / ranks, jnp.zeros((PAD - 1, PART), F32)], axis=0
        ).astype(BF16)

        def run(to, carry):
            cols = pl.ds(pl.multiple_of(to * wide_block, wide_block), wide_block)
            product = jnp.dot(lhs[:, cols_of(at)], hidden[cols_of(at), cols], preferred_element_type=F32)
            value = jnp.sum(product[:pair] * spins[:, cols].astype(F32), axis=0, keepdims=True) + product[pair : pair + 1]
            by_group[which, grp, :, cols] = value if at == 0 else by_group[which, grp, :, cols] + value
            return carry

        lax.fori_loop(0, samples // wide_block, run, 0)

    for at in range(parts):
        with jax.named_scope("forcew"):
            force_whole(at)
        with jax.named_scope("values0"):
            values_part(0, at, force_all, force_b_ref)

    def gather(slot, size, me, peer, send, recv):
        copies = []
        for step in range(1, size):
            copies.append(remote(slot(me), slot(me), send.at[step], recv.at[me], peer(lax.rem(me + step, size))))
            copies[-1].start()

        def finish():
            for step in range(1, size):
                source = lax.rem(me + size - step, size)
                remote(slot(source), slot(source), send.at[step], recv.at[source], sibling).wait_recv()
            for copy in copies:
                copy.wait_send()

        return finish

    def wide(x, lanes=128):
        return jnp.broadcast_to(x, (1, lanes))

    def sum_groups(which, first, second):
        by_group[which, grp, :, samples:] = jnp.concatenate([wide(first), wide(second)], axis=1)
        with jax.named_scope("redg"):
            gather(lambda at: by_group.at[which, at], groups, grp, group_device, group_send.at[which], group_recv.at[which])()
            mine = by_group[which, 0]
            for source in range(1, groups):
                mine = mine + by_group[which, source]
            by_rank[which, rank] = mine
        return mine, gather(
            lambda at: by_rank.at[which, at], ranks, rank, rank_device, rank_send.at[which], rank_recv.at[which]
        )

    def sum_ranks(which):
        whole = by_rank[which, 0]
        for source in range(1, ranks):
            whole = whole + by_rank[which, source]
        return whole[:, :samples], whole[:, samples : samples + 1], whole[:, samples + 128 : samples + 129]

    def gather_sets(which, values):
        fill = jnp.zeros((8 - len(values), 128), F32)
        by_set[which, member] = jnp.concatenate([wide(value) for value in values] + [fill], axis=0)
        return gather(lambda at: by_set.at[which, at], SETS, member, set_device, set_send.at[which], set_recv.at[which])

    def set_sum(which, row):
        value = by_set[which, 0, row : row + 1, :]
        for source in range(1, SETS):
            value = value + by_set[which, source, row : row + 1, :]
        return value[:, :1]

    def own_force(at):
        return force_all[at, core, parity, half]

    force_dot = total(force_b_ref[...] * force_b_ref[...]) / shards
    for at in range(parts):
        force_dot = force_dot + total(own_force(at) * own_force(at))
    mine, finish_ranks = sum_groups(0, force_dot, jnp.zeros((1, 1), F32))
    with jax.named_scope("redr"):
        by_shard[smp] = wide(total(mine[:, :samples]))
        finish_mean = gather(lambda at: by_shard.at[at], shards, smp, shard_device, shard_send, shard_recv)
        finish_ranks()
        values0, own_dot, _ = sum_ranks(0)
    with jax.named_scope("mean"):
        finish_mean()
        mean0 = by_shard[0]
        for source in range(1, shards):
            mean0 = mean0 + by_shard[source]
        centred = values0 - mean0[:, :1] / count
    with jax.named_scope("scaled"):
        for at in range(0, samples, 512):
            weights = centred[:, at : at + 512]
            scaled[:pair, at : at + 512] = (spins[:, at : at + 512].astype(F32) * weights).astype(BF16)
            scaled[pair:, at : at + 512] = jnp.concatenate(
                [weights, jnp.zeros((PAD - 1, 512), F32)], axis=0
            ).astype(BF16)

    def image_copy(at, which):
        source, target, where = (
            (image.at[at, 1 - core], image_core.at[at], sibling),
            (image.at[at, core, 1 - parity], image_z.at[at], z_partner),
            (image.at[at, core, parity], image_x.at[at], x_partner),
            (image_all.at[at, core, parity], image_all.at[at, core, parity], z_partner),
            (image_all.at[at, core, parity], image_all.at[at, core, parity], sibling),
            (image_all.at[at, core, 1 - parity], image_all.at[at, core, 1 - parity], sibling),
        )[which]
        return remote(source, target, image_send.at[at, which], image_recv.at[at, which], where)

    def image_arrived(at, which):
        target = (
            image_core.at[at], image_z.at[at], image_x.at[at],
            image_all.at[at, core, 1 - parity], image_all.at[at, 1 - core, parity], image_all.at[at, 1 - core, 1 - parity],
        )[which]
        remote(target, target, image_send.at[at, which], image_recv.at[at, which], sibling).wait_recv()

    def image_part(at):
        part = lax.dot_general(
            scaled[...], hidden[cols_of(at), :], (((1,), (1,)), ((), ())), preferred_element_type=F32
        )
        for to in range(SETS):
            image[at, to // 4, to // 2 % 2, to % 2] = part[to * rows : (to + 1) * rows]
        image_copy(at, 0).start()
        image_b[member, :, cols_of(at)] = part[pair : pair + 1]

    def sum_core(at):
        image_arrived(at, 0)
        image[at, core, 1 - parity] = image[at, core, 1 - parity] + image_core[at, 1 - parity]
        image_copy(at, 1).start()
        image[at, core, parity] = image[at, core, parity] + image_core[at, parity]

    def sum_z(at):
        image_arrived(at, 1)
        image[at, core, parity] = image[at, core, parity] + image_z[at]
        image_copy(at, 2).start()

    def sum_x(at):
        image_arrived(at, 2)
        image_all[at, core, parity] = image[at, core, parity] + image_x[at]
        image_copy(at, 3).start()
        image_copy(at, 4).start()

    def share_z(at):
        image_arrived(at, 3)
        image_copy(at, 5).start()

    def image_values(at):
        image_arrived(at, 4)
        image_arrived(at, 5)
        values_part(1, at, image_all, image_b[0])

    def named(name, step, *at):
        with jax.named_scope(name):
            step(*at)

    named("image", image_part, 0)
    finish_moment = gather_sets(0, [total(centred * centred), own_dot])
    named("image", image_part, 1)
    named("core", sum_core, 0)
    named("image", image_part, 2)
    named("core", sum_core, 1)
    named("image", image_part, 3)
    finish_bias = gather(lambda at: image_b.at[at], SETS, member, set_device, bias_send, bias_recv)
    named("core", sum_core, 2)
    named("core", sum_core, 3)
    named("sumz", sum_z, 0)
    named("sumz", sum_z, 1)
    with jax.named_scope("bias"):
        finish_moment()
        finish_bias()
        norm0 = set_sum(0, 1)
        step0 = norm0 / (set_sum(0, 0) / count + diag_shift * norm0)
        keep = 1.0 - diag_shift * step0
        pull = step0 / count
        whole_b = image_b[0]
        for source in range(1, SETS):
            whole_b = whole_b + image_b[source]
        image_b[0] = whole_b
    named("sumz", sum_z, 2)
    named("sumx", sum_x, 0)
    named("sumz", sum_z, 3)
    named("sumx", sum_x, 1)
    named("sumx", sum_x, 2)
    named("sharez", share_z, 0)
    named("sumx", sum_x, 3)
    named("values1", image_values, 0)
    named("sharez", share_z, 1)
    with jax.named_scope("norm"):
        residual_b = keep * force_b_ref[...] - pull * whole_b
        own_norm = total(residual_b * residual_b) / shards
        own_cross = total(residual_b * force_b_ref[...]) / shards
        for at in range(parts):
            residual = keep * own_force(at) - pull * image_all[at, core, parity, half]
            own_norm = own_norm + total(residual * residual)
            own_cross = own_cross + total(residual * own_force(at))
        finish_norm = gather_sets(1, [own_norm, own_cross])
    named("values1", image_values, 1)
    named("sharez", share_z, 2)
    named("values1", image_values, 2)
    named("sharez", share_z, 3)
    named("values1", image_values, 3)
    named("fnorm", finish_norm)

    _, finish_ranks = sum_groups(1, set_sum(1, 0), set_sum(1, 1))
    with jax.named_scope("redr"):
        finish_ranks()
        values1, norm1, cross = sum_ranks(1)
    beta = norm1 / norm0
    with jax.named_scope("sets"):
        values1 = (keep + beta) * centred - pull * values1
        mean1 = total(values1) / samples
        values1 = values1 - mean1
        gather_sets(2, [mean1, total(values1 * values1)])()
        middle = set_sum(2, 0) / SETS
        spread = jnp.zeros((1, 1), F32)
        for source in range(SETS):
            shift = by_set[2, source, 0:1, :1] - middle
            spread = spread + shift * shift
        variance1 = (set_sum(2, 1) + samples * spread) / count
    direction_dot = norm1 + 2.0 * beta * cross + beta * beta * norm0
    step1 = norm1 / (variance1 + diag_shift * direction_dot)

    for_force = step0 + step1 * (keep + beta)
    for_image = step1 * pull
    with jax.named_scope("out"):
        for at in range(parts):
            out_ref[:, cols_of(at)] = for_force * own_force(at) - for_image * image_all[at, core, parity, half]
        out_b_ref[...] = for_force * force_b_ref[...] - for_image * image_b[0]

        for copy in spin_copies + passed:
            copy.wait_send()
        for at in range(parts):
            for which in range(5):
                target = force_all.at[at, core, parity] if which > 2 else force_all.at[at, core, parity, half]
                remote(target, target, force_send.at[at, which], force_recv.at[at, which], sibling).wait_send()
            for which in range(6):
                image_copy(at, which).wait_send()


def body(groups, shards, spins_packed, weight, hidden_bias, force_w, force_b):
    words, here = spins_packed.shape
    inputs, units = weight.shape
    rows = force_w.shape[0]
    ranks = shards // SETS
    samples, pair = ranks * here, SETS * rows
    parts = units // PART
    quarter = here // LINE
    vmem = pl.BlockSpec(memory_space=pltpu.VMEM)
    anywhere = pl.BlockSpec(memory_space=pl.ANY)
    dma = pltpu.SemaphoreType.DMA
    update_w, update_b = pl.pallas_call(
        functools.partial(kernel, groups, shards),
        out_shape=(jax.ShapeDtypeStruct((rows, units), F32), jax.ShapeDtypeStruct((1, units), F32)),
        in_specs=[anywhere] * 5,
        out_specs=(vmem, vmem),
        scratch_shapes=[
            pltpu.VMEM((ranks, LINE, words, quarter), jnp.int32),
            pltpu.VMEM((inputs, units), BF16),
            pltpu.VMEM((units, inputs), BF16),
            pltpu.VMEM((1, units), F32),
            pltpu.VMEM((units, 128), F32),
            pltpu.VMEM((1, units), F32),
            pltpu.VMEM((inputs, 2 * quarter), BF16),
            pltpu.VMEM((pair, samples), BF16),
            pltpu.VMEM((units, samples), BF16),
            pltpu.VMEM((parts, 2, 2, 2, rows, PART), F32),
            pltpu.VMEM((pair + PAD, units), BF16),
            pltpu.VMEM((pair + PAD, samples), BF16),
            pltpu.VMEM((parts, 2, 2, 2, rows, PART), F32),
            pltpu.VMEM((parts, 2, 2, rows, PART), F32),
            pltpu.VMEM((parts, 2, rows, PART), F32),
            pltpu.VMEM((parts, 2, rows, PART), F32),
            pltpu.VMEM((parts, 2, 2, 2, rows, PART), F32),
            pltpu.VMEM((SETS, 1, units), F32),
            pltpu.VMEM((2, groups, 1, samples + EXTRA), F32),
            pltpu.VMEM((2, ranks, 1, samples + EXTRA), F32),
            pltpu.VMEM((3, SETS, 8, 128), F32),
            pltpu.VMEM((shards, 1, 128), F32),
            dma((3 + LINE + parts,)),
            dma((ranks,)),
            dma((ranks,)),
            dma((3, LINE)),
            dma((ranks, LINE)),
            dma((parts, 5)),
            dma((parts, 5)),
            dma((parts, 6)),
            dma((parts, 6)),
            dma((2, groups)),
            dma((2, groups)),
            dma((2, ranks)),
            dma((2, ranks)),
            dma((3, SETS)),
            dma((3, SETS)),
            dma((SETS,)),
            dma((SETS,)),
            dma((shards,)),
            dma((shards,)),
        ],
        compiler_params=pltpu.CompilerParams(
            collective_id=0, has_side_effects=True, vmem_limit_bytes=62 * 1024 * 1024
        ),
    )(spins_packed, weight, hidden_bias.reshape(1, -1), force_w, force_b.reshape(1, -1))
    return update_w, update_b.reshape(-1)


def solution(mesh):
    placed = (P(None, "smp"), P(None, "grp"), P("grp"), P("smp", "grp"), P("grp"))
    return jax.shard_map(
        functools.partial(body, mesh.shape["grp"], mesh.shape["smp"]),
        mesh=mesh, in_specs=placed, out_specs=(P("smp", "grp"), P("grp")), check_vma=False,
    )
```

```python
import functools

import jax
import jax.numpy as jnp
from jax import lax
from jax.experimental import pallas as pl
from jax.experimental.pallas import tpu as pltpu
from jax.sharding import PartitionSpec as P

MESH = pl.DeviceIdType.MESH
F32, BF16 = jnp.float32, jnp.bfloat16
diag_shift = 0.01
SETS = 8
EXTRA = 256
PAD = 16
PART = 256
LINE = 4


def total(x):
    return jnp.sum(jnp.sum(x, axis=0, keepdims=True), axis=1, keepdims=True)


def kernel(
    groups, shards,
    packed_in, weight_in, bias_in, force_in, force_b_in,
    image_ref, image_b_ref, own_ref, scale_ref,
    packed, weight, weight_t, bias_ref, bias_t, force_b_ref, tile, spins, hidden, force_all, lhs, scaled,
    image, image_core, image_z, image_x, image_all, image_b, by_group, by_rank, by_set, by_shard, by_total,
    load, spin_send, spin_recv, pass_send, pass_recv, force_send, force_recv, image_send, image_recv,
    gather_send, gather_recv,
):
    grp, smp = lax.axis_index("grp"), lax.axis_index("smp")
    words, here = packed_in.shape
    inputs, units = weight.shape
    rows = force_in.shape[0]
    ranks = shards // SETS
    pair = SETS * rows
    samples = ranks * here
    count = samples * SETS
    quarter = here // LINE
    parts = units // PART
    depth = 2 * ranks

    core, z, half = lax.rem(smp, 2), lax.rem(smp // 2, depth), smp // (2 * depth)
    parity, rank = lax.rem(z, 2), z // 2
    member = (core * 2 + parity) * 2 + half
    y, column = lax.rem(grp, LINE), grp // LINE

    def device(half_at, z_at, core_at):
        return {"smp": (half_at * depth + z_at) * 2 + core_at}

    sibling = device(half, z, 1 - core)
    z_partner = device(half, z + 1 - 2 * parity, core)
    x_partner = device(1 - half, z, core)

    def group_device(at):
        return {"grp": at}

    def line_device(at):
        return {"grp": column * LINE + at}

    def rank_device(at):
        return device(half, 2 * at + parity, core)

    def set_device(at):
        return device(lax.rem(at, 2), 2 * rank + lax.rem(at // 2, 2), at // 4)

    def shard_device(at):
        return {"smp": at}

    def remote(source, target, send, recv, where):
        return pltpu.make_async_remote_copy(
            source, target, send, recv, device_id=where, device_id_type=MESH
        )

    barrier = pltpu.get_barrier_semaphore()
    for size, me, peer in ((groups, grp, group_device), (ranks, rank, rank_device)):
        for step in range(1, size):
            pl.semaphore_signal(barrier, device_id=peer(lax.rem(me + step, size)), device_id_type=MESH)
    for where in (sibling, z_partner, x_partner):
        pl.semaphore_signal(barrier, device_id=where, device_id_type=MESH)

    def cols_of(at):
        return slice(at * PART, (at + 1) * PART)

    def cols_ds(at):
        return pl.ds(pl.multiple_of(at * PART, PART), PART)

    def load_all():
        copies = [
            pltpu.make_async_copy(weight_in, weight, load.at[0]),
            pltpu.make_async_copy(bias_in, bias_ref, load.at[1]),
            pltpu.make_async_copy(force_b_in, force_b_ref, load.at[2]),
        ]
        for at in range(LINE):
            copies.append(
                pltpu.make_async_copy(packed_in.at[:, pl.ds(at * quarter, quarter)], packed.at[rank, at], load.at[3])
            )
        for at in range(parts):
            copies.append(
                pltpu.make_async_copy(force_in.at[:, cols_ds(at)], force_all.at[at, core, parity, half], load.at[4])
            )
        for copy in copies:
            copy.start()
        for copy in copies[:3]:
            copy.wait()
        pltpu.make_async_copy(packed.at[rank], packed.at[rank], load.at[3]).wait()
        blocks = force_all.at[:, core, parity, half]
        pltpu.make_async_copy(blocks, blocks, load.at[4]).wait()

    load_all()

    def turn(at, carry):
        cols = pl.ds(pl.multiple_of(at * 256, 256), 256)
        weight_t[cols, :] = weight[:, cols].T
        bias_t[cols, :] = jnp.broadcast_to(bias_ref[:, cols], (128, 256)).T
        return carry

    with jax.named_scope("turn"):
        lax.fori_loop(0, units // 256, turn, 0)
    with jax.named_scope("barrier"):
        pl.semaphore_wait(barrier, groups + ranks + 1)

    after, before, across = lax.rem(rank + 1, ranks), lax.rem(rank + ranks - 1, ranks), lax.rem(rank + 2, ranks)

    def force_send_own(at, which, where):
        own = force_all.at[at, core, parity, half]
        remote(own, own, force_send.at[which], force_recv.at[at, which], where).start()

    def force_arrived(at, which):
        target = (
            force_all.at[at, core, 1 - parity, half],
            force_all.at[at, core, parity, 1 - half],
            force_all.at[at, core, 1 - parity, 1 - half],
            force_all.at[at, 1 - core, parity],
            force_all.at[at, 1 - core, 1 - parity],
        )[which]
        remote(target, target, force_send.at[which], force_recv.at[at, which], sibling).wait_recv()

    def force_x(at):
        force_arrived(at, 1)
        block_x = force_all.at[at, core, parity, 1 - half]
        remote(block_x, block_x, force_send.at[2], force_recv.at[at, 2], z_partner).start()
        ours = force_all.at[at, core, parity]
        remote(ours, ours, force_send.at[3], force_recv.at[at, 3], sibling).start()

    def force_z(at):
        force_arrived(at, 0)
        force_arrived(at, 2)
        theirs = force_all.at[at, core, 1 - parity]
        remote(theirs, theirs, force_send.at[4], force_recv.at[at, 4], sibling).start()

    def force_whole(at):
        force_arrived(at, 3)
        force_arrived(at, 4)

    def spin_send_to(step):
        own = packed.at[rank, y]
        return remote(own, own, spin_send.at[0], spin_recv.at[rank], rank_device(lax.rem(rank + step, ranks)))

    def spin_arrived(source):
        target = packed.at[source, y]
        remote(target, target, spin_send.at[0], spin_recv.at[source], sibling).wait_recv()

    def hand_on(source, slot):
        for step in range(1, LINE):
            piece = packed.at[source, y]
            remote(
                piece, piece, pass_send.at[slot], pass_recv.at[source, y], line_device(lax.rem(y + step, LINE))
            ).start()

    def handed(source, step):
        from_y = lax.rem(y + step, LINE)
        target = packed.at[source, from_y]
        remote(target, target, pass_send.at[0], pass_recv.at[source, from_y], sibling).wait_recv()
        return source, from_y

    for at in range(parts):
        force_send_own(at, 1, x_partner)
    for step in (1, ranks - 1, 2):
        spin_send_to(step).start()
    for at in range(parts):
        force_send_own(at, 0, z_partner)

    masks = jnp.left_shift(1, lax.broadcasted_iota(jnp.int32, (32, quarter), 0))

    def hidden_pair(*pieces):
        cols = [pl.ds(pl.multiple_of(source * here + at * quarter, quarter), quarter) for source, at in pieces]
        for which, (source, at) in enumerate(pieces):
            to = slice(which * quarter, (which + 1) * quarter)
            for word in range(words):
                bits = jnp.bitwise_and(jnp.broadcast_to(packed[source, at, word : word + 1, :], (32, quarter)), masks)
                tile[word * 32 : word * 32 + 32, to] = jnp.where(bits != 0, 1.0, -1.0).astype(BF16)
        for to in range(SETS):
            word = (to % 2) * 2 * depth + 4 * rank + 2 * (to // 2 % 2) + to // 4
            from_rows = pl.ds(pl.multiple_of(word * rows, rows), rows)
            for which in range(2):
                spins[to * rows : (to + 1) * rows, cols[which]] = tile[
                    from_rows, which * quarter : (which + 1) * quarter
                ]
        for unit in range(0, units, 512):
            these = pl.ds(unit, 512)
            pre = jnp.dot(weight_t[these, :], tile[...], preferred_element_type=F32)
            pre = pre + jnp.concatenate([bias_t[these, :]] * (2 * quarter // 128), axis=1)
            result = jnp.tanh(pre).astype(BF16)
            for which in range(2):
                hidden[these, cols[which]] = result[:, which * quarter : (which + 1) * quarter]

    def own_pair(at, carry):
        hidden_pair((rank, 2 * at), (rank, 2 * at + 1))
        return carry

    with jax.named_scope("hidden0"):
        lax.fori_loop(0, LINE // 2, own_pair, 0)
    with jax.named_scope("spinab"):
        spin_arrived(before)
        hand_on(before, 0)
        spin_arrived(after)
        hand_on(after, 1)
    with jax.named_scope("hidden1"):
        hidden_pair((before, y), (after, y))
    with jax.named_scope("spinc"):
        spin_arrived(across)
        hand_on(across, 2)
        piece = handed(before, 1)
    with jax.named_scope("hidden2"):
        hidden_pair((across, y), piece)

    def third(at, carry):
        first = jnp.where(at == 0, before, after)
        second = jnp.where(at == 0, after, before)
        with jax.named_scope("w3"):
            force_x(2 * at)
            force_x(2 * at + 1)
            pieces = handed(first, 3), handed(second, 1 + at)
        hidden_pair(*pieces)
        return carry

    def fourth(at, carry):
        first = jnp.where(at == 0, after, across)
        with jax.named_scope("w4"):
            pieces = handed(first, 2 + at), handed(across, 1 + at)
            force_z(2 * at)
            force_z(2 * at + 1)
        hidden_pair(*pieces)
        return carry

    with jax.named_scope("hidden3"):
        lax.fori_loop(0, 2, third, 0)
    with jax.named_scope("hidden4"):
        lax.fori_loop(0, 2, fourth, 0)

    wide_block = min(2048, samples)

    def fill_lhs(at, slots, row):
        for to in range(SETS):
            lhs[to * rows : (to + 1) * rows, cols_of(at)] = slots[at, to // 4, to // 2 % 2, to % 2].astype(BF16)
        lhs[pair:, cols_of(at)] = jnp.concatenate(
            [row[:, cols_of(at)] / ranks, jnp.zeros((PAD - 1, PART), F32)], axis=0
        ).astype(BF16)

    def values_of(which, first, last):
        these = slice(first * PART, last * PART)

        def run(to, carry):
            cols = pl.ds(pl.multiple_of(to * wide_block, wide_block), wide_block)
            product = jnp.dot(lhs[:, these], hidden[these, cols], preferred_element_type=F32)
            value = jnp.sum(product[:pair] * spins[:, cols].astype(F32), axis=0, keepdims=True) + product[pair : pair + 1]
            by_group[which, grp, :, cols] = value if first == 0 else by_group[which, grp, :, cols] + value
            return carry

        lax.fori_loop(0, samples // wide_block, run, 0)

    with jax.named_scope("forcew"):
        for at in range(parts):
            force_whole(at)
            fill_lhs(at, force_all, force_b_ref)
    with jax.named_scope("values0"):
        values_of(0, 0, parts)

    def gather(slots, which, size, me, peer):
        send, recv = gather_send.at[which], gather_recv.at[which]
        for step in range(1, size):
            remote(slots.at[me], slots.at[me], send, recv, peer(lax.rem(me + step, size))).start()
        others = slots.at[pl.ds(0, size - 1)]

        def finish():
            remote(others, others, send, recv, sibling).wait()

        return finish

    def wide(x, lanes=128):
        return jnp.broadcast_to(x, (1, lanes))

    def sum_groups(which, first, second, between):
        by_group[which, grp, :, samples:] = jnp.concatenate([wide(first), wide(second)], axis=1)
        with jax.named_scope("redg"):
            finish = gather(by_group.at[which], which, groups, grp, group_device)
            between()
            finish()
            mine = by_group[which, 0]
            for source in range(1, groups):
                mine = mine + by_group[which, source]
            by_rank[which, rank] = mine
        return gather(by_rank.at[which], 2 + which, ranks, rank, rank_device)

    def sum_ranks(which):
        whole = by_rank[which, 0]
        for source in range(1, ranks):
            whole = whole + by_rank[which, source]
        return whole[:, :samples], whole[:, samples : samples + 1], whole[:, samples + 128 : samples + 129]

    def gather_sets(which, values):
        fill = jnp.zeros((8 - len(values), 128), F32)
        by_set[which, member] = jnp.concatenate([wide(value) for value in values] + [fill], axis=0)
        return gather(by_set.at[which], 4 + which, SETS, member, set_device)

    def set_sum(which, row):
        value = by_set[which, 0, row : row + 1, :]
        for source in range(1, SETS):
            value = value + by_set[which, source, row : row + 1, :]
        return value[:, :1]

    def own_force(at):
        return force_all[at, core, parity, half]

    force_dot = total(force_b_ref[...] * force_b_ref[...]) / shards
    for at in range(parts):
        force_dot = force_dot + total(own_force(at) * own_force(at))
    by_shard[smp] = wide(total(by_group[0, grp, :, :samples]))
    finish_shards = []

    def total_shards():
        finish_shards.append(gather(by_shard, 8, shards, smp, shard_device))

    finish_ranks = sum_groups(0, force_dot, jnp.zeros((1, 1), F32), total_shards)
    with jax.named_scope("shards"):
        finish_shards[0]()
        mine = by_shard[0]
        for source in range(1, shards):
            mine = mine + by_shard[source]
        by_total[grp] = mine
        finish_total = gather(by_total, 9, groups, grp, group_device)
    with jax.named_scope("redr"):
        finish_ranks()
        values0, own_dot, _ = sum_ranks(0)
    with jax.named_scope("mean"):
        finish_total()
        mean0 = by_total[0]
        for source in range(1, groups):
            mean0 = mean0 + by_total[source]
        centred = values0 - mean0[:, :1] / count
    with jax.named_scope("scaled"):
        for at in range(0, samples, 512):
            weights = centred[:, at : at + 512]
            scaled[:pair, at : at + 512] = (spins[:, at : at + 512].astype(F32) * weights).astype(BF16)
            scaled[pair:, at : at + 512] = jnp.concatenate(
                [weights, jnp.zeros((PAD - 1, 512), F32)], axis=0
            ).astype(BF16)

    def image_copy(at, which):
        source, target, where = (
            (image.at[at, 1 - core], image_core.at[at], sibling),
            (image.at[at, core, 1 - parity], image_z.at[at], z_partner),
            (image.at[at, core, parity], image_x.at[at], x_partner),
            (image_all.at[at, core, parity], image_all.at[at, core, parity], z_partner),
            (image_all.at[at, core, parity], image_all.at[at, core, parity], sibling),
            (image_all.at[at, core, 1 - parity], image_all.at[at, core, 1 - parity], sibling),
        )[which]
        return remote(source, target, image_send.at[which], image_recv.at[at, which], where)

    def image_arrived(at, which):
        target = (
            image_core.at[at], image_z.at[at], image_x.at[at],
            image_all.at[at, core, 1 - parity], image_all.at[at, 1 - core, parity], image_all.at[at, 1 - core, 1 - parity],
        )[which]
        remote(target, target, image_send.at[which], image_recv.at[at, which], sibling).wait_recv()

    def image_part(at):
        part = lax.dot_general(
            scaled[...], hidden[cols_ds(at), :], (((1,), (1,)), ((), ())), preferred_element_type=F32
        )
        for to in range(SETS):
            image[at, to // 4, to // 2 % 2, to % 2] = part[to * rows : (to + 1) * rows]
        image_copy(at, 0).start()
        image_b[member, :, cols_ds(at)] = part[pair : pair + 1]

    def sum_core(at):
        image_arrived(at, 0)
        image[at, core, 1 - parity] = image[at, core, 1 - parity] + image_core[at, 1 - parity]
        image_copy(at, 1).start()
        image[at, core, parity] = image[at, core, parity] + image_core[at, parity]

    def sum_z(at):
        image_arrived(at, 1)
        image[at, core, parity] = image[at, core, parity] + image_z[at]
        image_copy(at, 2).start()

    def sum_x(at):
        image_arrived(at, 2)
        image_all[at, core, parity] = image[at, core, parity] + image_x[at]
        image_copy(at, 3).start()
        image_copy(at, 4).start()

    def share_z(at):
        image_arrived(at, 3)
        image_copy(at, 5).start()

    def image_values(at):
        image_arrived(at, 4)
        image_arrived(at, 5)
        fill_lhs(at, image_all, image_b[0])
        values_of(1, at, at + 1)

    def named(name, step, *at):
        with jax.named_scope(name):
            step(*at)

    finish_moment = gather_sets(0, [total(centred * centred), own_dot])

    def image_step(at, carry):
        image_part(at)

        @pl.when(at > 0)
        def _():
            sum_core(at - 1)

        return carry

    with jax.named_scope("image"):
        lax.fori_loop(0, parts, image_step, 0)
    finish_bias = gather(image_b, 7, SETS, member, set_device)
    named("core", sum_core, 3)
    named("sumz", sum_z, 0)
    named("sumz", sum_z, 1)
    named("sumz", sum_z, 2)
    named("sumx", sum_x, 0)
    named("sumz", sum_z, 3)
    named("sumx", sum_x, 1)
    with jax.named_scope("bias"):
        finish_moment()
        finish_bias()
        norm0 = set_sum(0, 1)
        step0 = norm0 / (set_sum(0, 0) / count + diag_shift * norm0)
        keep = 1.0 - diag_shift * step0
        pull = step0 / count
        whole_b = image_b[0]
        for source in range(1, SETS):
            whole_b = whole_b + image_b[source]
        image_b[0] = whole_b
    named("sumx", sum_x, 2)
    named("sharez", share_z, 0)
    named("values1", image_values, 0)
    named("sumx", sum_x, 3)
    named("sharez", share_z, 1)
    with jax.named_scope("norm"):
        residual_b = keep * force_b_ref[...] - pull * whole_b
        own_norm = total(residual_b * residual_b) / shards
        own_cross = total(residual_b * force_b_ref[...]) / shards
        image_b_ref[0:1, :] = whole_b
        image_b_ref[1:2, :] = force_b_ref[...]
        for at in range(parts):
            force, own = own_force(at), image_all[at, core, parity, half]
            residual = keep * force - pull * own
            own_norm = own_norm + total(residual * residual)
            own_cross = own_cross + total(residual * force)
            image_ref[:, cols_of(at)] = own
            own_ref[:, cols_of(at)] = force
        finish_norm = gather_sets(1, [own_norm, own_cross])
    named("values1", image_values, 1)
    named("sharez", share_z, 2)
    named("values1", image_values, 2)
    named("sharez", share_z, 3)
    named("values1", image_values, 3)
    named("fnorm", finish_norm)

    finish_ranks = sum_groups(1, set_sum(1, 0), set_sum(1, 1), lambda: None)
    with jax.named_scope("redr"):
        finish_ranks()
        values1, norm1, cross = sum_ranks(1)
    beta = norm1 / norm0
    with jax.named_scope("sets"):
        values1 = (keep + beta) * centred - pull * values1
        mean1 = total(values1) / samples
        values1 = values1 - mean1
        gather_sets(2, [mean1, total(values1 * values1)])()
        middle = set_sum(2, 0) / SETS
        spread = jnp.zeros((1, 1), F32)
        for source in range(SETS):
            shift = by_set[2, source, 0:1, :1] - middle
            spread = spread + shift * shift
        variance1 = (set_sum(2, 1) + samples * spread) / count
    direction_dot = norm1 + 2.0 * beta * cross + beta * beta * norm0
    step1 = norm1 / (variance1 + diag_shift * direction_dot)

    for_force = step0 + step1 * (keep + beta)
    for_image = step1 * pull
    scale_ref[...] = jnp.concatenate([wide(for_force), wide(for_image), jnp.zeros((6, 128), F32)], axis=0)
    with jax.named_scope("out"):
        pieces = packed.at[rank, pl.ds(0, LINE - 1)]
        remote(pieces, pieces, spin_send.at[0], spin_recv.at[0], sibling).wait_send()
        for slot in range(3):
            remote(pieces, pieces, pass_send.at[slot], spin_recv.at[0], sibling).wait_send()
        for which in range(5):
            blocks = force_all.at[:, core, parity] if which > 2 else force_all.at[:, core, parity, half]
            remote(blocks, blocks, force_send.at[which], spin_recv.at[0], sibling).wait_send()
        for which in range(6):
            blocks = image_core if which == 0 else image_z
            remote(blocks, blocks, image_send.at[which], spin_recv.at[0], sibling).wait_send()


def finish_kernel(image_ref, image_b_ref, force_ref, scale_ref, out_ref, out_b_ref):
    for_force, for_image = scale_ref[0:1, 0:1], scale_ref[1:2, 0:1]
    out_ref[...] = for_force * force_ref[...] - for_image * image_ref[...]
    out_b_ref[...] = for_force * image_b_ref[1:2, :] - for_image * image_b_ref[0:1, :]


def body(groups, shards, spins_packed, weight, hidden_bias, force_w, force_b):
    words, here = spins_packed.shape
    inputs, units = weight.shape
    rows = force_w.shape[0]
    ranks = shards // SETS
    samples, pair = ranks * here, SETS * rows
    parts = units // PART
    quarter = here // LINE
    vmem = pl.BlockSpec(memory_space=pltpu.VMEM)
    anywhere = pl.BlockSpec(memory_space=pl.ANY)
    dma = pltpu.SemaphoreType.DMA
    results = pl.pallas_call(
        functools.partial(kernel, groups, shards),
        out_shape=(
            pltpu.VMEM((rows, units), F32), pltpu.VMEM((8, units), F32),
            pltpu.VMEM((rows, units), F32), pltpu.VMEM((8, 128), F32),
        ),
        in_specs=[anywhere] * 5,
        out_specs=(vmem,) * 4,
        scratch_shapes=[
            pltpu.VMEM((ranks, LINE, words, quarter), jnp.int32),
            pltpu.VMEM((inputs, units), BF16),
            pltpu.VMEM((units, inputs), BF16),
            pltpu.VMEM((1, units), F32),
            pltpu.VMEM((units, 128), F32),
            pltpu.VMEM((1, units), F32),
            pltpu.VMEM((inputs, 2 * quarter), BF16),
            pltpu.VMEM((pair, samples), BF16),
            pltpu.VMEM((units, samples), BF16),
            pltpu.VMEM((parts, 2, 2, 2, rows, PART), F32),
            pltpu.VMEM((pair + PAD, units), BF16),
            pltpu.VMEM((pair + PAD, samples), BF16),
            pltpu.VMEM((parts, 2, 2, 2, rows, PART), F32),
            pltpu.VMEM((parts, 2, 2, rows, PART), F32),
            pltpu.VMEM((parts, 2, rows, PART), F32),
            pltpu.VMEM((parts, 2, rows, PART), F32),
            pltpu.VMEM((parts, 2, 2, 2, rows, PART), F32),
            pltpu.VMEM((SETS, 1, units), F32),
            pltpu.VMEM((2, groups, 1, samples + EXTRA), F32),
            pltpu.VMEM((2, ranks, 1, samples + EXTRA), F32),
            pltpu.VMEM((3, SETS, 8, 128), F32),
            pltpu.VMEM((shards, 1, 128), F32),
            pltpu.VMEM((groups, 1, 128), F32),
            dma((5,)),
            dma((1,)),
            dma((ranks,)),
            dma((3,)),
            dma((ranks, LINE)),
            dma((5,)),
            dma((parts, 5)),
            dma((6,)),
            dma((parts, 6)),
            dma((10,)),
            dma((10,)),
        ],
        compiler_params=pltpu.CompilerParams(
            collective_id=0, has_side_effects=True, vmem_limit_bytes=62 * 1024 * 1024
        ),
    )(spins_packed, weight, hidden_bias.reshape(1, -1), force_w, force_b.reshape(1, -1))
    update_w, update_b = pl.pallas_call(
        finish_kernel,
        out_shape=(jax.ShapeDtypeStruct((rows, units), F32), jax.ShapeDtypeStruct((1, units), F32)),
        in_specs=[vmem] * 4,
        out_specs=(vmem, vmem),
    )(*[pltpu.with_memory_space_constraint(result, pltpu.VMEM) for result in results])
    return update_w, update_b.reshape(-1)


def solution(mesh):
    placed = (P(None, "smp"), P(None, "grp"), P("grp"), P("smp", "grp"), P("grp"))
    return jax.shard_map(
        functools.partial(body, mesh.shape["grp"], mesh.shape["smp"]),
        mesh=mesh, in_specs=placed, out_specs=(P("smp", "grp"), P("grp")), check_vma=False,
    )
```

```python
import functools

import jax
import jax.numpy as jnp
from jax import lax
from jax.experimental import pallas as pl
from jax.experimental.pallas import tpu as pltpu
from jax.sharding import PartitionSpec as P

MESH = pl.DeviceIdType.MESH
F32, BF16 = jnp.float32, jnp.bfloat16
diag_shift = 0.01
SETS = 8
EXTRA = 256
PAD = 16
PART = 256
LINE = 4


def total(x):
    return jnp.sum(jnp.sum(x, axis=0, keepdims=True), axis=1, keepdims=True)


def kernel(
    groups, shards,
    packed_in, weight_in, bias_in, force_in, force_b_in,
    image_ref, image_b_ref, own_ref, scale_ref,
    packed, weight, weight_t, bias_ref, bias_t, force_b_ref, tile_a, tile_b, spins, hidden, force_all, lhs, scaled,
    image, image_core, image_z, image_x, image_all, image_b, by_group_a, by_group_b, by_rank_a, by_rank_b, by_set, by_shard, by_total,
    load, spin_send, spin_recv, pass_send, pass_recv, force_send, force_recv, image_send, image_recv,
    gather_send, gather_recv,
):
    grp, smp = lax.axis_index("grp"), lax.axis_index("smp")
    words, here = packed_in.shape
    inputs, units = weight.shape
    rows = force_in.shape[0]
    ranks = shards // SETS
    pair = SETS * rows
    samples = ranks * here
    count = samples * SETS
    quarter = here // LINE
    parts = units // PART
    depth = 2 * ranks

    core, z, half = lax.rem(smp, 2), lax.rem(smp // 2, depth), smp // (2 * depth)
    parity, rank = lax.rem(z, 2), z // 2
    member = (core * 2 + parity) * 2 + half
    y, column = lax.rem(grp, LINE), grp // LINE

    def device(half_at, z_at, core_at):
        return {"smp": (half_at * depth + z_at) * 2 + core_at}

    sibling = device(half, z, 1 - core)
    z_partner = device(half, z + 1 - 2 * parity, core)
    x_partner = device(1 - half, z, core)

    def group_device(at):
        return {"grp": at}

    def line_device(at):
        return {"grp": column * LINE + at}

    def rank_device(at):
        return device(half, 2 * at + parity, core)

    def set_device(at):
        return device(lax.rem(at, 2), 2 * rank + lax.rem(at // 2, 2), at // 4)

    def shard_device(at):
        return {"smp": at}

    def remote(source, target, send, recv, where):
        return pltpu.make_async_remote_copy(
            source, target, send, recv, device_id=where, device_id_type=MESH
        )

    barrier = pltpu.get_barrier_semaphore()
    for size, me, peer in ((groups, grp, group_device), (ranks, rank, rank_device)):
        for step in range(1, size):
            pl.semaphore_signal(barrier, device_id=peer(lax.rem(me + step, size)), device_id_type=MESH)
    for where in (sibling, z_partner, x_partner):
        pl.semaphore_signal(barrier, device_id=where, device_id_type=MESH)

    def cols_of(at):
        return slice(at * PART, (at + 1) * PART)

    def cols_ds(at):
        return pl.ds(pl.multiple_of(at * PART, PART), PART)

    def load_all():
        copies = [
            pltpu.make_async_copy(weight_in, weight, load.at[0]),
            pltpu.make_async_copy(bias_in, bias_ref, load.at[1]),
            pltpu.make_async_copy(force_b_in, force_b_ref, load.at[2]),
        ]
        for at in range(LINE):
            copies.append(
                pltpu.make_async_copy(packed_in.at[:, pl.ds(at * quarter, quarter)], packed.at[rank, at], load.at[3])
            )
        for at in range(parts):
            copies.append(
                pltpu.make_async_copy(force_in.at[:, cols_ds(at)], force_all.at[at, core, parity, half], load.at[4])
            )
        for copy in copies:
            copy.start()
        for copy in copies[:3]:
            copy.wait()
        pltpu.make_async_copy(packed.at[rank], packed.at[rank], load.at[3]).wait()
        blocks = force_all.at[:, core, parity, half]
        pltpu.make_async_copy(blocks, blocks, load.at[4]).wait()

    load_all()

    def turn(at, carry):
        cols = pl.ds(pl.multiple_of(at * 256, 256), 256)
        weight_t[cols, :] = weight[:, cols].T
        bias_t[cols, :] = jnp.broadcast_to(bias_ref[:, cols], (128, 256)).T
        return carry

    with jax.named_scope("turn"):
        lax.fori_loop(0, units // 256, turn, 0)
    after, before, across = lax.rem(rank + 1, ranks), lax.rem(rank + ranks - 1, ranks), lax.rem(rank + 2, ranks)

    def force_send_own(at, which, where):
        own = force_all.at[at, core, parity, half]
        remote(own, own, force_send.at[which], force_recv.at[at, which], where).start()

    def force_arrived(at, which):
        target = (
            force_all.at[at, core, 1 - parity, half],
            force_all.at[at, core, parity, 1 - half],
            force_all.at[at, core, 1 - parity, 1 - half],
            force_all.at[at, 1 - core, parity],
            force_all.at[at, 1 - core, 1 - parity],
        )[which]
        remote(target, target, force_send.at[which], force_recv.at[at, which], sibling).wait_recv()

    def force_x(at):
        force_arrived(at, 1)
        block_x = force_all.at[at, core, parity, 1 - half]
        remote(block_x, block_x, force_send.at[2], force_recv.at[at, 2], z_partner).start()
        ours = force_all.at[at, core, parity]
        remote(ours, ours, force_send.at[3], force_recv.at[at, 3], sibling).start()

    def force_z(at):
        force_arrived(at, 0)
        force_arrived(at, 2)
        theirs = force_all.at[at, core, 1 - parity]
        remote(theirs, theirs, force_send.at[4], force_recv.at[at, 4], sibling).start()

    def force_whole(at):
        force_arrived(at, 3)
        force_arrived(at, 4)

    def spin_send_to(step):
        own = packed.at[rank, y]
        return remote(own, own, spin_send.at[0], spin_recv.at[rank], rank_device(lax.rem(rank + step, ranks)))

    def spin_arrived(source):
        target = packed.at[source, y]
        remote(target, target, spin_send.at[0], spin_recv.at[source], sibling).wait_recv()

    def hand_on(source, slot):
        for step in range(1, LINE):
            piece = packed.at[source, y]
            remote(
                piece, piece, pass_send.at[slot], pass_recv.at[source, y], line_device(lax.rem(y + step, LINE))
            ).start()

    def handed(source, step):
        from_y = lax.rem(y + step, LINE)
        target = packed.at[source, from_y]
        remote(target, target, pass_send.at[0], pass_recv.at[source, from_y], sibling).wait_recv()
        return source, from_y

    masks = jnp.left_shift(1, lax.broadcasted_iota(jnp.int32, (32, quarter), 0))

    def places(pieces):
        return [pl.ds(pl.multiple_of(source * here + at * quarter, quarter), quarter) for source, at in pieces]

    def unpack(tile, pieces):
        cols = places(pieces)
        for which, (source, at) in enumerate(pieces):
            to = slice(which * quarter, (which + 1) * quarter)
            for word in range(words):
                bits = jnp.bitwise_and(jnp.broadcast_to(packed[source, at, word : word + 1, :], (32, quarter)), masks)
                tile[word * 32 : word * 32 + 32, to] = jnp.where(bits != 0, 1.0, -1.0).astype(BF16)
        for to in range(SETS):
            word = (to % 2) * 2 * depth + 4 * rank + 2 * (to // 2 % 2) + to // 4
            from_rows = pl.ds(pl.multiple_of(word * rows, rows), rows)
            for which in range(2):
                spins[to * rows : (to + 1) * rows, cols[which]] = tile[
                    from_rows, which * quarter : (which + 1) * quarter
                ]

    def activate(tile, pieces):
        cols = places(pieces)
        for unit in range(0, units, 512):
            these = pl.ds(unit, 512)
            pre = jnp.dot(weight_t[these, :], tile[...], preferred_element_type=F32)
            pre = pre + jnp.concatenate([bias_t[these, :]] * (2 * quarter // 128), axis=1)
            result = jnp.tanh(pre).astype(BF16)
            for which in range(2):
                hidden[these, cols[which]] = result[:, which * quarter : (which + 1) * quarter]

    first, second = ((rank, 0), (rank, 1)), ((rank, 2), (rank, 3))
    with jax.named_scope("unpack0"):
        unpack(tile_a, first)
    with jax.named_scope("barrier"):
        pl.semaphore_wait(barrier, groups + ranks + 1)
    for at in range(parts):
        force_send_own(at, 1, x_partner)
    for step in (1, ranks - 1, 2):
        spin_send_to(step).start()
    for at in range(parts):
        force_send_own(at, 0, z_partner)

    with jax.named_scope("hidden0"):
        unpack(tile_b, second)
        activate(tile_a, first)
    with jax.named_scope("hidden1"):
        activate(tile_b, second)
    with jax.named_scope("spinab"):
        spin_arrived(before)
        hand_on(before, 0)
        spin_arrived(after)
        hand_on(after, 1)
    with jax.named_scope("hidden2"):
        pieces = ((before, y), (after, y))
        unpack(tile_a, pieces)
        activate(tile_a, pieces)
    with jax.named_scope("spinc"):
        spin_arrived(across)
        hand_on(across, 2)
        for at in range(parts):
            force_x(at)
        pieces = ((across, y), handed(before, 1))
    with jax.named_scope("unpack3"):
        unpack(tile_b, pieces)
    now, later = tile_b, tile_a
    for step, ((source_a, from_a), (source_b, from_b)) in enumerate(
        (((before, 3), (after, 1)), ((after, 3), (before, 2)), ((after, 2), (across, 1)), ((across, 3), (across, 2)))
    ):
        with jax.named_scope("wait"):
            if step >= 2:
                force_z(2 * step - 4)
                force_z(2 * step - 3)
            coming = (handed(source_a, from_a), handed(source_b, from_b))
        with jax.named_scope("hidden3"):
            unpack(later, coming)
            activate(now, pieces)
        now, later, pieces = later, now, coming
    with jax.named_scope("hidden4"):
        activate(now, pieces)

    span = samples // 2
    by_group, by_rank = (by_group_a, by_group_b), (by_rank_a, by_rank_b)

    def fill_lhs(at, slots, row):
        for to in range(SETS):
            lhs[to * rows : (to + 1) * rows, cols_of(at)] = slots[at, to // 4, to // 2 % 2, to % 2].astype(BF16)
        lhs[pair:, cols_of(at)] = jnp.concatenate(
            [row[:, cols_of(at)] / ranks, jnp.zeros((PAD - 1, PART), F32)], axis=0
        ).astype(BF16)

    def values_of(which, first, last, side):
        these, cols = slice(first * PART, last * PART), slice(side * span, (side + 1) * span)
        product = jnp.dot(lhs[:, these], hidden[these, cols], preferred_element_type=F32)
        value = jnp.sum(product[:pair] * spins[:, cols].astype(F32), axis=0, keepdims=True) + product[pair : pair + 1]
        mine = by_group[side].at[which, grp, :, :span]
        mine[...] = value if first == 0 else mine[...] + value

    with jax.named_scope("forcew"):
        for at in range(parts):
            force_whole(at)
            fill_lhs(at, force_all, force_b_ref)
    def gather(slots, which, size, me, peer):
        send, recv = gather_send.at[which], gather_recv.at[which]
        for step in range(1, size):
            remote(slots.at[me], slots.at[me], send, recv, peer(lax.rem(me + step, size))).start()
        others = slots.at[pl.ds(0, size - 1)]

        def finish():
            remote(others, others, send, recv, sibling).wait()

        return finish

    def wide(x, lanes=128):
        return jnp.broadcast_to(x, (1, lanes))

    def send_groups(which, side):
        return gather(by_group[side].at[which], 2 * which + side, groups, grp, group_device)

    def send_ranks(which, side):
        mine = by_group[side][which, 0]
        for source in range(1, groups):
            mine = mine + by_group[side][which, source]
        by_rank[side][which, rank] = mine
        return gather(by_rank[side].at[which], 4 + 2 * which + side, ranks, rank, rank_device)

    def sum_ranks(which, side):
        whole = by_rank[side][which, 0]
        for source in range(1, ranks):
            whole = whole + by_rank[side][which, source]
        return whole

    def gather_sets(which, values):
        fill = jnp.zeros((8 - len(values), 128), F32)
        by_set[which, member] = jnp.concatenate([wide(value) for value in values] + [fill], axis=0)
        return gather(by_set.at[which], 8 + which, SETS, member, set_device)

    def set_sum(which, row):
        value = by_set[which, 0, row : row + 1, :]
        for source in range(1, SETS):
            value = value + by_set[which, source, row : row + 1, :]
        return value[:, :1]

    def own_force(at):
        return force_all[at, core, parity, half]

    force_dot = total(force_b_ref[...] * force_b_ref[...]) / shards
    for at in range(parts):
        force_dot = force_dot + total(own_force(at) * own_force(at))
    def extras(which, first, second):
        by_group[1][which, grp, :, span:] = jnp.concatenate([wide(first), wide(second)], axis=1)

    def own_sum(side):
        return total(by_group[side][0, grp, :, :span])

    with jax.named_scope("values0"):
        values_of(0, 0, parts, 0)
        finish_a = send_groups(0, 0)
        extras(0, force_dot, jnp.zeros((1, 1), F32))
        values_of(0, 0, parts, 1)
        finish_b = send_groups(0, 1)
    with jax.named_scope("redg"):
        by_shard[smp] = wide(own_sum(0) + own_sum(1))
        finish_shards = gather(by_shard, 12, shards, smp, shard_device)
        finish_a()
        finish_ranks_a = send_ranks(0, 0)
        finish_b()
        finish_ranks_b = send_ranks(0, 1)
    with jax.named_scope("shards"):
        finish_shards()
        mine = by_shard[0]
        for source in range(1, shards):
            mine = mine + by_shard[source]
        by_total[grp] = mine
        finish_total = gather(by_total, 13, groups, grp, group_device)
    with jax.named_scope("redr"):
        finish_ranks_a()
        finish_ranks_b()
        sums = [sum_ranks(0, side) for side in range(2)]
        own_dot = sums[1][:, span : span + 1]
    with jax.named_scope("mean"):
        finish_total()
        mean0 = by_total[0]
        for source in range(1, groups):
            mean0 = mean0 + by_total[source]
        mean0 = mean0[:, :1] / count
        centred = [whole[:, :span] - mean0 for whole in sums]
    with jax.named_scope("scaled"):
        for at in range(0, samples, 512):
            weights = centred[at // span][:, at % span : at % span + 512]
            scaled[:pair, at : at + 512] = (spins[:, at : at + 512].astype(F32) * weights).astype(BF16)
            scaled[pair:, at : at + 512] = jnp.concatenate(
                [weights, jnp.zeros((PAD - 1, 512), F32)], axis=0
            ).astype(BF16)

    def image_copy(at, which):
        source, target, where = (
            (image.at[at, 1 - core], image_core.at[at], sibling),
            (image.at[at, core, 1 - parity], image_z.at[at], z_partner),
            (image.at[at, core, parity], image_x.at[at], x_partner),
            (image_all.at[at, core, parity], image_all.at[at, core, parity], z_partner),
            (image_all.at[at, core, parity], image_all.at[at, core, parity], sibling),
            (image_all.at[at, core, 1 - parity], image_all.at[at, core, 1 - parity], sibling),
        )[which]
        return remote(source, target, image_send.at[which], image_recv.at[at, which], where)

    def image_arrived(at, which):
        target = (
            image_core.at[at], image_z.at[at], image_x.at[at],
            image_all.at[at, core, 1 - parity], image_all.at[at, 1 - core, parity], image_all.at[at, 1 - core, 1 - parity],
        )[which]
        remote(target, target, image_send.at[which], image_recv.at[at, which], sibling).wait_recv()

    def image_part(at):
        part = lax.dot_general(
            scaled[...], hidden[cols_ds(at), :], (((1,), (1,)), ((), ())), preferred_element_type=F32
        )
        for to in range(SETS):
            image[at, to // 4, to // 2 % 2, to % 2] = part[to * rows : (to + 1) * rows]
        image_copy(at, 0).start()
        image_b[member, :, cols_ds(at)] = part[pair : pair + 1]

    def sum_core(at):
        image_arrived(at, 0)
        image[at, core, 1 - parity] = image[at, core, 1 - parity] + image_core[at, 1 - parity]
        image_copy(at, 1).start()
        image[at, core, parity] = image[at, core, parity] + image_core[at, parity]

    def sum_z(at):
        image_arrived(at, 1)
        image[at, core, parity] = image[at, core, parity] + image_z[at]
        image_copy(at, 2).start()

    def sum_x(at):
        image_arrived(at, 2)
        image_all[at, core, parity] = image[at, core, parity] + image_x[at]
        image_copy(at, 3).start()
        image_copy(at, 4).start()

    def share_z(at):
        image_arrived(at, 3)
        image_copy(at, 5).start()

    def image_values(at):
        image_arrived(at, 4)
        image_arrived(at, 5)
        fill_lhs(at, image_all, image_b[0])
        values_of(1, at, at + 1, 0)
        if at < parts - 1:
            values_of(1, at, at + 1, 1)

    def named(name, step, *at):
        with jax.named_scope(name):
            step(*at)

    finish_moment = gather_sets(0, [total(centred[0] * centred[0]) + total(centred[1] * centred[1]), own_dot])

    def image_step(at, carry):
        image_part(at)

        @pl.when(at > 0)
        def _():
            sum_core(at - 1)

        return carry

    with jax.named_scope("image"):
        lax.fori_loop(0, parts, image_step, 0)
    finish_bias = gather(image_b, 11, SETS, member, set_device)
    named("core", sum_core, 3)
    named("sumz", sum_z, 0)
    named("sumz", sum_z, 1)
    named("sumz", sum_z, 2)
    named("sumx", sum_x, 0)
    named("sumz", sum_z, 3)
    named("sumx", sum_x, 1)
    with jax.named_scope("bias"):
        finish_moment()
        finish_bias()
        norm0 = set_sum(0, 1)
        step0 = norm0 / (set_sum(0, 0) / count + diag_shift * norm0)
        keep = 1.0 - diag_shift * step0
        pull = step0 / count
        whole_b = image_b[0]
        for source in range(1, SETS):
            whole_b = whole_b + image_b[source]
        image_b[0] = whole_b
    named("sumx", sum_x, 2)
    named("sharez", share_z, 0)
    named("sumx", sum_x, 3)
    named("sharez", share_z, 1)
    named("values1", image_values, 0)
    with jax.named_scope("norm"):
        residual_b = keep * force_b_ref[...] - pull * whole_b
        own_norm = total(residual_b * residual_b) / shards
        own_cross = total(residual_b * force_b_ref[...]) / shards
        image_b_ref[0:1, :] = whole_b
        image_b_ref[1:2, :] = force_b_ref[...]
        for at in range(parts):
            force, own = own_force(at), image_all[at, core, parity, half]
            residual = keep * force - pull * own
            own_norm = own_norm + total(residual * residual)
            own_cross = own_cross + total(residual * force)
            image_ref[:, cols_of(at)] = own
            own_ref[:, cols_of(at)] = force
        finish_norm = gather_sets(1, [own_norm, own_cross])
    named("sharez", share_z, 2)
    named("values1", image_values, 1)
    named("sharez", share_z, 3)
    named("values1", image_values, 2)
    named("fnorm", finish_norm)
    extras(1, set_sum(1, 0), set_sum(1, 1))
    with jax.named_scope("values1"):
        image_values(3)
        finish_a = send_groups(1, 0)
        values_of(1, parts - 1, parts, 1)
        finish_b = send_groups(1, 1)
    with jax.named_scope("redg"):
        finish_a()
        finish_ranks_a = send_ranks(1, 0)
        finish_b()
        finish_ranks_b = send_ranks(1, 1)
    with jax.named_scope("redr"):
        finish_ranks_a()
        finish_ranks_b()
        sums = [sum_ranks(1, side) for side in range(2)]
        norm1, cross = sums[1][:, span : span + 1], sums[1][:, span + 128 : span + 129]
    beta = norm1 / norm0
    with jax.named_scope("sets"):
        values1 = [(keep + beta) * centred[side] - pull * sums[side][:, :span] for side in range(2)]
        mean1 = (total(values1[0]) + total(values1[1])) / samples
        values1 = [value - mean1 for value in values1]
        gather_sets(2, [mean1, total(values1[0] * values1[0]) + total(values1[1] * values1[1])])()
        middle = set_sum(2, 0) / SETS
        spread = jnp.zeros((1, 1), F32)
        for source in range(SETS):
            shift = by_set[2, source, 0:1, :1] - middle
            spread = spread + shift * shift
        variance1 = (set_sum(2, 1) + samples * spread) / count
    direction_dot = norm1 + 2.0 * beta * cross + beta * beta * norm0
    step1 = norm1 / (variance1 + diag_shift * direction_dot)

    for_force = step0 + step1 * (keep + beta)
    for_image = step1 * pull
    scale_ref[...] = jnp.concatenate([wide(for_force), wide(for_image), jnp.zeros((6, 128), F32)], axis=0)
    with jax.named_scope("out"):
        pieces = packed.at[rank, pl.ds(0, LINE - 1)]
        remote(pieces, pieces, spin_send.at[0], spin_recv.at[0], sibling).wait_send()
        for slot in range(3):
            remote(pieces, pieces, pass_send.at[slot], spin_recv.at[0], sibling).wait_send()
        for which in range(5):
            blocks = force_all.at[:, core, parity] if which > 2 else force_all.at[:, core, parity, half]
            remote(blocks, blocks, force_send.at[which], spin_recv.at[0], sibling).wait_send()
        for which in range(6):
            blocks = image_core if which == 0 else image_z
            remote(blocks, blocks, image_send.at[which], spin_recv.at[0], sibling).wait_send()


def finish_kernel(image_ref, image_b_ref, force_ref, scale_ref, out_ref, out_b_ref):
    for_force, for_image = scale_ref[0:1, 0:1], scale_ref[1:2, 0:1]
    out_ref[...] = for_force * force_ref[...] - for_image * image_ref[...]
    out_b_ref[...] = for_force * image_b_ref[1:2, :] - for_image * image_b_ref[0:1, :]


def body(groups, shards, spins_packed, weight, hidden_bias, force_w, force_b):
    words, here = spins_packed.shape
    inputs, units = weight.shape
    rows = force_w.shape[0]
    ranks = shards // SETS
    samples, pair = ranks * here, SETS * rows
    parts = units // PART
    quarter = here // LINE
    vmem = pl.BlockSpec(memory_space=pltpu.VMEM)
    anywhere = pl.BlockSpec(memory_space=pl.ANY)
    dma = pltpu.SemaphoreType.DMA
    results = pl.pallas_call(
        functools.partial(kernel, groups, shards),
        out_shape=(
            pltpu.VMEM((rows, units), F32), pltpu.VMEM((8, units), F32),
            pltpu.VMEM((rows, units), F32), pltpu.VMEM((8, 128), F32),
        ),
        in_specs=[anywhere] * 5,
        out_specs=(vmem,) * 4,
        scratch_shapes=[
            pltpu.VMEM((ranks, LINE, words, quarter), jnp.int32),
            pltpu.VMEM((inputs, units), BF16),
            pltpu.VMEM((units, inputs), BF16),
            pltpu.VMEM((1, units), F32),
            pltpu.VMEM((units, 128), F32),
            pltpu.VMEM((1, units), F32),
            pltpu.VMEM((inputs, 2 * quarter), BF16),
            pltpu.VMEM((inputs, 2 * quarter), BF16),
            pltpu.VMEM((pair, samples), BF16),
            pltpu.VMEM((units, samples), BF16),
            pltpu.VMEM((parts, 2, 2, 2, rows, PART), F32),
            pltpu.VMEM((pair + PAD, units), BF16),
            pltpu.VMEM((pair + PAD, samples), BF16),
            pltpu.VMEM((parts, 2, 2, 2, rows, PART), F32),
            pltpu.VMEM((parts, 2, 2, rows, PART), F32),
            pltpu.VMEM((parts, 2, rows, PART), F32),
            pltpu.VMEM((parts, 2, rows, PART), F32),
            pltpu.VMEM((parts, 2, 2, 2, rows, PART), F32),
            pltpu.VMEM((SETS, 1, units), F32),
            pltpu.VMEM((2, groups, 1, samples // 2), F32),
            pltpu.VMEM((2, groups, 1, samples // 2 + EXTRA), F32),
            pltpu.VMEM((2, ranks, 1, samples // 2), F32),
            pltpu.VMEM((2, ranks, 1, samples // 2 + EXTRA), F32),
            pltpu.VMEM((3, SETS, 8, 128), F32),
            pltpu.VMEM((shards, 1, 128), F32),
            pltpu.VMEM((groups, 1, 128), F32),
            dma((5,)),
            dma((1,)),
            dma((ranks,)),
            dma((3,)),
            dma((ranks, LINE)),
            dma((5,)),
            dma((parts, 5)),
            dma((6,)),
            dma((parts, 6)),
            dma((14,)),
            dma((14,)),
        ],
        compiler_params=pltpu.CompilerParams(
            collective_id=0, has_side_effects=True, vmem_limit_bytes=62 * 1024 * 1024
        ),
    )(spins_packed, weight, hidden_bias.reshape(1, -1), force_w, force_b.reshape(1, -1))
    update_w, update_b = pl.pallas_call(
        finish_kernel,
        out_shape=(jax.ShapeDtypeStruct((rows, units), F32), jax.ShapeDtypeStruct((1, units), F32)),
        in_specs=[vmem] * 4,
        out_specs=(vmem, vmem),
    )(*[pltpu.with_memory_space_constraint(result, pltpu.VMEM) for result in results])
    return update_w, update_b.reshape(-1)


def solution(mesh):
    placed = (P(None, "smp"), P(None, "grp"), P("grp"), P("smp", "grp"), P("grp"))
    return jax.shard_map(
        functools.partial(body, mesh.shape["grp"], mesh.shape["smp"]),
        mesh=mesh, in_specs=placed, out_specs=(P("smp", "grp"), P("grp")), check_vma=False,
    )
```

```python
import functools

import jax
import jax.numpy as jnp
from jax import lax
from jax.experimental import pallas as pl
from jax.experimental.pallas import tpu as pltpu
from jax.sharding import PartitionSpec as P

MESH = pl.DeviceIdType.MESH
F32, BF16 = jnp.float32, jnp.bfloat16
diag_shift = 0.01
SETS = 8
EXTRA = 256
PAD = 16
PART = 256
LINE = 4


def total(x):
    return jnp.sum(jnp.sum(x, axis=0, keepdims=True), axis=1, keepdims=True)


def kernel(
    groups, shards,
    packed_in, weight_in, bias_in, force_in, force_b_in,
    image_ref, image_b_ref, own_ref, scale_ref,
    packed, weight, weight_t, bias_ref, bias_t, force_b_ref, tile, spins, hidden, force_all, lhs, scaled, plain,
    image, image_core, image_z, image_x, image_all, image_b, by_group_a, by_group_b, by_rank_a, by_rank_b, by_set, by_shard, by_total,
    load, spin_send, spin_recv, pass_send, pass_recv, force_send, force_recv, image_send, image_recv,
    gather_send, gather_recv,
):
    grp, smp = lax.axis_index("grp"), lax.axis_index("smp")
    words, here = packed_in.shape
    inputs, units = weight.shape
    rows = force_in.shape[0]
    ranks = shards // SETS
    pair = SETS * rows
    samples = ranks * here
    count = samples * SETS
    quarter = here // LINE
    parts = units // PART
    depth = 2 * ranks

    core, z, half = lax.rem(smp, 2), lax.rem(smp // 2, depth), smp // (2 * depth)
    parity, rank = lax.rem(z, 2), z // 2
    member = (core * 2 + parity) * 2 + half
    y, column = lax.rem(grp, LINE), grp // LINE

    def device(half_at, z_at, core_at):
        return {"smp": (half_at * depth + z_at) * 2 + core_at}

    sibling = device(half, z, 1 - core)
    z_partner = device(half, z + 1 - 2 * parity, core)
    x_partner = device(1 - half, z, core)

    def group_device(at):
        return {"grp": at}

    def line_device(at):
        return {"grp": column * LINE + at}

    def rank_device(at):
        return device(half, 2 * at + parity, core)

    def set_device(at):
        return device(lax.rem(at, 2), 2 * rank + lax.rem(at // 2, 2), at // 4)

    def shard_device(at):
        return {"smp": at}

    def remote(source, target, send, recv, where):
        return pltpu.make_async_remote_copy(
            source, target, send, recv, device_id=where, device_id_type=MESH
        )

    barrier = pltpu.get_barrier_semaphore()
    for size, me, peer in ((groups, grp, group_device), (ranks, rank, rank_device)):
        for step in range(1, size):
            pl.semaphore_signal(barrier, device_id=peer(lax.rem(me + step, size)), device_id_type=MESH)
    for where in (sibling, z_partner, x_partner):
        pl.semaphore_signal(barrier, device_id=where, device_id_type=MESH)

    def cols_of(at):
        return slice(at * PART, (at + 1) * PART)

    def cols_ds(at):
        return pl.ds(pl.multiple_of(at * PART, PART), PART)

    def load_all():
        copies = [
            pltpu.make_async_copy(weight_in, weight, load.at[0]),
            pltpu.make_async_copy(bias_in, bias_ref, load.at[1]),
            pltpu.make_async_copy(force_b_in, force_b_ref, load.at[2]),
        ]
        for at in range(LINE):
            copies.append(
                pltpu.make_async_copy(packed_in.at[:, pl.ds(at * quarter, quarter)], packed.at[rank, at], load.at[3])
            )
        for at in range(parts):
            copies.append(
                pltpu.make_async_copy(force_in.at[:, cols_ds(at)], force_all.at[at, core, parity, half], load.at[4])
            )
        for copy in copies:
            copy.start()
        for copy in copies[:3]:
            copy.wait()
        pltpu.make_async_copy(packed.at[rank], packed.at[rank], load.at[3]).wait()
        blocks = force_all.at[:, core, parity, half]
        pltpu.make_async_copy(blocks, blocks, load.at[4]).wait()

    load_all()

    def turn(at, carry):
        cols = pl.ds(pl.multiple_of(at * 256, 256), 256)
        weight_t[cols, :] = weight[:, cols].T
        bias_t[cols, :] = jnp.broadcast_to(bias_ref[:, cols], (128, 256)).T
        return carry

    with jax.named_scope("turn"):
        lax.fori_loop(0, units // 256, turn, 0)
    after, before, across = lax.rem(rank + 1, ranks), lax.rem(rank + ranks - 1, ranks), lax.rem(rank + 2, ranks)

    def force_send_own(at, which, where):
        own = force_all.at[at, core, parity, half]
        remote(own, own, force_send.at[which], force_recv.at[at, which], where).start()

    def force_arrived(at, which):
        target = (
            force_all.at[at, core, 1 - parity, half],
            force_all.at[at, core, parity, 1 - half],
            force_all.at[at, core, 1 - parity, 1 - half],
            force_all.at[at, 1 - core, parity],
            force_all.at[at, 1 - core, 1 - parity],
        )[which]
        remote(target, target, force_send.at[which], force_recv.at[at, which], sibling).wait_recv()

    def force_x(at):
        force_arrived(at, 1)
        block_x = force_all.at[at, core, parity, 1 - half]
        remote(block_x, block_x, force_send.at[2], force_recv.at[at, 2], z_partner).start()
        ours = force_all.at[at, core, parity]
        remote(ours, ours, force_send.at[3], force_recv.at[at, 3], sibling).start()

    def force_z(at):
        force_arrived(at, 0)
        force_arrived(at, 2)
        theirs = force_all.at[at, core, 1 - parity]
        remote(theirs, theirs, force_send.at[4], force_recv.at[at, 4], sibling).start()

    def force_whole(at):
        force_arrived(at, 3)
        force_arrived(at, 4)

    def spin_send_to(step):
        own = packed.at[rank, y]
        return remote(own, own, spin_send.at[0], spin_recv.at[rank], rank_device(lax.rem(rank + step, ranks)))

    def spin_arrived(source):
        target = packed.at[source, y]
        remote(target, target, spin_send.at[0], spin_recv.at[source], sibling).wait_recv()

    def hand_on(source, slot):
        for step in range(1, LINE):
            piece = packed.at[source, y]
            remote(
                piece, piece, pass_send.at[slot], pass_recv.at[source, y], line_device(lax.rem(y + step, LINE))
            ).start()

    def handed(source, step):
        from_y = lax.rem(y + step, LINE)
        target = packed.at[source, from_y]
        remote(target, target, pass_send.at[0], pass_recv.at[source, from_y], sibling).wait_recv()
        return source, from_y

    masks = jnp.left_shift(1, lax.broadcasted_iota(jnp.int32, (32, quarter), 0))

    def places(pieces):
        return [pl.ds(pl.multiple_of(source * here + at * quarter, quarter), quarter) for source, at in pieces]

    def unpack(pieces):
        cols = places(pieces)
        for which, (source, at) in enumerate(pieces):
            to = slice(which * quarter, (which + 1) * quarter)
            for word in range(words):
                bits = jnp.bitwise_and(jnp.broadcast_to(packed[source, at, word : word + 1, :], (32, quarter)), masks)
                tile[word * 32 : word * 32 + 32, to] = jnp.where(bits != 0, 1.0, -1.0).astype(BF16)
        for to in range(SETS):
            word = (to % 2) * 2 * depth + 4 * rank + 2 * (to // 2 % 2) + to // 4
            from_rows = pl.ds(pl.multiple_of(word * rows, rows), rows)
            for which in range(2):
                spins[to * rows : (to + 1) * rows, cols[which]] = tile[
                    from_rows, which * quarter : (which + 1) * quarter
                ]

    def activate(pieces):
        cols = places(pieces)
        for unit in range(0, units, 512):
            these = pl.ds(unit, 512)
            pre = jnp.dot(weight_t[these, :], tile[...], preferred_element_type=F32)
            pre = pre + jnp.concatenate([bias_t[these, :]] * (2 * quarter // 128), axis=1)
            result = jnp.tanh(pre).astype(BF16)
            for which in range(2):
                hidden[these, cols[which]] = result[:, which * quarter : (which + 1) * quarter]

    def hidden_of(*pieces):
        unpack(pieces)
        activate(pieces)

    first = (rank, 0), (rank, 1)
    spins[pair:, :] = (lax.broadcasted_iota(jnp.int32, (PAD, samples), 0) == 0).astype(F32).astype(BF16)
    unpack(first)
    with jax.named_scope("barrier"):
        pl.semaphore_wait(barrier, groups + ranks + 1)
    for at in range(parts):
        force_send_own(at, 1, x_partner)
    for step in (1, ranks - 1, 2):
        spin_send_to(step).start()
    for at in range(parts):
        force_send_own(at, 0, z_partner)

    with jax.named_scope("hidden0"):
        activate(first)
        hidden_of((rank, 2), (rank, 3))
    with jax.named_scope("spinab"):
        spin_arrived(before)
        hand_on(before, 0)
        spin_arrived(after)
        hand_on(after, 1)
    with jax.named_scope("hidden1"):
        hidden_of((before, y), (after, y))
    with jax.named_scope("spin1"):
        pieces = handed(before, 1), handed(after, 1)
    with jax.named_scope("hidden2"):
        hidden_of(*pieces)
    with jax.named_scope("spinc"):
        spin_arrived(across)
        hand_on(across, 2)
        for at in range(parts):
            force_x(at)
        pieces = (across, y), handed(before, 3)
    with jax.named_scope("hidden3"):
        hidden_of(*pieces)
    for step, ((source_a, from_a), (source_b, from_b)) in enumerate(
        (((after, 3), (before, 2)), ((after, 2), (across, 1)), ((across, 3), (across, 2)))
    ):
        with jax.named_scope("wait"):
            if step >= 1:
                force_z(2 * step - 2)
                force_z(2 * step - 1)
            pieces = handed(source_a, from_a), handed(source_b, from_b)
        with jax.named_scope("hidden4"):
            hidden_of(*pieces)

    span = samples // 2
    by_group, by_rank = (by_group_a, by_group_b), (by_rank_a, by_rank_b)

    def fill_lhs(at, slots, row):
        for to in range(SETS):
            lhs[to * rows : (to + 1) * rows, cols_of(at)] = slots[at, to // 4, to // 2 % 2, to % 2].astype(BF16)
        lhs[pair:, cols_of(at)] = jnp.concatenate(
            [row[:, cols_of(at)] / ranks, jnp.zeros((PAD - 1, PART), F32)], axis=0
        ).astype(BF16)

    def values_of(which, first, last, side, fresh):
        these, cols = slice(first * PART, last * PART), slice(side * span, (side + 1) * span)
        product = jnp.dot(lhs[:, these], hidden[these, cols], preferred_element_type=F32)
        value = jnp.sum(product[:pair] * spins[:pair, cols].astype(F32), axis=0, keepdims=True) + product[pair : pair + 1]
        mine = by_group[side].at[which, grp, :, :span]
        mine[...] = value if fresh else mine[...] + value

    with jax.named_scope("forcew"):
        for at in range(parts):
            force_whole(at)
            fill_lhs(at, force_all, force_b_ref)
    def gather(slots, which, size, me, peer):
        send, recv = gather_send.at[which], gather_recv.at[which]
        for step in range(1, size):
            remote(slots.at[me], slots.at[me], send, recv, peer(lax.rem(me + step, size))).start()
        others = slots.at[pl.ds(0, size - 1)]

        def finish():
            remote(others, others, send, recv, sibling).wait()

        return finish

    def wide(x, lanes=128):
        return jnp.broadcast_to(x, (1, lanes))

    def send_groups(which, side):
        return gather(by_group[side].at[which], 2 * which + side, groups, grp, group_device)

    def send_ranks(which, side):
        mine = by_group[side][which, 0]
        for source in range(1, groups):
            mine = mine + by_group[side][which, source]
        by_rank[side][which, rank] = mine
        return gather(by_rank[side].at[which], 4 + 2 * which + side, ranks, rank, rank_device)

    def sum_ranks(which, side):
        whole = by_rank[side][which, 0]
        for source in range(1, ranks):
            whole = whole + by_rank[side][which, source]
        return whole

    def gather_sets(which, values):
        fill = jnp.zeros((8 - len(values), 128), F32)
        by_set[which, member] = jnp.concatenate([wide(value) for value in values] + [fill], axis=0)
        return gather(by_set.at[which], 8 + which, SETS, member, set_device)

    def set_sum(which, row):
        value = by_set[which, 0, row : row + 1, :]
        for source in range(1, SETS):
            value = value + by_set[which, source, row : row + 1, :]
        return value[:, :1]

    def own_force(at):
        return force_all[at, core, parity, half]

    force_dot = total(force_b_ref[...] * force_b_ref[...]) / shards
    for at in range(parts):
        force_dot = force_dot + total(own_force(at) * own_force(at))
    def of_hidden(left, at):
        return lax.dot_general(
            left[...], hidden[cols_ds(at), :], (((1,), (1,)), ((), ())), preferred_element_type=F32
        )

    def extras(which, first, second):
        by_group[1][which, grp, :, span:] = jnp.concatenate([wide(first), wide(second)], axis=1)

    def own_sum(side):
        return total(by_group[side][0, grp, :, :span])

    with jax.named_scope("values0"):
        values_of(0, 0, parts, 0, True)
        finish_a = send_groups(0, 0)
        extras(0, force_dot, jnp.zeros((1, 1), F32))
        values_of(0, 0, parts, 1, True)
        finish_b = send_groups(0, 1)
    with jax.named_scope("redg"):
        by_shard[smp] = wide(own_sum(0) + own_sum(1))
        finish_shards = gather(by_shard, 12, shards, smp, shard_device)

        def plain_part(at, carry):
            plain[at] = of_hidden(spins, at)
            return carry

        lax.fori_loop(0, parts, plain_part, 0)
        finish_a()
        finish_ranks_a = send_ranks(0, 0)
        finish_b()
        finish_ranks_b = send_ranks(0, 1)
    with jax.named_scope("shards"):
        finish_shards()
        mine = by_shard[0]
        for source in range(1, shards):
            mine = mine + by_shard[source]
        by_total[grp] = mine
        finish_total = gather(by_total, 13, groups, grp, group_device)
    with jax.named_scope("redr"):
        finish_ranks_a()
        finish_ranks_b()
        sums = [sum_ranks(0, side) for side in range(2)]
        own_dot = sums[1][:, span : span + 1]
        mean_own = (total(sums[0][:, :span]) + total(sums[1][:, :span])) / samples
        centred = [whole[:, :span] - mean_own for whole in sums]
    with jax.named_scope("scaled"):
        for at in range(0, samples, 512):
            weights = centred[at // span][:, at % span : at % span + 512]
            scaled[:pair, at : at + 512] = (spins[:pair, at : at + 512].astype(F32) * weights).astype(BF16)
            scaled[pair:, at : at + 512] = jnp.concatenate(
                [weights, jnp.zeros((PAD - 1, 512), F32)], axis=0
            ).astype(BF16)

    def outer(at):
        return (x_partner, z_partner, half) if at % 2 == 0 else (z_partner, x_partner, parity)

    def pick(ref, at, which):
        return ref.at[:, which] if at % 2 == 0 else ref.at[which]

    def core_copy(at):
        return remote(image.at[at, 1 - core], image_core.at[at], image_send.at[0], image_recv.at[at, 0], sibling)

    def image_copy(at, which):
        far, near, place = outer(at)
        ours = pick(image_all.at[at, core], at, place)
        theirs = pick(image_all.at[at, core], at, 1 - place)
        source, target, where = (
            None,
            (pick(image.at[at, core], at, 1 - place), image_z.at[at], far),
            (pick(image.at[at, core], at, place), image_x.at[at], near),
            (ours, ours, far),
            (ours, ours, sibling),
            (theirs, theirs, sibling),
        )[which]
        return remote(source, target, image_send.at[which], image_recv.at[at, which], where)

    def image_arrived(at, which):
        place = outer(at)[2]
        target = (
            image_core.at[at], image_z.at[at], image_x.at[at],
            pick(image_all.at[at, core], at, 1 - place),
            pick(image_all.at[at, 1 - core], at, place),
            pick(image_all.at[at, 1 - core], at, 1 - place),
        )[which]
        remote(target, target, image_send.at[which], image_recv.at[at, which], sibling).wait_recv()

    def image_part(at, carry):
        part = of_hidden(scaled, at)
        for to in range(SETS):
            image[at, to // 4, to // 2 % 2, to % 2] = part[to * rows : (to + 1) * rows]
        image_b[member, :, cols_ds(at)] = part[pair : pair + 1]
        return carry

    def shifted(at):
        for to in range(SETS):
            block = image.at[at, to // 4, to // 2 % 2, to % 2]
            block[...] = block[...] + shift * plain[at, to * rows : (to + 1) * rows]
        core_copy(at).start()
        image_b[member, :, cols_ds(at)] = image_b[member, :, cols_ds(at)] + shift * plain[at, pair : pair + 1]

    def sum_core(at):
        place = outer(at)[2]
        image_arrived(at, 0)
        theirs = pick(image.at[at, core], at, 1 - place)
        theirs[...] = theirs[...] + pick(image_core.at[at], at, 1 - place)[...]
        image_copy(at, 1).start()
        ours = pick(image.at[at, core], at, place)
        ours[...] = ours[...] + pick(image_core.at[at], at, place)[...]

    def sum_outer(at):
        image_arrived(at, 1)
        ours = pick(image.at[at, core], at, outer(at)[2])
        ours[...] = ours[...] + image_z[at]
        image_copy(at, 2).start()

    def sum_inner(at):
        image_arrived(at, 2)
        place = outer(at)[2]
        pick(image_all.at[at, core], at, place)[...] = pick(image.at[at, core], at, place)[...] + image_x[at]
        image_copy(at, 3).start()
        image_copy(at, 4).start()

    def share(at):
        image_arrived(at, 3)
        image_copy(at, 5).start()

    def image_values(at, fresh, *sides):
        image_arrived(at, 4)
        image_arrived(at, 5)
        fill_lhs(at, image_all, image_b[0])
        for side in sides:
            values_of(1, at, at + 1, side, fresh)

    def named(name, step, *at):
        with jax.named_scope(name):
            step(*at)

    with jax.named_scope("image"):
        lax.fori_loop(0, 2, image_part, 0)
    with jax.named_scope("mean"):
        finish_total()
        mean0 = by_total[0]
        for source in range(1, groups):
            mean0 = mean0 + by_total[source]
        shift = mean_own - mean0[:, :1] / count
        shifted(0)
        shifted(1)
        moment = total(centred[0] * centred[0]) + total(centred[1] * centred[1]) + samples * shift * shift
        finish_moment = gather_sets(0, [moment, own_dot])

    def image_step(at, carry):
        image_part(at, 0)
        shifted(at)

        @pl.when(at == 2)
        def _():
            sum_core(0)
            sum_core(1)

        return carry

    with jax.named_scope("image"):
        lax.fori_loop(2, parts, image_step, 0)
    finish_bias = gather(image_b, 11, SETS, member, set_device)
    named("core", sum_core, 2)
    named("core", sum_core, 3)
    named("outer", sum_outer, 1)
    named("outer", sum_outer, 0)
    named("outer", sum_outer, 2)
    named("outer", sum_outer, 3)
    with jax.named_scope("bias"):
        finish_moment()
        finish_bias()
        norm0 = set_sum(0, 1)
        step0 = norm0 / (set_sum(0, 0) / count + diag_shift * norm0)
        keep = 1.0 - diag_shift * step0
        pull = step0 / count
        whole_b = image_b[0]
        for source in range(1, SETS):
            whole_b = whole_b + image_b[source]
        image_b[0] = whole_b
    named("inner", sum_inner, 0)
    named("inner", sum_inner, 1)
    named("inner", sum_inner, 2)
    named("inner", sum_inner, 3)
    with jax.named_scope("norm"):
        residual_b = keep * force_b_ref[...] - pull * whole_b
        own_norm = total(residual_b * residual_b) / shards
        own_cross = total(residual_b * force_b_ref[...]) / shards
        image_b_ref[0:1, :] = whole_b
        image_b_ref[1:2, :] = force_b_ref[...]
        for at in range(parts):
            force, own = own_force(at), image_all[at, core, parity, half]
            residual = keep * force - pull * own
            own_norm = own_norm + total(residual * residual)
            own_cross = own_cross + total(residual * force)
            image_ref[:, cols_of(at)] = own
            own_ref[:, cols_of(at)] = force
        finish_norm = gather_sets(1, [own_norm, own_cross])
    named("share", share, 1)
    named("share", share, 0)
    named("values1", image_values, 1, True, 0, 1)
    named("share", share, 2)
    named("values1", image_values, 0, False, 0, 1)
    named("share", share, 3)
    named("values1", image_values, 2, False, 0, 1)
    named("fnorm", finish_norm)
    extras(1, set_sum(1, 0), set_sum(1, 1))
    with jax.named_scope("values1"):
        image_values(3, False, 0)
        finish_a = send_groups(1, 0)
        values_of(1, 3, 4, 1, False)
        finish_b = send_groups(1, 1)
    with jax.named_scope("redg"):
        finish_a()
        finish_ranks_a = send_ranks(1, 0)
        finish_b()
        finish_ranks_b = send_ranks(1, 1)
    with jax.named_scope("redr"):
        finish_ranks_a()
        finish_ranks_b()
        sums = [sum_ranks(1, side) for side in range(2)]
        norm1, cross = sums[1][:, span : span + 1], sums[1][:, span + 128 : span + 129]
    beta = norm1 / norm0
    with jax.named_scope("sets"):
        values1 = [(keep + beta) * (centred[side] + shift) - pull * sums[side][:, :span] for side in range(2)]
        mean1 = (total(values1[0]) + total(values1[1])) / samples
        values1 = [value - mean1 for value in values1]
        gather_sets(2, [mean1, total(values1[0] * values1[0]) + total(values1[1] * values1[1])])()
        middle = set_sum(2, 0) / SETS
        spread = jnp.zeros((1, 1), F32)
        for source in range(SETS):
            shift = by_set[2, source, 0:1, :1] - middle
            spread = spread + shift * shift
        variance1 = (set_sum(2, 1) + samples * spread) / count
    direction_dot = norm1 + 2.0 * beta * cross + beta * beta * norm0
    step1 = norm1 / (variance1 + diag_shift * direction_dot)

    for_force = step0 + step1 * (keep + beta)
    for_image = step1 * pull
    scale_ref[...] = jnp.concatenate([wide(for_force), wide(for_image), jnp.zeros((6, 128), F32)], axis=0)
    with jax.named_scope("out"):
        pieces = packed.at[rank, pl.ds(0, LINE - 1)]
        remote(pieces, pieces, spin_send.at[0], spin_recv.at[0], sibling).wait_send()
        for slot in range(3):
            remote(pieces, pieces, pass_send.at[slot], spin_recv.at[0], sibling).wait_send()
        for which in range(5):
            blocks = force_all.at[:, core, parity] if which > 2 else force_all.at[:, core, parity, half]
            remote(blocks, blocks, force_send.at[which], spin_recv.at[0], sibling).wait_send()
        for which in range(6):
            blocks = image_core if which == 0 else image_z
            remote(blocks, blocks, image_send.at[which], spin_recv.at[0], sibling).wait_send()


def finish_kernel(image_ref, image_b_ref, force_ref, scale_ref, out_ref, out_b_ref):
    for_force, for_image = scale_ref[0:1, 0:1], scale_ref[1:2, 0:1]
    out_ref[...] = for_force * force_ref[...] - for_image * image_ref[...]
    out_b_ref[...] = for_force * image_b_ref[1:2, :] - for_image * image_b_ref[0:1, :]


def body(groups, shards, spins_packed, weight, hidden_bias, force_w, force_b):
    words, here = spins_packed.shape
    inputs, units = weight.shape
    rows = force_w.shape[0]
    ranks = shards // SETS
    samples, pair = ranks * here, SETS * rows
    parts = units // PART
    quarter = here // LINE
    vmem = pl.BlockSpec(memory_space=pltpu.VMEM)
    anywhere = pl.BlockSpec(memory_space=pl.ANY)
    dma = pltpu.SemaphoreType.DMA
    results = pl.pallas_call(
        functools.partial(kernel, groups, shards),
        out_shape=(
            pltpu.VMEM((rows, units), F32), pltpu.VMEM((8, units), F32),
            pltpu.VMEM((rows, units), F32), pltpu.VMEM((8, 128), F32),
        ),
        in_specs=[anywhere] * 5,
        out_specs=(vmem,) * 4,
        scratch_shapes=[
            pltpu.VMEM((ranks, LINE, words, quarter), jnp.int32),
            pltpu.VMEM((inputs, units), BF16),
            pltpu.VMEM((units, inputs), BF16),
            pltpu.VMEM((1, units), F32),
            pltpu.VMEM((units, 128), F32),
            pltpu.VMEM((1, units), F32),
            pltpu.VMEM((inputs, 2 * quarter), BF16),
            pltpu.VMEM((pair + PAD, samples), BF16),
            pltpu.VMEM((units, samples), BF16),
            pltpu.VMEM((parts, 2, 2, 2, rows, PART), F32),
            pltpu.VMEM((pair + PAD, units), BF16),
            pltpu.VMEM((pair + PAD, samples), BF16),
            pltpu.VMEM((parts, pair + PAD, PART), F32),
            pltpu.VMEM((parts, 2, 2, 2, rows, PART), F32),
            pltpu.VMEM((parts, 2, 2, rows, PART), F32),
            pltpu.VMEM((parts, 2, rows, PART), F32),
            pltpu.VMEM((parts, 2, rows, PART), F32),
            pltpu.VMEM((parts, 2, 2, 2, rows, PART), F32),
            pltpu.VMEM((SETS, 1, units), F32),
            pltpu.VMEM((2, groups, 1, samples // 2), F32),
            pltpu.VMEM((2, groups, 1, samples // 2 + EXTRA), F32),
            pltpu.VMEM((2, ranks, 1, samples // 2), F32),
            pltpu.VMEM((2, ranks, 1, samples // 2 + EXTRA), F32),
            pltpu.VMEM((3, SETS, 8, 128), F32),
            pltpu.VMEM((shards, 1, 128), F32),
            pltpu.VMEM((groups, 1, 128), F32),
            dma((5,)),
            dma((1,)),
            dma((ranks,)),
            dma((3,)),
            dma((ranks, LINE)),
            dma((5,)),
            dma((parts, 5)),
            dma((6,)),
            dma((parts, 6)),
            dma((14,)),
            dma((14,)),
        ],
        compiler_params=pltpu.CompilerParams(
            collective_id=0, has_side_effects=True, vmem_limit_bytes=62 * 1024 * 1024
        ),
    )(spins_packed, weight, hidden_bias.reshape(1, -1), force_w, force_b.reshape(1, -1))
    update_w, update_b = pl.pallas_call(
        finish_kernel,
        out_shape=(jax.ShapeDtypeStruct((rows, units), F32), jax.ShapeDtypeStruct((1, units), F32)),
        in_specs=[vmem] * 4,
        out_specs=(vmem, vmem),
    )(*[pltpu.with_memory_space_constraint(result, pltpu.VMEM) for result in results])
    return update_w, update_b.reshape(-1)


def solution(mesh):
    placed = (P(None, "smp"), P(None, "grp"), P("grp"), P("smp", "grp"), P("grp"))
    return jax.shard_map(
        functools.partial(body, mesh.shape["grp"], mesh.shape["smp"]),
        mesh=mesh, in_specs=placed, out_specs=(P("smp", "grp"), P("grp")), check_vma=False,
    )
```

```python
import functools

import jax
import jax.numpy as jnp
from jax import lax
from jax.experimental import pallas as pl
from jax.experimental.pallas import tpu as pltpu
from jax.sharding import PartitionSpec as P

MESH = pl.DeviceIdType.MESH
F32, BF16 = jnp.float32, jnp.bfloat16
diag_shift = 0.01
SETS = 8
EXTRA = 256
PAD = 16
PART = 256
LINE = 4


def total(x):
    return jnp.sum(jnp.sum(x, axis=0, keepdims=True), axis=1, keepdims=True)


def kernel(
    groups, shards,
    packed_in, weight_in, bias_in, force_in, force_b_in,
    image_ref, image_b_ref, own_ref, scale_ref,
    packed, weight, weight_t, bias_ref, bias_t, force_b_ref, tile, spins, hidden, force_all, lhs, scaled, plain,
    image, image_core, image_z, image_x, image_all, image_b, by_group_a, by_group_b, by_rank_a, by_rank_b, by_set, by_shard, by_total,
    load, spin_send, spin_recv, pass_send, pass_recv, force_send, force_recv, image_send, image_recv,
    gather_send, gather_recv,
):
    grp, smp = lax.axis_index("grp"), lax.axis_index("smp")
    words, here = packed_in.shape
    inputs, units = weight.shape
    rows = force_in.shape[0]
    ranks = shards // SETS
    pair = SETS * rows
    samples = ranks * here
    count = samples * SETS
    quarter = here // LINE
    parts = units // PART
    depth = 2 * ranks

    core, z, half = lax.rem(smp, 2), lax.rem(smp // 2, depth), smp // (2 * depth)
    parity, rank = lax.rem(z, 2), z // 2
    member = (core * 2 + parity) * 2 + half
    y, column = lax.rem(grp, LINE), grp // LINE

    def device(half_at, z_at, core_at):
        return {"smp": (half_at * depth + z_at) * 2 + core_at}

    sibling = device(half, z, 1 - core)
    z_partner = device(half, z + 1 - 2 * parity, core)
    x_partner = device(1 - half, z, core)

    def group_device(at):
        return {"grp": at}

    def line_device(at):
        return {"grp": column * LINE + at}

    def rank_device(at):
        return device(half, 2 * at + parity, core)

    def set_device(at):
        return device(lax.rem(at, 2), 2 * rank + lax.rem(at // 2, 2), at // 4)

    def shard_device(at):
        return {"smp": at}

    def remote(source, target, send, recv, where):
        return pltpu.make_async_remote_copy(
            source, target, send, recv, device_id=where, device_id_type=MESH
        )

    barrier = pltpu.get_barrier_semaphore()
    for size, me, peer in ((groups, grp, group_device), (ranks, rank, rank_device)):
        for step in range(1, size):
            pl.semaphore_signal(barrier, device_id=peer(lax.rem(me + step, size)), device_id_type=MESH)
    for where in (sibling, z_partner, x_partner):
        pl.semaphore_signal(barrier, device_id=where, device_id_type=MESH)

    def cols_of(at):
        return slice(at * PART, (at + 1) * PART)

    def cols_ds(at):
        return pl.ds(pl.multiple_of(at * PART, PART), PART)

    copies = []
    for at in range(LINE):
        copies.append(
            pltpu.make_async_copy(packed_in.at[:, pl.ds(at * quarter, quarter)], packed.at[rank, at], load.at[3])
        )
    for at in range(parts):
        copies.append(
            pltpu.make_async_copy(force_in.at[:, cols_ds(at)], force_all.at[at, core, parity, half], load.at[4])
        )
    later = [
        pltpu.make_async_copy(weight_in, weight, load.at[0]),
        pltpu.make_async_copy(bias_in, bias_ref, load.at[1]),
        pltpu.make_async_copy(force_b_in, force_b_ref, load.at[2]),
    ]
    for copy in copies + later:
        copy.start()
    pltpu.make_async_copy(packed.at[rank], packed.at[rank], load.at[3]).wait()
    blocks = force_all.at[:, core, parity, half]
    pltpu.make_async_copy(blocks, blocks, load.at[4]).wait()

    def turn(at, carry):
        cols = pl.ds(pl.multiple_of(at * 256, 256), 256)
        weight_t[cols, :] = weight[:, cols].T
        bias_t[cols, :] = jnp.broadcast_to(bias_ref[:, cols], (128, 256)).T
        return carry

    after, before, across = lax.rem(rank + 1, ranks), lax.rem(rank + ranks - 1, ranks), lax.rem(rank + 2, ranks)

    def force_send_own(at, which, where):
        own = force_all.at[at, core, parity, half]
        remote(own, own, force_send.at[which], force_recv.at[at, which], where).start()

    def force_arrived(at, which):
        target = (
            force_all.at[at, core, 1 - parity, half],
            force_all.at[at, core, parity, 1 - half],
            force_all.at[at, core, 1 - parity, 1 - half],
            force_all.at[at, 1 - core, parity],
            force_all.at[at, 1 - core, 1 - parity],
        )[which]
        remote(target, target, force_send.at[which], force_recv.at[at, which], sibling).wait_recv()

    def force_x(at):
        force_arrived(at, 1)
        block_x = force_all.at[at, core, parity, 1 - half]
        remote(block_x, block_x, force_send.at[2], force_recv.at[at, 2], z_partner).start()
        ours = force_all.at[at, core, parity]
        remote(ours, ours, force_send.at[3], force_recv.at[at, 3], sibling).start()

    def force_z(at):
        force_arrived(at, 0)
        force_arrived(at, 2)
        theirs = force_all.at[at, core, 1 - parity]
        remote(theirs, theirs, force_send.at[4], force_recv.at[at, 4], sibling).start()

    def force_whole(at):
        force_arrived(at, 3)
        force_arrived(at, 4)

    def spin_send_to(step):
        own = packed.at[rank, y]
        return remote(own, own, spin_send.at[0], spin_recv.at[rank], rank_device(lax.rem(rank + step, ranks)))

    def spin_arrived(source):
        target = packed.at[source, y]
        remote(target, target, spin_send.at[0], spin_recv.at[source], sibling).wait_recv()

    def hand_on(source, slot):
        for step in (1, 3, 2):
            piece = packed.at[source, y]
            remote(
                piece, piece, pass_send.at[slot], pass_recv.at[source, y], line_device(lax.rem(y + step, LINE))
            ).start()

    def handed(source, step):
        from_y = lax.rem(y + step, LINE)
        target = packed.at[source, from_y]
        remote(target, target, pass_send.at[0], pass_recv.at[source, from_y], sibling).wait_recv()
        return source, from_y

    masks = jnp.left_shift(1, lax.broadcasted_iota(jnp.int32, (32, quarter), 0))

    def places(pieces):
        return [pl.ds(pl.multiple_of(source * here + at * quarter, quarter), quarter) for source, at in pieces]

    def unpack(pieces):
        cols = places(pieces)
        for which, (source, at) in enumerate(pieces):
            to = slice(which * quarter, (which + 1) * quarter)
            for word in range(words):
                bits = jnp.bitwise_and(jnp.broadcast_to(packed[source, at, word : word + 1, :], (32, quarter)), masks)
                tile[word * 32 : word * 32 + 32, to] = jnp.where(bits != 0, 1.0, -1.0).astype(BF16)
        for to in range(SETS):
            word = (to % 2) * 2 * depth + 4 * rank + 2 * (to // 2 % 2) + to // 4
            from_rows = pl.ds(pl.multiple_of(word * rows, rows), rows)
            for which in range(2):
                spins[to * rows : (to + 1) * rows, cols[which]] = tile[
                    from_rows, which * quarter : (which + 1) * quarter
                ]

    def activate(pieces):
        cols = places(pieces)
        for unit in range(0, units, 1024):
            these = pl.ds(unit, 1024)
            pre = jnp.dot(weight_t[these, :], tile[...], preferred_element_type=F32)
            pre = pre + jnp.concatenate([bias_t[these, :]] * (2 * quarter // 128), axis=1)
            result = jnp.tanh(pre).astype(BF16)
            for which in range(2):
                hidden[these, cols[which]] = result[:, which * quarter : (which + 1) * quarter]

    def hidden_of(*pieces):
        unpack(pieces)
        activate(pieces)

    with jax.named_scope("barrier"):
        pl.semaphore_wait(barrier, groups + ranks + 1)
    for at in range(parts):
        force_send_own(at, 1, x_partner)
    for step in (1, ranks - 1, 2):
        spin_send_to(step).start()
    for at in range(parts):
        force_send_own(at, 0, z_partner)

    spins[pair:, :] = (lax.broadcasted_iota(jnp.int32, (PAD, samples), 0) == 0).astype(F32).astype(BF16)
    with jax.named_scope("turn"):
        for copy in later:
            copy.wait()
        lax.fori_loop(0, units // 256, turn, 0)
    with jax.named_scope("hidden0"):
        hidden_of((rank, 0), (rank, 1))
        hidden_of((rank, 2), (rank, 3))
    with jax.named_scope("spinab"):
        spin_arrived(before)
        hand_on(before, 0)
        spin_arrived(after)
        hand_on(after, 1)
    with jax.named_scope("hidden1"):
        hidden_of((before, y), (after, y))
    with jax.named_scope("spinc"):
        spin_arrived(across)
        hand_on(across, 2)
        for at in range(parts):
            force_x(at)
        pieces = (across, y), handed(before, 1)
    with jax.named_scope("hidden2"):
        hidden_of(*pieces)
    with jax.named_scope("wait"):
        pieces = handed(before, 3), handed(after, 1), handed(after, 3), handed(before, 2)
    with jax.named_scope("hidden3"):
        hidden_of(*pieces[:2])
        hidden_of(*pieces[2:])
    with jax.named_scope("wait"):
        for at in range(parts):
            force_z(at)
        pieces = handed(after, 2), handed(across, 1), handed(across, 3), handed(across, 2)
    with jax.named_scope("hidden4"):
        hidden_of(*pieces[:2])
        hidden_of(*pieces[2:])

    span = samples // 2
    by_group, by_rank = (by_group_a, by_group_b), (by_rank_a, by_rank_b)

    def fill_lhs(at, slots, row):
        for to in range(SETS):
            lhs[to * rows : (to + 1) * rows, cols_of(at)] = slots[at, to // 4, to // 2 % 2, to % 2].astype(BF16)
        lhs[pair:, cols_of(at)] = jnp.concatenate(
            [row[:, cols_of(at)] / ranks, jnp.zeros((PAD - 1, PART), F32)], axis=0
        ).astype(BF16)

    def values_of(which, first, last, side, fresh):
        these, cols = slice(first * PART, last * PART), slice(side * span, (side + 1) * span)
        product = jnp.dot(lhs[:, these], hidden[these, cols], preferred_element_type=F32)
        value = jnp.sum(product[:pair] * spins[:pair, cols].astype(F32), axis=0, keepdims=True) + product[pair : pair + 1]
        mine = by_group[side].at[which, grp, :, :span]
        mine[...] = value if fresh else mine[...] + value

    with jax.named_scope("forcew"):
        for at in range(parts):
            force_whole(at)
            fill_lhs(at, force_all, force_b_ref)
    def gather(slots, which, size, me, peer):
        send, recv = gather_send.at[which], gather_recv.at[which]
        for step in range(1, size):
            remote(slots.at[me], slots.at[me], send, recv, peer(lax.rem(me + step, size))).start()
        others = slots.at[pl.ds(0, size - 1)]

        def finish():
            remote(others, others, send, recv, sibling).wait()

        return finish

    def wide(x, lanes=128):
        return jnp.broadcast_to(x, (1, lanes))

    def send_groups(which, side):
        return gather(by_group[side].at[which], 2 * which + side, groups, grp, group_device)

    def send_ranks(which, side):
        mine = by_group[side][which, 0]
        for source in range(1, groups):
            mine = mine + by_group[side][which, source]
        by_rank[side][which, rank] = mine
        return gather(by_rank[side].at[which], 4 + 2 * which + side, ranks, rank, rank_device)

    def sum_ranks(which, side):
        whole = by_rank[side][which, 0]
        for source in range(1, ranks):
            whole = whole + by_rank[side][which, source]
        return whole

    def gather_sets(which, values):
        fill = jnp.zeros((8 - len(values), 128), F32)
        by_set[which, member] = jnp.concatenate([wide(value) for value in values] + [fill], axis=0)
        return gather(by_set.at[which], 8 + which, SETS, member, set_device)

    def set_sum(which, row):
        value = by_set[which, 0, row : row + 1, :]
        for source in range(1, SETS):
            value = value + by_set[which, source, row : row + 1, :]
        return value[:, :1]

    def own_force(at):
        return force_all[at, core, parity, half]

    force_dot = total(force_b_ref[...] * force_b_ref[...]) / shards
    for at in range(parts):
        force_dot = force_dot + total(own_force(at) * own_force(at))
    def of_hidden(left, at):
        return lax.dot_general(
            left[...], hidden[cols_ds(at), :], (((1,), (1,)), ((), ())), preferred_element_type=F32
        )

    def extras(which, first, second):
        by_group[1][which, grp, :, span:] = jnp.concatenate([wide(first), wide(second)], axis=1)

    def own_sum(side):
        return total(by_group[side][0, grp, :, :span])

    with jax.named_scope("values0"):
        values_of(0, 0, parts, 0, True)
        finish_a = send_groups(0, 0)
        extras(0, force_dot, jnp.zeros((1, 1), F32))
        values_of(0, 0, parts, 1, True)
        finish_b = send_groups(0, 1)
    with jax.named_scope("redg"):
        by_shard[smp] = wide(own_sum(0) + own_sum(1))
        finish_shards = gather(by_shard, 12, shards, smp, shard_device)

        def plain_part(at, carry):
            plain[at] = of_hidden(spins, at)
            return carry

        lax.fori_loop(0, parts, plain_part, 0)
        finish_a()
        finish_ranks_a = send_ranks(0, 0)
        finish_b()
        finish_ranks_b = send_ranks(0, 1)
    with jax.named_scope("shards"):
        finish_shards()
        mine = by_shard[0]
        for source in range(1, shards):
            mine = mine + by_shard[source]
        by_total[grp] = mine
        finish_total = gather(by_total, 13, groups, grp, group_device)
    with jax.named_scope("redr"):
        finish_ranks_a()
        finish_ranks_b()
        sums = [sum_ranks(0, side) for side in range(2)]
        own_dot = sums[1][:, span : span + 1]
        mean_own = (total(sums[0][:, :span]) + total(sums[1][:, :span])) / samples
        centred = [whole[:, :span] - mean_own for whole in sums]
    with jax.named_scope("scaled"):
        for at in range(0, samples, 512):
            weights = centred[at // span][:, at % span : at % span + 512]
            scaled[:pair, at : at + 512] = (spins[:pair, at : at + 512].astype(F32) * weights).astype(BF16)
            scaled[pair:, at : at + 512] = jnp.concatenate(
                [weights, jnp.zeros((PAD - 1, 512), F32)], axis=0
            ).astype(BF16)

    def outer(at):
        return (x_partner, z_partner, half) if at % 2 == 0 else (z_partner, x_partner, parity)

    def pick(ref, at, which):
        return ref.at[:, which] if at % 2 == 0 else ref.at[which]

    def core_copy(at):
        return remote(image.at[at, 1 - core], image_core.at[at], image_send.at[0], image_recv.at[at, 0], sibling)

    def image_copy(at, which):
        far, near, place = outer(at)
        ours = pick(image_all.at[at, core], at, place)
        theirs = pick(image_all.at[at, core], at, 1 - place)
        source, target, where = (
            None,
            (pick(image.at[at, core], at, 1 - place), image_z.at[at], far),
            (pick(image.at[at, core], at, place), image_x.at[at], near),
            (ours, ours, far),
            (ours, ours, sibling),
            (theirs, theirs, sibling),
        )[which]
        return remote(source, target, image_send.at[which], image_recv.at[at, which], where)

    def image_arrived(at, which):
        place = outer(at)[2]
        target = (
            image_core.at[at], image_z.at[at], image_x.at[at],
            pick(image_all.at[at, core], at, 1 - place),
            pick(image_all.at[at, 1 - core], at, place),
            pick(image_all.at[at, 1 - core], at, 1 - place),
        )[which]
        remote(target, target, image_send.at[which], image_recv.at[at, which], sibling).wait_recv()

    def image_part(at, carry):
        part = of_hidden(scaled, at)
        for to in range(SETS):
            image[at, to // 4, to // 2 % 2, to % 2] = part[to * rows : (to + 1) * rows]
        image_b[member, :, cols_ds(at)] = part[pair : pair + 1]
        return carry

    def shifted(at):
        for to in range(SETS):
            block = image.at[at, to // 4, to // 2 % 2, to % 2]
            block[...] = block[...] + shift * plain[at, to * rows : (to + 1) * rows]
        core_copy(at).start()
        image_b[member, :, cols_ds(at)] = image_b[member, :, cols_ds(at)] + shift * plain[at, pair : pair + 1]

    def sum_core(at):
        place = outer(at)[2]
        image_arrived(at, 0)
        theirs = pick(image.at[at, core], at, 1 - place)
        theirs[...] = theirs[...] + pick(image_core.at[at], at, 1 - place)[...]
        image_copy(at, 1).start()
        ours = pick(image.at[at, core], at, place)
        ours[...] = ours[...] + pick(image_core.at[at], at, place)[...]

    def sum_outer(at):
        image_arrived(at, 1)
        ours = pick(image.at[at, core], at, outer(at)[2])
        ours[...] = ours[...] + image_z[at]
        image_copy(at, 2).start()

    def sum_inner(at):
        image_arrived(at, 2)
        place = outer(at)[2]
        pick(image_all.at[at, core], at, place)[...] = pick(image.at[at, core], at, place)[...] + image_x[at]
        image_copy(at, 3).start()
        image_copy(at, 4).start()

    def share(at):
        image_arrived(at, 3)
        image_copy(at, 5).start()

    def image_ready(at):
        image_arrived(at, 4)
        image_arrived(at, 5)
        fill_lhs(at, image_all, image_b[0])

    def named(name, step, *at):
        with jax.named_scope(name):
            step(*at)

    with jax.named_scope("image"):
        lax.fori_loop(0, 2, image_part, 0)
    with jax.named_scope("mean"):
        finish_total()
        mean0 = by_total[0]
        for source in range(1, groups):
            mean0 = mean0 + by_total[source]
        shift = mean_own - mean0[:, :1] / count
        shifted(0)
        shifted(1)
        moment = total(centred[0] * centred[0]) + total(centred[1] * centred[1]) + samples * shift * shift
        finish_moment = gather_sets(0, [moment, own_dot])

    def image_step(at, carry):
        image_part(at, 0)
        shifted(at)

        @pl.when(at == 2)
        def _():
            sum_core(0)
            sum_core(1)

        return carry

    with jax.named_scope("image"):
        lax.fori_loop(2, parts, image_step, 0)
    finish_bias = gather(image_b, 11, SETS, member, set_device)
    named("core", sum_core, 2)
    named("core", sum_core, 3)
    named("outer", sum_outer, 1)
    named("outer", sum_outer, 0)
    named("outer", sum_outer, 2)
    named("outer", sum_outer, 3)
    with jax.named_scope("bias"):
        finish_moment()
        finish_bias()
        norm0 = set_sum(0, 1)
        step0 = norm0 / (set_sum(0, 0) / count + diag_shift * norm0)
        keep = 1.0 - diag_shift * step0
        pull = step0 / count
        whole_b = image_b[0]
        for source in range(1, SETS):
            whole_b = whole_b + image_b[source]
        image_b[0] = whole_b
    named("inner", sum_inner, 0)
    named("inner", sum_inner, 1)
    named("inner", sum_inner, 2)
    named("inner", sum_inner, 3)
    with jax.named_scope("norm"):
        residual_b = keep * force_b_ref[...] - pull * whole_b
        own_norm = total(residual_b * residual_b) / shards
        own_cross = total(residual_b * force_b_ref[...]) / shards
        image_b_ref[0:1, :] = whole_b
        image_b_ref[1:2, :] = force_b_ref[...]
        for at in range(parts):
            force, own = own_force(at), image_all[at, core, parity, half]
            residual = keep * force - pull * own
            own_norm = own_norm + total(residual * residual)
            own_cross = own_cross + total(residual * force)
            image_ref[:, cols_of(at)] = own
            own_ref[:, cols_of(at)] = force
        finish_norm = gather_sets(1, [own_norm, own_cross])
    named("share", share, 1)
    named("share", share, 0)
    named("ready", image_ready, 1)
    named("share", share, 2)
    named("ready", image_ready, 0)
    with jax.named_scope("values1"):
        values_of(1, 0, 2, 0, True)
    named("share", share, 3)
    with jax.named_scope("values1"):
        values_of(1, 0, 2, 1, True)
    named("ready", image_ready, 2)
    named("ready", image_ready, 3)
    named("fnorm", finish_norm)
    extras(1, set_sum(1, 0), set_sum(1, 1))
    with jax.named_scope("values1"):
        values_of(1, 2, 4, 0, False)
        finish_a = send_groups(1, 0)
        values_of(1, 2, 4, 1, False)
        finish_b = send_groups(1, 1)
    with jax.named_scope("redg"):
        finish_a()
        finish_ranks_a = send_ranks(1, 0)
        finish_b()
        finish_ranks_b = send_ranks(1, 1)
    with jax.named_scope("redr"):
        finish_ranks_a()
        finish_ranks_b()
        sums = [sum_ranks(1, side) for side in range(2)]
        norm1, cross = sums[1][:, span : span + 1], sums[1][:, span + 128 : span + 129]
    beta = norm1 / norm0
    with jax.named_scope("sets"):
        values1 = [(keep + beta) * (centred[side] + shift) - pull * sums[side][:, :span] for side in range(2)]
        mean1 = (total(values1[0]) + total(values1[1])) / samples
        values1 = [value - mean1 for value in values1]
        gather_sets(2, [mean1, total(values1[0] * values1[0]) + total(values1[1] * values1[1])])()
        middle = set_sum(2, 0) / SETS
        spread = jnp.zeros((1, 1), F32)
        for source in range(SETS):
            shift = by_set[2, source, 0:1, :1] - middle
            spread = spread + shift * shift
        variance1 = (set_sum(2, 1) + samples * spread) / count
    direction_dot = norm1 + 2.0 * beta * cross + beta * beta * norm0
    step1 = norm1 / (variance1 + diag_shift * direction_dot)

    for_force = step0 + step1 * (keep + beta)
    for_image = step1 * pull
    scale_ref[...] = jnp.concatenate([wide(for_force), wide(for_image), jnp.zeros((6, 128), F32)], axis=0)
    with jax.named_scope("out"):
        pieces = packed.at[rank, pl.ds(0, LINE - 1)]
        remote(pieces, pieces, spin_send.at[0], spin_recv.at[0], sibling).wait_send()
        for slot in range(3):
            remote(pieces, pieces, pass_send.at[slot], spin_recv.at[0], sibling).wait_send()
        for which in range(5):
            blocks = force_all.at[:, core, parity] if which > 2 else force_all.at[:, core, parity, half]
            remote(blocks, blocks, force_send.at[which], spin_recv.at[0], sibling).wait_send()
        for which in range(6):
            blocks = image_core if which == 0 else image_z
            remote(blocks, blocks, image_send.at[which], spin_recv.at[0], sibling).wait_send()


def finish_kernel(image_ref, image_b_ref, force_ref, scale_ref, out_ref, out_b_ref):
    for_force, for_image = scale_ref[0:1, 0:1], scale_ref[1:2, 0:1]
    out_ref[...] = for_force * force_ref[...] - for_image * image_ref[...]
    out_b_ref[...] = for_force * image_b_ref[1:2, :] - for_image * image_b_ref[0:1, :]


def body(groups, shards, spins_packed, weight, hidden_bias, force_w, force_b):
    words, here = spins_packed.shape
    inputs, units = weight.shape
    rows = force_w.shape[0]
    ranks = shards // SETS
    samples, pair = ranks * here, SETS * rows
    parts = units // PART
    quarter = here // LINE
    vmem = pl.BlockSpec(memory_space=pltpu.VMEM)
    anywhere = pl.BlockSpec(memory_space=pl.ANY)
    dma = pltpu.SemaphoreType.DMA
    results = pl.pallas_call(
        functools.partial(kernel, groups, shards),
        out_shape=(
            pltpu.VMEM((rows, units), F32), pltpu.VMEM((8, units), F32),
            pltpu.VMEM((rows, units), F32), pltpu.VMEM((8, 128), F32),
        ),
        in_specs=[anywhere] * 5,
        out_specs=(vmem,) * 4,
        scratch_shapes=[
            pltpu.VMEM((ranks, LINE, words, quarter), jnp.int32),
            pltpu.VMEM((inputs, units), BF16),
            pltpu.VMEM((units, inputs), BF16),
            pltpu.VMEM((1, units), F32),
            pltpu.VMEM((units, 128), F32),
            pltpu.VMEM((1, units), F32),
            pltpu.VMEM((inputs, 2 * quarter), BF16),
            pltpu.VMEM((pair + PAD, samples), BF16),
            pltpu.VMEM((units, samples), BF16),
            pltpu.VMEM((parts, 2, 2, 2, rows, PART), F32),
            pltpu.VMEM((pair + PAD, units), BF16),
            pltpu.VMEM((pair + PAD, samples), BF16),
            pltpu.VMEM((parts, pair + PAD, PART), F32),
            pltpu.VMEM((parts, 2, 2, 2, rows, PART), F32),
            pltpu.VMEM((parts, 2, 2, rows, PART), F32),
            pltpu.VMEM((parts, 2, rows, PART), F32),
            pltpu.VMEM((parts, 2, rows, PART), F32),
            pltpu.VMEM((parts, 2, 2, 2, rows, PART), F32),
            pltpu.VMEM((SETS, 1, units), F32),
            pltpu.VMEM((2, groups, 1, samples // 2), F32),
            pltpu.VMEM((2, groups, 1, samples // 2 + EXTRA), F32),
            pltpu.VMEM((2, ranks, 1, samples // 2), F32),
            pltpu.VMEM((2, ranks, 1, samples // 2 + EXTRA), F32),
            pltpu.VMEM((3, SETS, 8, 128), F32),
            pltpu.VMEM((shards, 1, 128), F32),
            pltpu.VMEM((groups, 1, 128), F32),
            dma((5,)),
            dma((1,)),
            dma((ranks,)),
            dma((3,)),
            dma((ranks, LINE)),
            dma((5,)),
            dma((parts, 5)),
            dma((6,)),
            dma((parts, 6)),
            dma((14,)),
            dma((14,)),
        ],
        compiler_params=pltpu.CompilerParams(
            collective_id=0, has_side_effects=True, vmem_limit_bytes=62 * 1024 * 1024
        ),
    )(spins_packed, weight, hidden_bias.reshape(1, -1), force_w, force_b.reshape(1, -1))
    update_w, update_b = pl.pallas_call(
        finish_kernel,
        out_shape=(jax.ShapeDtypeStruct((rows, units), F32), jax.ShapeDtypeStruct((1, units), F32)),
        in_specs=[vmem] * 4,
        out_specs=(vmem, vmem),
    )(*[pltpu.with_memory_space_constraint(result, pltpu.VMEM) for result in results])
    return update_w, update_b.reshape(-1)


def solution(mesh):
    placed = (P(None, "smp"), P(None, "grp"), P("grp"), P("smp", "grp"), P("grp"))
    return jax.shard_map(
        functools.partial(body, mesh.shape["grp"], mesh.shape["smp"]),
        mesh=mesh, in_specs=placed, out_specs=(P("smp", "grp"), P("grp")), check_vma=False,
    )
```

```python
import functools

import jax
import jax.numpy as jnp
from jax import lax
from jax.experimental import pallas as pl
from jax.experimental.pallas import tpu as pltpu
from jax.sharding import PartitionSpec as P

MESH = pl.DeviceIdType.MESH
F32, BF16 = jnp.float32, jnp.bfloat16
diag_shift = 0.01
SETS = 8
EXTRA = 256
PAD = 16
PART = 256
PIECE = 128
LINE = 4


def total(x):
    return jnp.sum(jnp.sum(x, axis=0, keepdims=True), axis=1, keepdims=True)


def kernel(
    groups, shards,
    packed_in, weight_in, bias_in, force_in, force_b_in,
    image_ref, image_b_ref, own_ref, scale_ref,
    packed, weight, weight_t, bias_ref, bias_t, force_b_ref, tile, spins, hidden, force_all, lhs, scaled, plain,
    image, image_core, image_z, image_x, image_all, image_b, by_group_a, by_group_b, by_rank_a, by_rank_b, by_set, by_shard, by_total,
    load, spin_send, spin_recv, pass_send, pass_recv, force_send, force_recv, image_send, image_recv,
    gather_send, gather_recv,
):
    grp, smp = lax.axis_index("grp"), lax.axis_index("smp")
    words, here = packed_in.shape
    inputs, units = weight.shape
    rows = force_in.shape[0]
    ranks = shards // SETS
    pair = SETS * rows
    samples = ranks * here
    count = samples * SETS
    quarter = here // LINE
    parts = units // PART
    pieces = units // PIECE
    depth = 2 * ranks

    core, z, half = lax.rem(smp, 2), lax.rem(smp // 2, depth), smp // (2 * depth)
    parity, rank = lax.rem(z, 2), z // 2
    member = (core * 2 + parity) * 2 + half
    y, column = lax.rem(grp, LINE), grp // LINE

    def device(half_at, z_at, core_at):
        return {"smp": (half_at * depth + z_at) * 2 + core_at}

    sibling = device(half, z, 1 - core)
    z_partner = device(half, z + 1 - 2 * parity, core)
    x_partner = device(1 - half, z, core)

    def group_device(at):
        return {"grp": at}

    def line_device(at):
        return {"grp": column * LINE + at}

    def rank_device(at):
        return device(half, 2 * at + parity, core)

    def set_device(at):
        return device(lax.rem(at, 2), 2 * rank + lax.rem(at // 2, 2), at // 4)

    def shard_device(at):
        return {"smp": at}

    def remote(source, target, send, recv, where):
        return pltpu.make_async_remote_copy(
            source, target, send, recv, device_id=where, device_id_type=MESH
        )

    barrier = pltpu.get_barrier_semaphore()
    for size, me, peer in ((groups, grp, group_device), (ranks, rank, rank_device)):
        for step in range(1, size):
            pl.semaphore_signal(barrier, device_id=peer(lax.rem(me + step, size)), device_id_type=MESH)
    for where in (sibling, z_partner, x_partner):
        pl.semaphore_signal(barrier, device_id=where, device_id_type=MESH)

    def cols_of(at):
        return slice(at * PART, (at + 1) * PART)

    def cols_ds(at):
        return pl.ds(pl.multiple_of(at * PART, PART), PART)

    copies = []
    for at in range(LINE):
        copies.append(
            pltpu.make_async_copy(packed_in.at[:, pl.ds(at * quarter, quarter)], packed.at[rank, at], load.at[3])
        )
    for at in range(parts):
        copies.append(
            pltpu.make_async_copy(force_in.at[:, cols_ds(at)], force_all.at[at, core, parity, half], load.at[4])
        )
    later = [
        pltpu.make_async_copy(weight_in, weight, load.at[0]),
        pltpu.make_async_copy(bias_in, bias_ref, load.at[1]),
        pltpu.make_async_copy(force_b_in, force_b_ref, load.at[2]),
    ]
    for copy in copies + later:
        copy.start()
    pltpu.make_async_copy(packed.at[rank], packed.at[rank], load.at[3]).wait()
    blocks = force_all.at[:, core, parity, half]
    pltpu.make_async_copy(blocks, blocks, load.at[4]).wait()

    def turn(at, carry):
        cols = pl.ds(pl.multiple_of(at * 256, 256), 256)
        weight_t[cols, :] = weight[:, cols].T
        bias_t[cols, :] = jnp.broadcast_to(bias_ref[:, cols], (128, 256)).T
        return carry

    after, before, across = lax.rem(rank + 1, ranks), lax.rem(rank + ranks - 1, ranks), lax.rem(rank + 2, ranks)

    def force_send_own(at, which, where):
        own = force_all.at[at, core, parity, half]
        remote(own, own, force_send.at[which], force_recv.at[at, which], where).start()

    def force_arrived(at, which):
        target = (
            force_all.at[at, core, 1 - parity, half],
            force_all.at[at, core, parity, 1 - half],
            force_all.at[at, core, 1 - parity, 1 - half],
            force_all.at[at, 1 - core, parity],
            force_all.at[at, 1 - core, 1 - parity],
        )[which]
        remote(target, target, force_send.at[which], force_recv.at[at, which], sibling).wait_recv()

    def force_x(at):
        force_arrived(at, 1)
        block_x = force_all.at[at, core, parity, 1 - half]
        remote(block_x, block_x, force_send.at[2], force_recv.at[at, 2], z_partner).start()
        ours = force_all.at[at, core, parity]
        remote(ours, ours, force_send.at[3], force_recv.at[at, 3], sibling).start()

    def force_z(at):
        force_arrived(at, 0)
        force_arrived(at, 2)
        theirs = force_all.at[at, core, 1 - parity]
        remote(theirs, theirs, force_send.at[4], force_recv.at[at, 4], sibling).start()

    def force_whole(at):
        force_arrived(at, 3)
        force_arrived(at, 4)

    def spin_send_to(step):
        own = packed.at[rank, y]
        return remote(own, own, spin_send.at[0], spin_recv.at[rank], rank_device(lax.rem(rank + step, ranks)))

    def spin_arrived(source):
        target = packed.at[source, y]
        remote(target, target, spin_send.at[0], spin_recv.at[source], sibling).wait_recv()

    def hand_on(source, slot):
        for step in (1, 3, 2):
            piece = packed.at[source, y]
            remote(
                piece, piece, pass_send.at[slot], pass_recv.at[source, y], line_device(lax.rem(y + step, LINE))
            ).start()

    def handed(source, step):
        from_y = lax.rem(y + step, LINE)
        target = packed.at[source, from_y]
        remote(target, target, pass_send.at[0], pass_recv.at[source, from_y], sibling).wait_recv()
        return source, from_y

    masks = jnp.left_shift(1, lax.broadcasted_iota(jnp.int32, (32, quarter), 0))

    def places(tiles):
        return [pl.ds(pl.multiple_of(source * here + at * quarter, quarter), quarter) for source, at in tiles]

    def unpack(tiles):
        cols = places(tiles)
        for which, (source, at) in enumerate(tiles):
            to = slice(which * quarter, (which + 1) * quarter)
            for word in range(words):
                bits = jnp.bitwise_and(jnp.broadcast_to(packed[source, at, word : word + 1, :], (32, quarter)), masks)
                tile[word * 32 : word * 32 + 32, to] = jnp.where(bits != 0, 1.0, -1.0).astype(BF16)
        for to in range(SETS):
            word = (to % 2) * 2 * depth + 4 * rank + 2 * (to // 2 % 2) + to // 4
            from_rows = pl.ds(pl.multiple_of(word * rows, rows), rows)
            for which in range(2):
                spins[to * rows : (to + 1) * rows, cols[which]] = tile[
                    from_rows, which * quarter : (which + 1) * quarter
                ]

    def activate(tiles):
        cols = places(tiles)
        for unit in range(0, units, 1024):
            these = pl.ds(unit, 1024)
            pre = jnp.dot(weight_t[these, :], tile[...], preferred_element_type=F32)
            pre = pre + jnp.concatenate([bias_t[these, :]] * (2 * quarter // 128), axis=1)
            result = jnp.tanh(pre).astype(BF16)
            for which in range(2):
                hidden[these, cols[which]] = result[:, which * quarter : (which + 1) * quarter]

    def hidden_of(*tiles):
        unpack(tiles)
        activate(tiles)

    with jax.named_scope("barrier"):
        pl.semaphore_wait(barrier, groups + ranks + 1)
    for at in range(parts):
        force_send_own(at, 1, x_partner)
    for step in (1, ranks - 1, 2):
        spin_send_to(step).start()
    for at in range(parts):
        force_send_own(at, 0, z_partner)

    spins[pair:, :] = (lax.broadcasted_iota(jnp.int32, (PAD, samples), 0) == 0).astype(F32).astype(BF16)
    with jax.named_scope("turn"):
        for copy in later:
            copy.wait()
        lax.fori_loop(0, units // 256, turn, 0)
    with jax.named_scope("hidden0"):
        hidden_of((rank, 0), (rank, 1))
        hidden_of((rank, 2), (rank, 3))
    with jax.named_scope("spinab"):
        spin_arrived(before)
        hand_on(before, 0)
        spin_arrived(after)
        hand_on(after, 1)
    with jax.named_scope("hidden1"):
        hidden_of((before, y), (after, y))
    with jax.named_scope("spinc"):
        spin_arrived(across)
        hand_on(across, 2)
        for at in range(parts):
            force_x(at)
        tiles = (across, y), handed(before, 1)
    with jax.named_scope("hidden2"):
        hidden_of(*tiles)
    with jax.named_scope("wait"):
        tiles = handed(before, 3), handed(after, 1), handed(after, 3), handed(before, 2)
    with jax.named_scope("hidden3"):
        hidden_of(*tiles[:2])
        hidden_of(*tiles[2:])
    with jax.named_scope("wait"):
        for at in range(parts):
            force_z(at)
        tiles = handed(after, 2), handed(across, 1), handed(across, 3), handed(across, 2)
    with jax.named_scope("hidden4"):
        hidden_of(*tiles[:2])
        hidden_of(*tiles[2:])

    span = samples // 2
    by_group, by_rank = (by_group_a, by_group_b), (by_rank_a, by_rank_b)

    def fill_lhs(at, slots, row):
        width = slots.shape[-1]
        cols = slice(at * width, (at + 1) * width)
        for to in range(SETS):
            lhs[to * rows : (to + 1) * rows, cols] = slots[at, to // 4, to // 2 % 2, to % 2].astype(BF16)
        lhs[pair:, cols] = jnp.concatenate(
            [row[:, cols] / ranks, jnp.zeros((PAD - 1, width), F32)], axis=0
        ).astype(BF16)

    def values_of(which, first, last, side, fresh):
        these, cols = slice(first * PART, last * PART), slice(side * span, (side + 1) * span)
        product = jnp.dot(lhs[:, these], hidden[these, cols], preferred_element_type=F32)
        value = jnp.sum(product[:pair] * spins[:pair, cols].astype(F32), axis=0, keepdims=True) + product[pair : pair + 1]
        mine = by_group[side].at[which, grp, :, :span]
        mine[...] = value if fresh else mine[...] + value

    with jax.named_scope("forcew"):
        for at in range(parts):
            force_whole(at)
            fill_lhs(at, force_all, force_b_ref)
    def gather(slots, which, size, me, peer):
        send, recv = gather_send.at[which], gather_recv.at[which]
        for step in range(1, size):
            remote(slots.at[me], slots.at[me], send, recv, peer(lax.rem(me + step, size))).start()
        others = slots.at[pl.ds(0, size - 1)]

        def finish():
            remote(others, others, send, recv, sibling).wait()

        return finish

    def gather_shards():
        send, recv = gather_send.at[12], gather_recv.at[12]
        for far in sorted(range(depth), key=lambda apart: -min(apart, depth - apart)):
            for half_at in (1 - half, half):
                for core_at in (1 - core, core):
                    if far or half_at is not half or core_at is not core:
                        where = device(half_at, lax.rem(z + far, depth), core_at)
                        remote(by_shard.at[smp], by_shard.at[smp], send, recv, where).start()
        others = by_shard.at[pl.ds(0, shards - 1)]

        def finish():
            remote(others, others, send, recv, sibling).wait()

        return finish

    def wide(x, lanes=128):
        return jnp.broadcast_to(x, (1, lanes))

    def send_groups(which, side):
        return gather(by_group[side].at[which], 2 * which + side, groups, grp, group_device)

    def send_ranks(which, side):
        mine = by_group[side][which, 0]
        for source in range(1, groups):
            mine = mine + by_group[side][which, source]
        by_rank[side][which, rank] = mine
        return gather(by_rank[side].at[which], 4 + 2 * which + side, ranks, rank, rank_device)

    def sum_ranks(which, side):
        whole = by_rank[side][which, 0]
        for source in range(1, ranks):
            whole = whole + by_rank[side][which, source]
        return whole

    def gather_sets(which, values):
        fill = jnp.zeros((8 - len(values), 128), F32)
        by_set[which, member] = jnp.concatenate([wide(value) for value in values] + [fill], axis=0)
        return gather(by_set.at[which], 8 + which, SETS, member, set_device)

    def set_sum(which, row):
        value = by_set[which, 0, row : row + 1, :]
        for source in range(1, SETS):
            value = value + by_set[which, source, row : row + 1, :]
        return value[:, :1]

    def own_force(at):
        return force_all[at, core, parity, half]

    force_dot = total(force_b_ref[...] * force_b_ref[...]) / shards
    for at in range(parts):
        force_dot = force_dot + total(own_force(at) * own_force(at))
    def of_hidden(left, at):
        return lax.dot_general(
            left[...], hidden[cols_ds(at), :], (((1,), (1,)), ((), ())), preferred_element_type=F32
        )

    def extras(which, first, second):
        by_group[1][which, grp, :, span:] = jnp.concatenate([wide(first), wide(second)], axis=1)

    def own_sum(side):
        return total(by_group[side][0, grp, :, :span])

    with jax.named_scope("values0"):
        values_of(0, 0, parts, 0, True)
        finish_a = send_groups(0, 0)
        extras(0, force_dot, jnp.zeros((1, 1), F32))
        values_of(0, 0, parts, 1, True)
        finish_b = send_groups(0, 1)
    with jax.named_scope("redg"):
        by_shard[smp] = wide(own_sum(0) + own_sum(1))
        finish_shards = gather_shards()

        def plain_part(at, carry):
            plain[at] = of_hidden(spins, at)
            return carry

        lax.fori_loop(0, parts - 1, plain_part, 0)
        finish_a()
        finish_ranks_a = send_ranks(0, 0)
        finish_b()
        finish_ranks_b = send_ranks(0, 1)
        lax.fori_loop(parts - 1, parts, plain_part, 0)
    with jax.named_scope("shards"):
        finish_shards()
        mine = by_shard[0]
        for source in range(1, shards):
            mine = mine + by_shard[source]
        by_total[grp] = mine
        finish_total = gather(by_total, 13, groups, grp, group_device)
    with jax.named_scope("redr"):
        finish_ranks_a()
        finish_ranks_b()
        sums = [sum_ranks(0, side) for side in range(2)]
        own_dot = sums[1][:, span : span + 1]
        mean_own = (total(sums[0][:, :span]) + total(sums[1][:, :span])) / samples
        centred = [whole[:, :span] - mean_own for whole in sums]
    with jax.named_scope("scaled"):
        for at in range(0, samples, 512):
            weights = centred[at // span][:, at % span : at % span + 512]
            scaled[:pair, at : at + 512] = (spins[:pair, at : at + 512].astype(F32) * weights).astype(BF16)
            scaled[pair:, at : at + 512] = jnp.concatenate(
                [weights, jnp.zeros((PAD - 1, 512), F32)], axis=0
            ).astype(BF16)

    def outer(at):
        return (x_partner, z_partner, half) if at % 2 == 0 else (z_partner, x_partner, parity)

    def pick(ref, at, which):
        return ref.at[:, which] if at % 2 == 0 else ref.at[which]

    def core_copy(at):
        return remote(image.at[at, 1 - core], image_core.at[at], image_send.at[0], image_recv.at[at, 0], sibling)

    def image_copy(at, which):
        far, near, place = outer(at)
        ours = pick(image_all.at[at, core], at, place)
        theirs = pick(image_all.at[at, core], at, 1 - place)
        source, target, where = (
            None,
            (pick(image.at[at, core], at, 1 - place), image_z.at[at], far),
            (pick(image.at[at, core], at, place), image_x.at[at], near),
            (ours, ours, far),
            (ours, ours, sibling),
            (theirs, theirs, sibling),
        )[which]
        return remote(source, target, image_send.at[which], image_recv.at[at, which], where)

    def image_arrived(at, which):
        place = outer(at)[2]
        target = (
            image_core.at[at], image_z.at[at], image_x.at[at],
            pick(image_all.at[at, core], at, 1 - place),
            pick(image_all.at[at, 1 - core], at, place),
            pick(image_all.at[at, 1 - core], at, 1 - place),
        )[which]
        remote(target, target, image_send.at[which], image_recv.at[at, which], sibling).wait_recv()

    per = PART // PIECE

    def image_part(at, carry):
        part = of_hidden(scaled, at)
        for to in range(SETS):
            for which in range(per):
                image[per * at + which, to // 4, to // 2 % 2, to % 2] = part[
                    to * rows : (to + 1) * rows, which * PIECE : (which + 1) * PIECE
                ]
        image_b[member, :, cols_ds(at)] = part[pair : pair + 1]
        return carry

    def shifted(at):
        for which in range(per):
            for to in range(SETS):
                block = image.at[per * at + which, to // 4, to // 2 % 2, to % 2]
                block[...] = block[...] + shift * plain[
                    at, to * rows : (to + 1) * rows, which * PIECE : (which + 1) * PIECE
                ]
            core_copy(per * at + which).start()
        image_b[member, :, cols_ds(at)] = image_b[member, :, cols_ds(at)] + shift * plain[at, pair : pair + 1]

    def sum_core(at):
        place = outer(at)[2]
        image_arrived(at, 0)
        theirs = pick(image.at[at, core], at, 1 - place)
        theirs[...] = theirs[...] + pick(image_core.at[at], at, 1 - place)[...]
        image_copy(at, 1).start()
        ours = pick(image.at[at, core], at, place)
        ours[...] = ours[...] + pick(image_core.at[at], at, place)[...]

    def sum_outer(at):
        image_arrived(at, 1)
        ours = pick(image.at[at, core], at, outer(at)[2])
        ours[...] = ours[...] + image_z[at]
        image_copy(at, 2).start()

    def sum_inner(at):
        image_arrived(at, 2)
        place = outer(at)[2]
        pick(image_all.at[at, core], at, place)[...] = pick(image.at[at, core], at, place)[...] + image_x[at]
        image_copy(at, 3).start()
        image_copy(at, 4).start()

    def share(at):
        image_arrived(at, 3)
        image_copy(at, 5).start()

    def image_ready(at):
        image_arrived(at, 4)
        image_arrived(at, 5)
        fill_lhs(at, image_all, image_b[0])

    def named(name, step, *at):
        with jax.named_scope(name):
            step(*at)

    with jax.named_scope("image"):
        lax.fori_loop(0, 2, image_part, 0)
    with jax.named_scope("mean"):
        finish_total()
        mean0 = by_total[0]
        for source in range(1, groups):
            mean0 = mean0 + by_total[source]
        shift = mean_own - mean0[:, :1] / count
        shifted(0)
        shifted(1)
        moment = total(centred[0] * centred[0]) + total(centred[1] * centred[1]) + samples * shift * shift
        finish_moment = gather_sets(0, [moment, own_dot])

    def image_step(at, carry):
        image_part(at, 0)
        shifted(at)

        @pl.when(at == 2)
        def _():
            for piece in range(2 * per):
                sum_core(piece)

        return carry

    with jax.named_scope("image"):
        lax.fori_loop(2, parts, image_step, 0)
    finish_bias = gather(image_b, 11, SETS, member, set_device)
    turns = [at ^ 1 for at in range(pieces)]
    for at in range(2 * per, pieces):
        named("core", sum_core, at)
    for at in turns:
        named("outer", sum_outer, at)
    with jax.named_scope("bias"):
        finish_moment()
        finish_bias()
        norm0 = set_sum(0, 1)
        step0 = norm0 / (set_sum(0, 0) / count + diag_shift * norm0)
        keep = 1.0 - diag_shift * step0
        pull = step0 / count
        whole_b = image_b[0]
        for source in range(1, SETS):
            whole_b = whole_b + image_b[source]
        image_b[0] = whole_b
    for at in range(pieces):
        named("inner", sum_inner, at)
    with jax.named_scope("norm"):
        residual_b = keep * force_b_ref[...] - pull * whole_b
        own_norm = total(residual_b * residual_b) / shards
        own_cross = total(residual_b * force_b_ref[...]) / shards
        image_b_ref[0:1, :] = whole_b
        image_b_ref[1:2, :] = force_b_ref[...]
        for at in range(parts):
            own_ref[:, cols_of(at)] = own_force(at)
        for at in range(pieces):
            image_ref[:, at * PIECE : (at + 1) * PIECE] = image_all[at, core, parity, half]
        residual = keep * own_ref[...] - pull * image_ref[...]
        own_norm = own_norm + total(residual * residual)
        own_cross = own_cross + total(residual * own_ref[...])
        finish_norm = gather_sets(1, [own_norm, own_cross])
    near, last = turns[: pieces // 2], turns[pieces // 2 :]
    for at in near:
        named("share", share, at)
    for at in near[:2]:
        named("ready", image_ready, at)
    for at in last[:2]:
        named("share", share, at)
    for at in near[2:]:
        named("ready", image_ready, at)
    with jax.named_scope("values1"):
        values_of(1, 0, 2, 0, True)
    for at in last[2:]:
        named("share", share, at)
    with jax.named_scope("values1"):
        values_of(1, 0, 2, 1, True)
    for at in last:
        named("ready", image_ready, at)
    named("fnorm", finish_norm)
    extras(1, set_sum(1, 0), set_sum(1, 1))
    with jax.named_scope("values1"):
        values_of(1, 2, 4, 0, False)
        finish_a = send_groups(1, 0)
        values_of(1, 2, 4, 1, False)
        finish_b = send_groups(1, 1)
    with jax.named_scope("redg"):
        finish_a()
        finish_ranks_a = send_ranks(1, 0)
        finish_b()
        finish_ranks_b = send_ranks(1, 1)
    with jax.named_scope("redr"):
        finish_ranks_a()
        finish_ranks_b()
        sums = [sum_ranks(1, side) for side in range(2)]
        norm1, cross = sums[1][:, span : span + 1], sums[1][:, span + 128 : span + 129]
    beta = norm1 / norm0
    with jax.named_scope("sets"):
        values1 = [(keep + beta) * (centred[side] + shift) - pull * sums[side][:, :span] for side in range(2)]
        mean1 = (total(values1[0]) + total(values1[1])) / samples
        values1 = [value - mean1 for value in values1]
        gather_sets(2, [mean1, total(values1[0] * values1[0]) + total(values1[1] * values1[1])])()
        middle = set_sum(2, 0) / SETS
        spread = jnp.zeros((1, 1), F32)
        for source in range(SETS):
            shift = by_set[2, source, 0:1, :1] - middle
            spread = spread + shift * shift
        variance1 = (set_sum(2, 1) + samples * spread) / count
    direction_dot = norm1 + 2.0 * beta * cross + beta * beta * norm0
    step1 = norm1 / (variance1 + diag_shift * direction_dot)

    for_force = step0 + step1 * (keep + beta)
    for_image = step1 * pull
    scale_ref[...] = jnp.concatenate([wide(for_force), wide(for_image), jnp.zeros((6, 128), F32)], axis=0)
    with jax.named_scope("out"):
        pieces = packed.at[rank, pl.ds(0, LINE - 1)]
        remote(pieces, pieces, spin_send.at[0], spin_recv.at[0], sibling).wait_send()
        for slot in range(3):
            remote(pieces, pieces, pass_send.at[slot], spin_recv.at[0], sibling).wait_send()
        for which in range(5):
            blocks = force_all.at[:, core, parity] if which > 2 else force_all.at[:, core, parity, half]
            remote(blocks, blocks, force_send.at[which], spin_recv.at[0], sibling).wait_send()
        for which in range(6):
            blocks = image_core if which == 0 else image_z
            remote(blocks, blocks, image_send.at[which], spin_recv.at[0], sibling).wait_send()


def finish_kernel(image_ref, image_b_ref, force_ref, scale_ref, out_ref, out_b_ref):
    for_force, for_image = scale_ref[0:1, 0:1], scale_ref[1:2, 0:1]
    out_ref[...] = for_force * force_ref[...] - for_image * image_ref[...]
    out_b_ref[...] = for_force * image_b_ref[1:2, :] - for_image * image_b_ref[0:1, :]


def body(groups, shards, spins_packed, weight, hidden_bias, force_w, force_b):
    words, here = spins_packed.shape
    inputs, units = weight.shape
    rows = force_w.shape[0]
    ranks = shards // SETS
    samples, pair = ranks * here, SETS * rows
    parts, pieces = units // PART, units // PIECE
    quarter = here // LINE
    vmem = pl.BlockSpec(memory_space=pltpu.VMEM)
    anywhere = pl.BlockSpec(memory_space=pl.ANY)
    dma = pltpu.SemaphoreType.DMA
    results = pl.pallas_call(
        functools.partial(kernel, groups, shards),
        out_shape=(
            pltpu.VMEM((rows, units), F32), pltpu.VMEM((8, units), F32),
            pltpu.VMEM((rows, units), F32), pltpu.VMEM((8, 128), F32),
        ),
        in_specs=[anywhere] * 5,
        out_specs=(vmem,) * 4,
        scratch_shapes=[
            pltpu.VMEM((ranks, LINE, words, quarter), jnp.int32),
            pltpu.VMEM((inputs, units), BF16),
            pltpu.VMEM((units, inputs), BF16),
            pltpu.VMEM((1, units), F32),
            pltpu.VMEM((units, 128), F32),
            pltpu.VMEM((1, units), F32),
            pltpu.VMEM((inputs, 2 * quarter), BF16),
            pltpu.VMEM((pair + PAD, samples), BF16),
            pltpu.VMEM((units, samples), BF16),
            pltpu.VMEM((parts, 2, 2, 2, rows, PART), F32),
            pltpu.VMEM((pair + PAD, units), BF16),
            pltpu.VMEM((pair + PAD, samples), BF16),
            pltpu.VMEM((parts, pair + PAD, PART), F32),
            pltpu.VMEM((pieces, 2, 2, 2, rows, PIECE), F32),
            pltpu.VMEM((pieces, 2, 2, rows, PIECE), F32),
            pltpu.VMEM((pieces, 2, rows, PIECE), F32),
            pltpu.VMEM((pieces, 2, rows, PIECE), F32),
            pltpu.VMEM((pieces, 2, 2, 2, rows, PIECE), F32),
            pltpu.VMEM((SETS, 1, units), F32),
            pltpu.VMEM((2, groups, 1, samples // 2), F32),
            pltpu.VMEM((2, groups, 1, samples // 2 + EXTRA), F32),
            pltpu.VMEM((2, ranks, 1, samples // 2), F32),
            pltpu.VMEM((2, ranks, 1, samples // 2 + EXTRA), F32),
            pltpu.VMEM((3, SETS, 8, 128), F32),
            pltpu.VMEM((shards, 1, 128), F32),
            pltpu.VMEM((groups, 1, 128), F32),
            dma((5,)),
            dma((1,)),
            dma((ranks,)),
            dma((3,)),
            dma((ranks, LINE)),
            dma((5,)),
            dma((parts, 5)),
            dma((6,)),
            dma((pieces, 6)),
            dma((14,)),
            dma((14,)),
        ],
        compiler_params=pltpu.CompilerParams(
            collective_id=0, has_side_effects=True, vmem_limit_bytes=62 * 1024 * 1024
        ),
    )(spins_packed, weight, hidden_bias.reshape(1, -1), force_w, force_b.reshape(1, -1))
    update_w, update_b = pl.pallas_call(
        finish_kernel,
        out_shape=(jax.ShapeDtypeStruct((rows, units), F32), jax.ShapeDtypeStruct((1, units), F32)),
        in_specs=[vmem] * 4,
        out_specs=(vmem, vmem),
    )(*[pltpu.with_memory_space_constraint(result, pltpu.VMEM) for result in results])
    return update_w, update_b.reshape(-1)


def solution(mesh):
    placed = (P(None, "smp"), P(None, "grp"), P("grp"), P("smp", "grp"), P("grp"))
    return jax.shard_map(
        functools.partial(body, mesh.shape["grp"], mesh.shape["smp"]),
        mesh=mesh, in_specs=placed, out_specs=(P("smp", "grp"), P("grp")), check_vma=False,
    )
```

```python
import functools

import jax
import jax.numpy as jnp
from jax import lax
from jax.experimental import pallas as pl
from jax.experimental.pallas import tpu as pltpu
from jax.sharding import PartitionSpec as P

MESH = pl.DeviceIdType.MESH
F32, BF16 = jnp.float32, jnp.bfloat16
diag_shift = 0.01
SETS = 8
EXTRA = 256
PAD = 16
PART = 256
PIECE = 128
LINE = 4


def total(x):
    return jnp.sum(jnp.sum(x, axis=0, keepdims=True), axis=1, keepdims=True)


def kernel(
    groups, shards,
    packed_in, weight_in, bias_in, force_in, force_b_in,
    image_ref, image_b_ref, own_ref, scale_ref,
    packed, weight, weight_t, bias_ref, bias_t, force_b_ref, tile, spins, hidden, force_all, lhs, scaled, plain,
    image, image_core, image_z, image_x, image_all, image_b, by_group_a, by_group_b, by_rank_a, by_rank_b, by_set, by_shard, by_total,
    load, spin_send, spin_recv, pass_send, pass_recv, force_send, force_recv, image_send, image_recv,
    gather_send, gather_recv,
):
    grp, smp = lax.axis_index("grp"), lax.axis_index("smp")
    words, here = packed_in.shape
    inputs, units = weight.shape
    rows = force_in.shape[0]
    ranks = shards // SETS
    pair = SETS * rows
    samples = ranks * here
    count = samples * SETS
    quarter = here // LINE
    parts = units // PART
    pieces = units // PIECE
    depth = 2 * ranks

    core, z, half = lax.rem(smp, 2), lax.rem(smp // 2, depth), smp // (2 * depth)
    parity, rank = lax.rem(z, 2), z // 2
    member = (core * 2 + parity) * 2 + half
    y, column = lax.rem(grp, LINE), grp // LINE

    def device(half_at, z_at, core_at):
        return {"smp": (half_at * depth + z_at) * 2 + core_at}

    sibling = device(half, z, 1 - core)
    z_partner = device(half, z + 1 - 2 * parity, core)
    x_partner = device(1 - half, z, core)

    def group_device(at):
        return {"grp": at}

    def line_device(at):
        return {"grp": column * LINE + at}

    def rank_device(at):
        return device(half, 2 * at + parity, core)

    def remote(source, target, send, recv, where):
        return pltpu.make_async_remote_copy(
            source, target, send, recv, device_id=where, device_id_type=MESH
        )

    barrier = pltpu.get_barrier_semaphore()
    for size, me, peer in ((groups, grp, group_device), (ranks, rank, rank_device)):
        for step in range(1, size):
            pl.semaphore_signal(barrier, device_id=peer(lax.rem(me + step, size)), device_id_type=MESH)
    for where in (sibling, z_partner, x_partner):
        pl.semaphore_signal(barrier, device_id=where, device_id_type=MESH)

    def cols_of(at):
        return slice(at * PART, (at + 1) * PART)

    def cols_ds(at):
        return pl.ds(pl.multiple_of(at * PART, PART), PART)

    copies = []
    for at in range(LINE):
        copies.append(
            pltpu.make_async_copy(packed_in.at[:, pl.ds(at * quarter, quarter)], packed.at[rank, at], load.at[3])
        )
    for at in range(parts):
        copies.append(
            pltpu.make_async_copy(force_in.at[:, cols_ds(at)], force_all.at[at, core, parity, half], load.at[4])
        )
    later = [
        pltpu.make_async_copy(weight_in, weight, load.at[0]),
        pltpu.make_async_copy(bias_in, bias_ref, load.at[1]),
        pltpu.make_async_copy(force_b_in, force_b_ref, load.at[2]),
    ]
    for copy in copies + later:
        copy.start()
    pltpu.make_async_copy(packed.at[rank], packed.at[rank], load.at[3]).wait()
    blocks = force_all.at[:, core, parity, half]
    pltpu.make_async_copy(blocks, blocks, load.at[4]).wait()

    def turn(at, carry):
        cols = pl.ds(pl.multiple_of(at * 256, 256), 256)
        weight_t[cols, :] = weight[:, cols].T
        bias_t[cols, :] = jnp.broadcast_to(bias_ref[:, cols], (128, 256)).T
        return carry

    after, before, across = lax.rem(rank + 1, ranks), lax.rem(rank + ranks - 1, ranks), lax.rem(rank + 2, ranks)

    def force_copy(which):
        source, recv, where = (
            (force_all.at[:, core, parity, half], 0, z_partner),
            (force_all.at[:, core, parity, half], 1, x_partner),
            (force_all.at[:, core, parity, 1 - half], 0, z_partner),
            (force_all.at[:, core, parity], 2, sibling),
            (force_all.at[:, core, 1 - parity], 2, sibling),
        )[which]
        return remote(source, source, force_send.at[which], force_recv.at[recv], where)

    def force_arrived(which):
        target = (
            force_all.at[:, core, 1 - parity], force_all.at[:, core, parity, 1 - half], force_all.at[:, 1 - core]
        )[which]
        remote(target, target, force_send.at[which], force_recv.at[which], sibling).wait_recv()

    def spin_send_to(step):
        own = packed.at[rank, y]
        return remote(own, own, spin_send.at[0], spin_recv.at[rank], rank_device(lax.rem(rank + step, ranks)))

    def spin_arrived(source):
        target = packed.at[source, y]
        remote(target, target, spin_send.at[0], spin_recv.at[source], sibling).wait_recv()

    def hand_on(source, slot):
        for step in (1, 3, 2):
            piece = packed.at[source, y]
            remote(
                piece, piece, pass_send.at[slot], pass_recv.at[source, y], line_device(lax.rem(y + step, LINE))
            ).start()

    def handed(source, step):
        from_y = lax.rem(y + step, LINE)
        target = packed.at[source, from_y]
        remote(target, target, pass_send.at[0], pass_recv.at[source, from_y], sibling).wait_recv()
        return source, from_y

    masks = jnp.left_shift(1, lax.broadcasted_iota(jnp.int32, (32, quarter), 0))

    def places(tiles):
        return [pl.ds(pl.multiple_of(source * here + at * quarter, quarter), quarter) for source, at in tiles]

    def unpack(tiles):
        cols = places(tiles)
        for which, (source, at) in enumerate(tiles):
            to = slice(which * quarter, (which + 1) * quarter)
            for word in range(words):
                bits = jnp.bitwise_and(jnp.broadcast_to(packed[source, at, word : word + 1, :], (32, quarter)), masks)
                tile[word * 32 : word * 32 + 32, to] = jnp.where(bits != 0, 1.0, -1.0).astype(BF16)
        for to in range(SETS):
            word = (to % 2) * 2 * depth + 4 * rank + 2 * (to // 2 % 2) + to // 4
            from_rows = pl.ds(pl.multiple_of(word * rows, rows), rows)
            for which in range(2):
                spins[to * rows : (to + 1) * rows, cols[which]] = tile[
                    from_rows, which * quarter : (which + 1) * quarter
                ]

    def activate(tiles):
        cols = places(tiles)
        for unit in range(0, units, 1024):
            these = pl.ds(unit, 1024)
            pre = jnp.dot(weight_t[these, :], tile[...], preferred_element_type=F32)
            pre = pre + jnp.concatenate([bias_t[these, :]] * (2 * quarter // 128), axis=1)
            result = jnp.tanh(pre).astype(BF16)
            for which in range(2):
                hidden[these, cols[which]] = result[:, which * quarter : (which + 1) * quarter]

    def hidden_of(*tiles):
        unpack(tiles)
        activate(tiles)

    with jax.named_scope("barrier"):
        pl.semaphore_wait(barrier, groups + ranks + 1)
    force_copy(1).start()
    for step in (2, 1, ranks - 1):
        spin_send_to(step).start()
    force_copy(0).start()

    spins[pair:, :] = (lax.broadcasted_iota(jnp.int32, (PAD, samples), 0) == 0).astype(F32).astype(BF16)
    with jax.named_scope("turn"):
        for copy in later:
            copy.wait()
        lax.fori_loop(0, units // 256, turn, 0)
    with jax.named_scope("hidden0"):
        hidden_of((rank, 0), (rank, 1))
        hidden_of((rank, 2), (rank, 3))
    with jax.named_scope("spinab"):
        spin_arrived(before)
        hand_on(before, 0)
        spin_arrived(after)
        hand_on(after, 1)
    with jax.named_scope("hidden1"):
        hidden_of((before, y), (after, y))
    with jax.named_scope("spinc"):
        spin_arrived(across)
        hand_on(across, 2)
        force_arrived(1)
        force_copy(2).start()
        force_copy(3).start()
        tiles = (across, y), handed(before, 3)
    with jax.named_scope("hidden2"):
        hidden_of(*tiles)
    with jax.named_scope("wait"):
        tiles = handed(after, 3), handed(before, 1), handed(after, 1), handed(before, 2)
    with jax.named_scope("hidden3"):
        hidden_of(*tiles[:2])
        hidden_of(*tiles[2:])
    with jax.named_scope("wait"):
        force_arrived(0)
        force_copy(4).start()
        tiles = handed(after, 2), handed(across, 1), handed(across, 3), handed(across, 2)
    with jax.named_scope("hidden4"):
        hidden_of(*tiles[:2])
        hidden_of(*tiles[2:])

    span = samples // 2
    by_group, by_rank = (by_group_a, by_group_b), (by_rank_a, by_rank_b)

    def fill_lhs(at, slots, row):
        width = slots.shape[-1]
        cols = slice(at * width, (at + 1) * width)
        for to in range(SETS):
            lhs[to * rows : (to + 1) * rows, cols] = slots[at, to // 4, to // 2 % 2, to % 2].astype(BF16)
        lhs[pair:, cols] = jnp.concatenate(
            [row[:, cols] / ranks, jnp.zeros((PAD - 1, width), F32)], axis=0
        ).astype(BF16)

    def values_of(which, first, last, side, fresh):
        these, cols = slice(first * PART, last * PART), slice(side * span, (side + 1) * span)
        product = jnp.dot(lhs[:, these], hidden[these, cols], preferred_element_type=F32)
        value = jnp.sum(product[:pair] * spins[:pair, cols].astype(F32), axis=0, keepdims=True) + product[pair : pair + 1]
        mine = by_group[side].at[which, grp, :, :span]
        mine[...] = value if fresh else mine[...] + value

    with jax.named_scope("forcew"):
        force_arrived(2)
        for at in range(parts):
            fill_lhs(at, force_all, force_b_ref)
    other_groups = [
        {"grp": (1 - column if across_x else column) * LINE + lax.rem(y + step, LINE)}
        for across_x, step in ((1, 2), (0, 2), (1, 1), (1, 3), (0, 1), (0, 3), (1, 0))
    ]
    other_ranks = [rank_device(lax.rem(rank + step, ranks)) for step in (2, 1, 3)]
    other_sets = [
        device(half_at, z_at, core_at)
        for half_at in (1 - half, half)
        for z_at in (z + 1 - 2 * parity, z)
        for core_at in (1 - core, core)
    ][:-1]

    def gather(slots, which, size, me, peers):
        send, recv = gather_send.at[which], gather_recv.at[which]
        for peer in peers:
            remote(slots.at[me], slots.at[me], send, recv, peer).start()
        others = slots.at[pl.ds(0, size - 1)]

        def finish():
            remote(others, others, send, recv, sibling).wait()

        return finish

    def gather_shards():
        send, recv = gather_send.at[12], gather_recv.at[12]
        for far in sorted(range(depth), key=lambda apart: -min(apart, depth - apart)):
            for half_at in (1 - half, half):
                for core_at in (1 - core, core):
                    if far or half_at is not half or core_at is not core:
                        where = device(half_at, lax.rem(z + far, depth), core_at)
                        remote(by_shard.at[smp], by_shard.at[smp], send, recv, where).start()
        others = by_shard.at[pl.ds(0, shards - 1)]

        def finish():
            remote(others, others, send, recv, sibling).wait()

        return finish

    def wide(x, lanes=128):
        return jnp.broadcast_to(x, (1, lanes))

    def send_groups(which, side):
        return gather(by_group[side].at[which], 2 * which + side, groups, grp, other_groups)

    def send_ranks(which, side):
        mine = by_group[side][which, 0]
        for source in range(1, groups):
            mine = mine + by_group[side][which, source]
        by_rank[side][which, rank] = mine
        return gather(by_rank[side].at[which], 4 + 2 * which + side, ranks, rank, other_ranks)

    def sum_ranks(which, side):
        whole = by_rank[side][which, 0]
        for source in range(1, ranks):
            whole = whole + by_rank[side][which, source]
        return whole

    def gather_sets(which, first, second):
        by_set[which, member] = jnp.concatenate([wide(first, 64), wide(second, 64)], axis=1)
        return gather(by_set.at[which], 8 + which, SETS, member, other_sets)

    def set_sum(which, row):
        value = by_set[which, 0]
        for source in range(1, SETS):
            value = value + by_set[which, source]
        return value[:, 64 * row : 64 * row + 1]

    def own_force(at):
        return force_all[at, core, parity, half]

    force_dot = total(force_b_ref[...] * force_b_ref[...]) / shards
    for at in range(parts):
        force_dot = force_dot + total(own_force(at) * own_force(at))
    def of_hidden(left, at):
        return lax.dot_general(
            left[...], hidden[cols_ds(at), :], (((1,), (1,)), ((), ())), preferred_element_type=F32
        )

    def extras(which, first, second):
        by_group[1][which, grp, :, span:] = jnp.concatenate([wide(first), wide(second)], axis=1)

    def own_sum(side):
        return total(by_group[side][0, grp, :, :span])

    with jax.named_scope("values0"):
        values_of(0, 0, parts, 0, True)
        finish_a = send_groups(0, 0)
        extras(0, force_dot, jnp.zeros((1, 1), F32))
        values_of(0, 0, parts, 1, True)
        finish_b = send_groups(0, 1)
    with jax.named_scope("redg"):
        by_shard[smp] = wide(own_sum(0) + own_sum(1))
        finish_shards = gather_shards()

        def plain_part(at, carry):
            plain[at] = of_hidden(spins, at)
            return carry

        lax.fori_loop(0, parts - 1, plain_part, 0)
        finish_a()
        finish_ranks_a = send_ranks(0, 0)
        finish_b()
        finish_ranks_b = send_ranks(0, 1)
        lax.fori_loop(parts - 1, parts, plain_part, 0)
    with jax.named_scope("shards"):
        finish_shards()
        mine = by_shard[0]
        for source in range(1, shards):
            mine = mine + by_shard[source]
        by_total[grp] = mine
        finish_total = gather(by_total, 13, groups, grp, other_groups)
    with jax.named_scope("redr"):
        finish_ranks_a()
        finish_ranks_b()
        sums = [sum_ranks(0, side) for side in range(2)]
        own_dot = sums[1][:, span : span + 1]
        mean_own = (total(sums[0][:, :span]) + total(sums[1][:, :span])) / samples
        centred = [whole[:, :span] - mean_own for whole in sums]
    with jax.named_scope("scaled"):
        for at in range(0, samples, 512):
            weights = centred[at // span][:, at % span : at % span + 512]
            scaled[:pair, at : at + 512] = (spins[:pair, at : at + 512].astype(F32) * weights).astype(BF16)
            scaled[pair:, at : at + 512] = jnp.concatenate(
                [weights, jnp.zeros((PAD - 1, 512), F32)], axis=0
            ).astype(BF16)

    def outer(at):
        return (x_partner, z_partner, half) if at % 2 == 0 else (z_partner, x_partner, parity)

    def pick(ref, at, which):
        return ref.at[:, which] if at % 2 == 0 else ref.at[which]

    def core_copy(at):
        return remote(image.at[at, 1 - core], image_core.at[at], image_send.at[0], image_recv.at[at, 0], sibling)

    def image_copy(at, which):
        far, near, place = outer(at)
        ours = pick(image_all.at[at, core], at, place)
        theirs = pick(image_all.at[at, core], at, 1 - place)
        source, target, where = (
            None,
            (pick(image.at[at, core], at, 1 - place), image_z.at[at], far),
            (pick(image.at[at, core], at, place), image_x.at[at], near),
            (ours, ours, far),
            (ours, ours, sibling),
            (theirs, theirs, sibling),
        )[which]
        return remote(source, target, image_send.at[which], image_recv.at[at, min(which, 4)], where)

    def image_arrived(at, which):
        place = outer(at)[2]
        target = (
            image_core.at[at], image_z.at[at], image_x.at[at],
            pick(image_all.at[at, core], at, 1 - place),
            image_all.at[at, 1 - core],
        )[which]
        remote(target, target, image_send.at[which], image_recv.at[at, which], sibling).wait_recv()

    per = PART // PIECE

    def image_part(at, carry):
        part = of_hidden(scaled, at)
        for to in range(SETS):
            for which in range(per):
                image[per * at + which, to // 4, to // 2 % 2, to % 2] = part[
                    to * rows : (to + 1) * rows, which * PIECE : (which + 1) * PIECE
                ]
        image_b[member, :, cols_ds(at)] = part[pair : pair + 1]
        return carry

    def shifted(at):
        for which in range(per):
            for to in range(SETS):
                block = image.at[per * at + which, to // 4, to // 2 % 2, to % 2]
                block[...] = block[...] + shift * plain[
                    at, to * rows : (to + 1) * rows, which * PIECE : (which + 1) * PIECE
                ]
            core_copy(per * at + which).start()
        image_b[member, :, cols_ds(at)] = image_b[member, :, cols_ds(at)] + shift * plain[at, pair : pair + 1]

    def sum_core(at):
        place = outer(at)[2]
        image_arrived(at, 0)
        theirs = pick(image.at[at, core], at, 1 - place)
        theirs[...] = theirs[...] + pick(image_core.at[at], at, 1 - place)[...]
        image_copy(at, 1).start()
        ours = pick(image.at[at, core], at, place)
        ours[...] = ours[...] + pick(image_core.at[at], at, place)[...]

    def sum_outer(at):
        image_arrived(at, 1)
        ours = pick(image.at[at, core], at, outer(at)[2])
        ours[...] = ours[...] + image_z[at]
        image_copy(at, 2).start()

    def sum_inner(at):
        image_arrived(at, 2)
        place = outer(at)[2]
        pick(image_all.at[at, core], at, place)[...] = pick(image.at[at, core], at, place)[...] + image_x[at]
        image_copy(at, 3).start()
        image_copy(at, 4).start()

    def share(at):
        image_arrived(at, 3)
        image_copy(at, 5).start()

    def image_ready(at):
        image_arrived(at, 4)
        fill_lhs(at, image_all, image_b[0])

    def named(name, step, *at):
        with jax.named_scope(name):
            step(*at)

    with jax.named_scope("image"):
        lax.fori_loop(0, 2, image_part, 0)
    with jax.named_scope("mean"):
        finish_total()
        mean0 = by_total[0]
        for source in range(1, groups):
            mean0 = mean0 + by_total[source]
        shift = mean_own - mean0[:, :1] / count
        shifted(0)
        shifted(1)
        moment = total(centred[0] * centred[0]) + total(centred[1] * centred[1]) + samples * shift * shift
        finish_moment = gather_sets(0, moment, own_dot)

    def image_step(at, carry):
        image_part(at, 0)
        shifted(at)

        @pl.when(at == 2)
        def _():
            for piece in range(2 * per):
                sum_core(piece)

        return carry

    with jax.named_scope("image"):
        lax.fori_loop(2, parts, image_step, 0)
    finish_bias = gather(image_b, 11, SETS, member, other_sets)
    turns = [at ^ 1 for at in range(pieces)]
    for at in range(2 * per, pieces):
        named("core", sum_core, at)
    for at in turns:
        named("outer", sum_outer, at)
    with jax.named_scope("bias"):
        finish_moment()
        finish_bias()
        norm0 = set_sum(0, 1)
        step0 = norm0 / (set_sum(0, 0) / count + diag_shift * norm0)
        keep = 1.0 - diag_shift * step0
        pull = step0 / count
        whole_b = image_b[0]
        for source in range(1, SETS):
            whole_b = whole_b + image_b[source]
        image_b[0] = whole_b
    for at in range(pieces):
        named("inner", sum_inner, at)
    with jax.named_scope("norm"):
        residual_b = keep * force_b_ref[...] - pull * whole_b
        own_norm = total(residual_b * residual_b) / shards
        own_cross = total(residual_b * force_b_ref[...]) / shards
        image_b_ref[0:1, :] = whole_b
        image_b_ref[1:2, :] = force_b_ref[...]
        for at in range(parts):
            own_ref[:, cols_of(at)] = own_force(at)
        for at in range(pieces):
            image_ref[:, at * PIECE : (at + 1) * PIECE] = image_all[at, core, parity, half]
        residual = keep * own_ref[...] - pull * image_ref[...]
        own_norm = own_norm + total(residual * residual)
        own_cross = own_cross + total(residual * own_ref[...])
        finish_norm = gather_sets(1, own_norm, own_cross)
    near, last = turns[: pieces // 2], turns[pieces // 2 :]
    for at in near:
        named("share", share, at)
    for at in near[:2]:
        named("ready", image_ready, at)
    for at in last[:2]:
        named("share", share, at)
    for at in near[2:]:
        named("ready", image_ready, at)
    with jax.named_scope("values1"):
        values_of(1, 0, 2, 0, True)
    for at in last[2:]:
        named("share", share, at)
    with jax.named_scope("values1"):
        values_of(1, 0, 2, 1, True)
    for at in last:
        named("ready", image_ready, at)
    named("fnorm", finish_norm)
    extras(1, set_sum(1, 0), set_sum(1, 1))
    with jax.named_scope("values1"):
        values_of(1, 2, 4, 0, False)
        finish_a = send_groups(1, 0)
        values_of(1, 2, 4, 1, False)
        finish_b = send_groups(1, 1)
    with jax.named_scope("redg"):
        finish_a()
        finish_ranks_a = send_ranks(1, 0)
        finish_b()
        finish_ranks_b = send_ranks(1, 1)
    with jax.named_scope("redr"):
        finish_ranks_a()
        finish_ranks_b()
        sums = [sum_ranks(1, side) for side in range(2)]
        norm1, cross = sums[1][:, span : span + 1], sums[1][:, span + 128 : span + 129]
    beta = norm1 / norm0
    with jax.named_scope("sets"):
        values1 = [(keep + beta) * (centred[side] + shift) - pull * sums[side][:, :span] for side in range(2)]
        mean1 = (total(values1[0]) + total(values1[1])) / samples
        values1 = [value - mean1 for value in values1]
        gather_sets(2, mean1, total(values1[0] * values1[0]) + total(values1[1] * values1[1]))()
        middle = set_sum(2, 0) / SETS
        spread = jnp.zeros((1, 1), F32)
        for source in range(SETS):
            shift = by_set[2, source][:, :1] - middle
            spread = spread + shift * shift
        variance1 = (set_sum(2, 1) + samples * spread) / count
    direction_dot = norm1 + 2.0 * beta * cross + beta * beta * norm0
    step1 = norm1 / (variance1 + diag_shift * direction_dot)

    for_force = step0 + step1 * (keep + beta)
    for_image = step1 * pull
    scale_ref[...] = jnp.concatenate([wide(for_force), wide(for_image), jnp.zeros((6, 128), F32)], axis=0)
    with jax.named_scope("out"):
        pieces = packed.at[rank, pl.ds(0, LINE - 1)]
        remote(pieces, pieces, spin_send.at[0], spin_recv.at[0], sibling).wait_send()
        for slot in range(3):
            remote(pieces, pieces, pass_send.at[slot], spin_recv.at[0], sibling).wait_send()
        for which in range(5):
            force_copy(which).wait_send()
        for which in range(6):
            blocks = image_core if which == 0 else image_z
            remote(blocks, blocks, image_send.at[which], spin_recv.at[0], sibling).wait_send()


def finish_kernel(image_ref, image_b_ref, force_ref, scale_ref, out_ref, out_b_ref):
    for_force, for_image = scale_ref[0:1, 0:1], scale_ref[1:2, 0:1]
    out_ref[...] = for_force * force_ref[...] - for_image * image_ref[...]
    out_b_ref[...] = for_force * image_b_ref[1:2, :] - for_image * image_b_ref[0:1, :]


def body(groups, shards, spins_packed, weight, hidden_bias, force_w, force_b):
    words, here = spins_packed.shape
    inputs, units = weight.shape
    rows = force_w.shape[0]
    ranks = shards // SETS
    samples, pair = ranks * here, SETS * rows
    parts, pieces = units // PART, units // PIECE
    quarter = here // LINE
    vmem = pl.BlockSpec(memory_space=pltpu.VMEM)
    anywhere = pl.BlockSpec(memory_space=pl.ANY)
    dma = pltpu.SemaphoreType.DMA
    results = pl.pallas_call(
        functools.partial(kernel, groups, shards),
        out_shape=(
            pltpu.VMEM((rows, units), F32), pltpu.VMEM((8, units), F32),
            pltpu.VMEM((rows, units), F32), pltpu.VMEM((8, 128), F32),
        ),
        in_specs=[anywhere] * 5,
        out_specs=(vmem,) * 4,
        scratch_shapes=[
            pltpu.VMEM((ranks, LINE, words, quarter), jnp.int32),
            pltpu.VMEM((inputs, units), BF16),
            pltpu.VMEM((units, inputs), BF16),
            pltpu.VMEM((1, units), F32),
            pltpu.VMEM((units, 128), F32),
            pltpu.VMEM((1, units), F32),
            pltpu.VMEM((inputs, 2 * quarter), BF16),
            pltpu.VMEM((pair + PAD, samples), BF16),
            pltpu.VMEM((units, samples), BF16),
            pltpu.VMEM((parts, 2, 2, 2, rows, PART), F32),
            pltpu.VMEM((pair + PAD, units), BF16),
            pltpu.VMEM((pair + PAD, samples), BF16),
            pltpu.VMEM((parts, pair + PAD, PART), F32),
            pltpu.VMEM((pieces, 2, 2, 2, rows, PIECE), F32),
            pltpu.VMEM((pieces, 2, 2, rows, PIECE), F32),
            pltpu.VMEM((pieces, 2, rows, PIECE), F32),
            pltpu.VMEM((pieces, 2, rows, PIECE), F32),
            pltpu.VMEM((pieces, 2, 2, 2, rows, PIECE), F32),
            pltpu.VMEM((SETS, 1, units), F32),
            pltpu.VMEM((2, groups, 1, samples // 2), F32),
            pltpu.VMEM((2, groups, 1, samples // 2 + EXTRA), F32),
            pltpu.VMEM((2, ranks, 1, samples // 2), F32),
            pltpu.VMEM((2, ranks, 1, samples // 2 + EXTRA), F32),
            pltpu.VMEM((3, SETS, 1, 128), F32),
            pltpu.VMEM((shards, 1, 128), F32),
            pltpu.VMEM((groups, 1, 128), F32),
            dma((5,)),
            dma((1,)),
            dma((ranks,)),
            dma((3,)),
            dma((ranks, LINE)),
            dma((5,)),
            dma((3,)),
            dma((6,)),
            dma((pieces, 5)),
            dma((14,)),
            dma((14,)),
        ],
        compiler_params=pltpu.CompilerParams(
            collective_id=0, has_side_effects=True, vmem_limit_bytes=62 * 1024 * 1024
        ),
    )(spins_packed, weight, hidden_bias.reshape(1, -1), force_w, force_b.reshape(1, -1))
    update_w, update_b = pl.pallas_call(
        finish_kernel,
        out_shape=(jax.ShapeDtypeStruct((rows, units), F32), jax.ShapeDtypeStruct((1, units), F32)),
        in_specs=[vmem] * 4,
        out_specs=(vmem, vmem),
    )(*[pltpu.with_memory_space_constraint(result, pltpu.VMEM) for result in results])
    return update_w, update_b.reshape(-1)


def solution(mesh):
    placed = (P(None, "smp"), P(None, "grp"), P("grp"), P("smp", "grp"), P("grp"))
    return jax.shard_map(
        functools.partial(body, mesh.shape["grp"], mesh.shape["smp"]),
        mesh=mesh, in_specs=placed, out_specs=(P("smp", "grp"), P("grp")), check_vma=False,
    )
```

```python
import functools

import jax
import jax.numpy as jnp
from jax import lax
from jax.experimental import pallas as pl
from jax.experimental.pallas import tpu as pltpu
from jax.sharding import PartitionSpec as P

MESH = pl.DeviceIdType.MESH
F32, BF16 = jnp.float32, jnp.bfloat16
diag_shift = 0.01
SETS = 8
EXTRA = 256
PAD = 16
PART = 256
PIECE = 128
LINE = 4


def total(x):
    return jnp.sum(jnp.sum(x, axis=0, keepdims=True), axis=1, keepdims=True)


def kernel(
    groups, shards,
    packed_in, weight_in, bias_in, force_in, force_b_in,
    image_ref, image_b_ref, own_ref, scale_ref,
    packed, weight, weight_t, bias_ref, bias_t, force_b_ref, tile, spins, hidden, force_all, lhs, scaled, plain,
    image, image_core, image_z, image_x, image_all, image_b, by_group_a, by_group_b, by_rank_a, by_rank_b, by_set, by_shard, by_total,
    load, spin_send, spin_recv, pass_send, pass_recv, force_send, force_recv, image_send, image_recv,
    gather_send, gather_recv,
):
    grp, smp = lax.axis_index("grp"), lax.axis_index("smp")
    words, here = packed_in.shape
    inputs, units = weight.shape
    rows = force_in.shape[0]
    ranks = shards // SETS
    pair = SETS * rows
    samples = ranks * here
    count = samples * SETS
    quarter = here // LINE
    parts = units // PART
    pieces = units // PIECE
    depth = 2 * ranks

    core, z, half = lax.rem(smp, 2), lax.rem(smp // 2, depth), smp // (2 * depth)
    parity, rank = lax.rem(z, 2), z // 2
    member = (core * 2 + parity) * 2 + half
    y, column = lax.rem(grp, LINE), grp // LINE

    def device(half_at, z_at, core_at):
        return {"smp": (half_at * depth + z_at) * 2 + core_at}

    sibling = device(half, z, 1 - core)
    z_partner = device(half, z + 1 - 2 * parity, core)
    x_partner = device(1 - half, z, core)

    def group_device(at):
        return {"grp": at}

    def line_device(at):
        return {"grp": column * LINE + at}

    def rank_device(at):
        return device(half, 2 * at + parity, core)

    def remote(source, target, send, recv, where):
        return pltpu.make_async_remote_copy(
            source, target, send, recv, device_id=where, device_id_type=MESH
        )

    barrier = pltpu.get_barrier_semaphore()
    greeted = [line_device(lax.rem(y + step, LINE)) for step in range(1, LINE)]
    greeted += [group_device((1 - column) * LINE + y), sibling, z_partner, x_partner]
    greeted += [rank_device(lax.rem(rank + step, ranks)) for step in (1, ranks - 1)]
    for where in greeted:
        pl.semaphore_signal(barrier, device_id=where, device_id_type=MESH)

    def cols_of(at):
        return slice(at * PART, (at + 1) * PART)

    def cols_ds(at):
        return pl.ds(pl.multiple_of(at * PART, PART), PART)

    copies = []
    for at in range(LINE):
        copies.append(
            pltpu.make_async_copy(packed_in.at[:, pl.ds(at * quarter, quarter)], packed.at[rank, at], load.at[3])
        )
    for at in range(parts):
        copies.append(
            pltpu.make_async_copy(force_in.at[:, cols_ds(at)], force_all.at[at, core, parity, half], load.at[4])
        )
    later = [
        pltpu.make_async_copy(weight_in, weight, load.at[0]),
        pltpu.make_async_copy(bias_in, bias_ref, load.at[1]),
        pltpu.make_async_copy(force_b_in, force_b_ref, load.at[2]),
    ]
    for copy in copies + later:
        copy.start()
    pltpu.make_async_copy(packed.at[rank], packed.at[rank], load.at[3]).wait()
    blocks = force_all.at[:, core, parity, half]
    pltpu.make_async_copy(blocks, blocks, load.at[4]).wait()

    def turn(at, carry):
        cols = pl.ds(pl.multiple_of(at * 256, 256), 256)
        weight_t[cols, :] = weight[:, cols].T
        bias_t[cols, :] = jnp.broadcast_to(bias_ref[:, cols], (128, 256)).T
        return carry

    after, before, across = lax.rem(rank + 1, ranks), lax.rem(rank + ranks - 1, ranks), lax.rem(rank + 2, ranks)

    def force_copy(which):
        source, recv, where = (
            (force_all.at[:, core, parity, half], 0, z_partner),
            (force_all.at[:, core, parity, half], 1, x_partner),
            (force_all.at[:, core, parity, 1 - half], 0, z_partner),
            (force_all.at[:, core, parity], 2, sibling),
            (force_all.at[:, core, 1 - parity], 2, sibling),
        )[which]
        return remote(source, source, force_send.at[which], force_recv.at[recv], where)

    def force_arrived(which):
        target = (
            force_all.at[:, core, 1 - parity], force_all.at[:, core, parity, 1 - half], force_all.at[:, 1 - core]
        )[which]
        remote(target, target, force_send.at[which], force_recv.at[which], sibling).wait_recv()

    def spin_send_to(step):
        own = packed.at[rank, y]
        return remote(own, own, spin_send.at[0], spin_recv.at[rank], rank_device(lax.rem(rank + step, ranks)))

    def spin_arrived(source):
        target = packed.at[source, y]
        remote(target, target, spin_send.at[0], spin_recv.at[source], sibling).wait_recv()

    def hand_on(source, slot):
        for step in (1, 3, 2):
            piece = packed.at[source, y]
            remote(
                piece, piece, pass_send.at[slot], pass_recv.at[source, y], line_device(lax.rem(y + step, LINE))
            ).start()

    def handed(source, step):
        from_y = lax.rem(y + step, LINE)
        target = packed.at[source, from_y]
        remote(target, target, pass_send.at[0], pass_recv.at[source, from_y], sibling).wait_recv()
        return source, from_y

    masks = jnp.left_shift(1, lax.broadcasted_iota(jnp.int32, (32, quarter), 0))

    def places(tiles):
        return [pl.ds(pl.multiple_of(source * here + at * quarter, quarter), quarter) for source, at in tiles]

    def unpack(tiles):
        cols = places(tiles)
        for which, (source, at) in enumerate(tiles):
            to = slice(which * quarter, (which + 1) * quarter)
            for word in range(words):
                bits = jnp.bitwise_and(jnp.broadcast_to(packed[source, at, word : word + 1, :], (32, quarter)), masks)
                tile[word * 32 : word * 32 + 32, to] = jnp.where(bits != 0, 1.0, -1.0).astype(BF16)
        for to in range(SETS):
            word = (to % 2) * 2 * depth + 4 * rank + 2 * (to // 2 % 2) + to // 4
            from_rows = pl.ds(pl.multiple_of(word * rows, rows), rows)
            for which in range(2):
                spins[to * rows : (to + 1) * rows, cols[which]] = tile[
                    from_rows, which * quarter : (which + 1) * quarter
                ]

    def activate(tiles):
        cols = places(tiles)
        for unit in range(0, units, 1024):
            these = pl.ds(unit, 1024)
            pre = jnp.dot(weight_t[these, :], tile[...], preferred_element_type=F32)
            pre = pre + jnp.concatenate([bias_t[these, :]] * (2 * quarter // 128), axis=1)
            result = jnp.tanh(pre).astype(BF16)
            for which in range(2):
                hidden[these, cols[which]] = result[:, which * quarter : (which + 1) * quarter]

    def hidden_of(*tiles):
        unpack(tiles)
        activate(tiles)

    with jax.named_scope("barrier"):
        pl.semaphore_wait(barrier, len(greeted))
    force_copy(1).start()
    for step in (1, ranks - 1):
        spin_send_to(step).start()
    force_copy(0).start()

    spins[pair:, :] = (lax.broadcasted_iota(jnp.int32, (PAD, samples), 0) == 0).astype(F32).astype(BF16)
    with jax.named_scope("turn"):
        for copy in later:
            copy.wait()
        lax.fori_loop(0, units // 256, turn, 0)
    with jax.named_scope("hidden0"):
        hidden_of((rank, 0), (rank, 1))
        hidden_of((rank, 2), (rank, 3))
    with jax.named_scope("spinab"):
        spin_arrived(before)
        relayed = packed.at[before, y]
        remote(relayed, relayed, spin_send.at[0], spin_recv.at[before], rank_device(after)).start()
        hand_on(before, 0)
        spin_arrived(after)
        hand_on(after, 1)
    with jax.named_scope("hidden1"):
        hidden_of((before, y), (after, y))
    with jax.named_scope("spinc"):
        spin_arrived(across)
        hand_on(across, 2)
        force_arrived(1)
        force_copy(2).start()
        force_copy(3).start()
        tiles = (across, y), handed(before, 3)
    with jax.named_scope("hidden2"):
        hidden_of(*tiles)
    with jax.named_scope("wait"):
        tiles = handed(after, 3), handed(before, 1), handed(after, 1), handed(before, 2)
    with jax.named_scope("hidden3"):
        hidden_of(*tiles[:2])
        hidden_of(*tiles[2:])
    with jax.named_scope("wait"):
        force_arrived(0)
        force_copy(4).start()
        tiles = handed(after, 2), handed(across, 1), handed(across, 3), handed(across, 2)
    with jax.named_scope("hidden4"):
        hidden_of(*tiles[:2])
        hidden_of(*tiles[2:])

    span = samples // 2
    by_group, by_rank = (by_group_a, by_group_b), (by_rank_a, by_rank_b)

    def fill_lhs(at, slots, row):
        width = slots.shape[-1]
        cols = slice(at * width, (at + 1) * width)
        for to in range(SETS):
            lhs[to * rows : (to + 1) * rows, cols] = slots[at, to // 4, to // 2 % 2, to % 2].astype(BF16)
        lhs[pair:, cols] = jnp.concatenate(
            [row[:, cols] / ranks, jnp.zeros((PAD - 1, width), F32)], axis=0
        ).astype(BF16)

    def values_of(which, first, last, side, fresh):
        these, cols = slice(first * PART, last * PART), slice(side * span, (side + 1) * span)
        product = jnp.dot(lhs[:, these], hidden[these, cols], preferred_element_type=F32)
        value = jnp.sum(product[:pair] * spins[:pair, cols].astype(F32), axis=0, keepdims=True) + product[pair : pair + 1]
        mine = by_group[side].at[which, grp, :, :span]
        mine[...] = value if fresh else mine[...] + value

    with jax.named_scope("forcew"):
        force_arrived(2)
        for at in range(parts):
            fill_lhs(at, force_all, force_b_ref)
    other_groups = [group_device(lax.rem(grp + step, groups)) for step in range(1, groups)]
    other_ranks = [rank_device(lax.rem(rank + step, ranks)) for step in range(1, ranks)]
    other_sets = [
        device(half_at, z_at, core_at)
        for core_at in (core, 1 - core)
        for z_at in (z, z + 1 - 2 * parity)
        for half_at in (half, 1 - half)
    ][1:]

    def gather(slots, which, size, me, peers):
        send, recv = gather_send.at[which], gather_recv.at[which]
        for peer in peers:
            remote(slots.at[me], slots.at[me], send, recv, peer).start()
        others = slots.at[pl.ds(0, size - 1)]

        def finish():
            remote(others, others, send, recv, sibling).wait()

        return finish

    def gather_shards():
        send, recv = gather_send.at[12], gather_recv.at[12]
        for far in sorted(range(depth), key=lambda apart: -min(apart, depth - apart)):
            for half_at in (1 - half, half):
                for core_at in (1 - core, core):
                    if far or half_at is not half or core_at is not core:
                        where = device(half_at, lax.rem(z + far, depth), core_at)
                        remote(by_shard.at[smp], by_shard.at[smp], send, recv, where).start()
        others = by_shard.at[pl.ds(0, shards - 1)]

        def finish():
            remote(others, others, send, recv, sibling).wait()

        return finish

    def wide(x, lanes=128):
        return jnp.broadcast_to(x, (1, lanes))

    def send_groups(which, side):
        return gather(by_group[side].at[which], 2 * which + side, groups, grp, other_groups)

    def send_ranks(which, side):
        mine = by_group[side][which, 0]
        for source in range(1, groups):
            mine = mine + by_group[side][which, source]
        by_rank[side][which, rank] = mine
        return gather(by_rank[side].at[which], 4 + 2 * which + side, ranks, rank, other_ranks)

    def sum_ranks(which, side):
        whole = by_rank[side][which, 0]
        for source in range(1, ranks):
            whole = whole + by_rank[side][which, source]
        return whole

    def gather_sets(which, first, second):
        by_set[which, member] = jnp.concatenate([wide(first), wide(second), jnp.zeros((6, 128), F32)], axis=0)
        return gather(by_set.at[which], 8 + which, SETS, member, other_sets)

    def set_sum(which, row):
        value = by_set[which, 0, row : row + 1, :]
        for source in range(1, SETS):
            value = value + by_set[which, source, row : row + 1, :]
        return value[:, :1]

    def own_force(at):
        return force_all[at, core, parity, half]

    force_dot = total(force_b_ref[...] * force_b_ref[...]) / shards
    for at in range(parts):
        force_dot = force_dot + total(own_force(at) * own_force(at))
    def of_hidden(left, at):
        return lax.dot_general(
            left[...], hidden[cols_ds(at), :], (((1,), (1,)), ((), ())), preferred_element_type=F32
        )

    def extras(which, first, second):
        by_group[1][which, grp, :, span:] = jnp.concatenate([wide(first), wide(second)], axis=1)

    def own_sum(side):
        return total(by_group[side][0, grp, :, :span])

    with jax.named_scope("values0"):
        values_of(0, 0, parts, 0, True)
        finish_a = send_groups(0, 0)
        extras(0, force_dot, jnp.zeros((1, 1), F32))
        values_of(0, 0, parts, 1, True)
        finish_b = send_groups(0, 1)
    with jax.named_scope("redg"):
        by_shard[smp] = wide(own_sum(0) + own_sum(1))
        finish_shards = gather_shards()

        def plain_part(at, carry):
            plain[at] = of_hidden(spins, at)
            return carry

        lax.fori_loop(0, 1, plain_part, 0)
        finish_a()
        finish_ranks_a = send_ranks(0, 0)
        finish_b()
        finish_ranks_b = send_ranks(0, 1)
        lax.fori_loop(1, 2, plain_part, 0)
    with jax.named_scope("shards"):
        finish_shards()
        mine = by_shard[0]
        for source in range(1, shards):
            mine = mine + by_shard[source]
        by_total[grp] = mine
        finish_total = gather(by_total, 13, groups, grp, other_groups)
    with jax.named_scope("redr"):
        lax.fori_loop(2, parts, plain_part, 0)
        finish_ranks_a()
        finish_ranks_b()
        sums = [sum_ranks(0, side) for side in range(2)]
        own_dot = sums[1][:, span : span + 1]
        mean_own = (total(sums[0][:, :span]) + total(sums[1][:, :span])) / samples
        centred = [whole[:, :span] - mean_own for whole in sums]
    with jax.named_scope("scaled"):
        for at in range(0, samples, 512):
            weights = centred[at // span][:, at % span : at % span + 512]
            scaled[:pair, at : at + 512] = (spins[:pair, at : at + 512].astype(F32) * weights).astype(BF16)
            scaled[pair:, at : at + 512] = jnp.concatenate(
                [weights, jnp.zeros((PAD - 1, 512), F32)], axis=0
            ).astype(BF16)

    def outer(at):
        return (x_partner, z_partner, half) if at % 2 == 0 else (z_partner, x_partner, parity)

    def pick(ref, at, which):
        return ref.at[:, which] if at % 2 == 0 else ref.at[which]

    def core_copy(at):
        return remote(image.at[at, 1 - core], image_core.at[at], image_send.at[0], image_recv.at[at, 0], sibling)

    def image_copy(at, which):
        far, near, place = outer(at)
        ours = pick(image_all.at[at, core], at, place)
        theirs = pick(image_all.at[at, core], at, 1 - place)
        source, target, where = (
            None,
            (pick(image.at[at, core], at, 1 - place), image_z.at[at], far),
            (pick(image.at[at, core], at, place), image_x.at[at], near),
            (ours, ours, far),
            (ours, ours, sibling),
            (theirs, theirs, sibling),
        )[which]
        return remote(source, target, image_send.at[which], image_recv.at[at, min(which, 4)], where)

    def image_arrived(at, which):
        place = outer(at)[2]
        target = (
            image_core.at[at], image_z.at[at], image_x.at[at],
            pick(image_all.at[at, core], at, 1 - place),
            image_all.at[at, 1 - core],
        )[which]
        remote(target, target, image_send.at[which], image_recv.at[at, which], sibling).wait_recv()

    per = PART // PIECE

    def image_part(at, carry):
        part = of_hidden(scaled, at)
        for to in range(SETS):
            for which in range(per):
                image[per * at + which, to // 4, to // 2 % 2, to % 2] = part[
                    to * rows : (to + 1) * rows, which * PIECE : (which + 1) * PIECE
                ]
        image_b[member, :, cols_ds(at)] = part[pair : pair + 1]
        return carry

    def shifted(at):
        for which in range(per):
            for to in range(SETS):
                block = image.at[per * at + which, to // 4, to // 2 % 2, to % 2]
                block[...] = block[...] + shift * plain[
                    at, to * rows : (to + 1) * rows, which * PIECE : (which + 1) * PIECE
                ]
            core_copy(per * at + which).start()
        image_b[member, :, cols_ds(at)] = image_b[member, :, cols_ds(at)] + shift * plain[at, pair : pair + 1]

    def sum_core(at):
        place = outer(at)[2]
        image_arrived(at, 0)
        theirs = pick(image.at[at, core], at, 1 - place)
        theirs[...] = theirs[...] + pick(image_core.at[at], at, 1 - place)[...]
        image_copy(at, 1).start()
        ours = pick(image.at[at, core], at, place)
        ours[...] = ours[...] + pick(image_core.at[at], at, place)[...]

    def sum_outer(at):
        image_arrived(at, 1)
        ours = pick(image.at[at, core], at, outer(at)[2])
        ours[...] = ours[...] + image_z[at]
        image_copy(at, 2).start()

    def sum_inner(at):
        image_arrived(at, 2)
        place = outer(at)[2]
        pick(image_all.at[at, core], at, place)[...] = pick(image.at[at, core], at, place)[...] + image_x[at]
        image_copy(at, 3).start()
        image_copy(at, 4).start()

    def share(at):
        image_arrived(at, 3)
        image_copy(at, 5).start()

    def image_ready(at):
        image_arrived(at, 4)
        fill_lhs(at, image_all, image_b[0])

    def named(name, step, *at):
        with jax.named_scope(name):
            step(*at)

    with jax.named_scope("image"):
        lax.fori_loop(0, 2, image_part, 0)
    with jax.named_scope("mean"):
        finish_total()
        mean0 = by_total[0]
        for source in range(1, groups):
            mean0 = mean0 + by_total[source]
        shift = mean_own - mean0[:, :1] / count
        shifted(0)
        shifted(1)
        moment = total(centred[0] * centred[0]) + total(centred[1] * centred[1]) + samples * shift * shift
        finish_moment = gather_sets(0, moment, own_dot)

    def image_step(at, carry):
        image_part(at, 0)
        shifted(at)

        @pl.when(at == 2)
        def _():
            for piece in range(2 * per):
                sum_core(piece)

        return carry

    with jax.named_scope("image"):
        lax.fori_loop(2, parts, image_step, 0)
    finish_bias = gather(image_b, 11, SETS, member, other_sets)
    turns = [at ^ 1 for at in range(pieces)]
    for at in range(2 * per, pieces):
        named("core", sum_core, at)
    for at in turns:
        named("outer", sum_outer, at)
    with jax.named_scope("bias"):
        finish_moment()
        finish_bias()
        norm0 = set_sum(0, 1)
        step0 = norm0 / (set_sum(0, 0) / count + diag_shift * norm0)
        keep = 1.0 - diag_shift * step0
        pull = step0 / count
        whole_b = image_b[0]
        for source in range(1, SETS):
            whole_b = whole_b + image_b[source]
        image_b[0] = whole_b
    for at in range(pieces):
        named("inner", sum_inner, at)
    with jax.named_scope("norm"):
        residual_b = keep * force_b_ref[...] - pull * whole_b
        own_norm = total(residual_b * residual_b) / shards
        own_cross = total(residual_b * force_b_ref[...]) / shards
        image_b_ref[0:1, :] = whole_b
        image_b_ref[1:2, :] = force_b_ref[...]
        for at in range(parts):
            own_ref[:, cols_of(at)] = own_force(at)
        for at in range(pieces):
            image_ref[:, at * PIECE : (at + 1) * PIECE] = image_all[at, core, parity, half]
        residual = keep * own_ref[...] - pull * image_ref[...]
        own_norm = own_norm + total(residual * residual)
        own_cross = own_cross + total(residual * own_ref[...])
        finish_norm = gather_sets(1, own_norm, own_cross)
    near, last = turns[: pieces // 2], turns[pieces // 2 :]
    for at in near:
        named("share", share, at)
    for at in near[:2]:
        named("ready", image_ready, at)
    for at in last[:2]:
        named("share", share, at)
    for at in near[2:]:
        named("ready", image_ready, at)
    with jax.named_scope("values1"):
        values_of(1, 0, 2, 0, True)
    for at in last[2:]:
        named("share", share, at)
    with jax.named_scope("values1"):
        values_of(1, 0, 2, 1, True)
    for at in last:
        named("ready", image_ready, at)
    named("fnorm", finish_norm)
    extras(1, set_sum(1, 0), set_sum(1, 1))
    with jax.named_scope("values1"):
        values_of(1, 2, 4, 0, False)
        finish_a = send_groups(1, 0)
        values_of(1, 2, 4, 1, False)
        finish_b = send_groups(1, 1)
    with jax.named_scope("redg"):
        finish_a()
        finish_ranks_a = send_ranks(1, 0)
        finish_b()
        finish_ranks_b = send_ranks(1, 1)
    with jax.named_scope("redr"):
        finish_ranks_a()
        finish_ranks_b()
        sums = [sum_ranks(1, side) for side in range(2)]
        norm1, cross = sums[1][:, span : span + 1], sums[1][:, span + 128 : span + 129]
    beta = norm1 / norm0
    with jax.named_scope("sets"):
        values1 = [(keep + beta) * (centred[side] + shift) - pull * sums[side][:, :span] for side in range(2)]
        mean1 = (total(values1[0]) + total(values1[1])) / samples
        values1 = [value - mean1 for value in values1]
        gather_sets(2, mean1, total(values1[0] * values1[0]) + total(values1[1] * values1[1]))()
        middle = set_sum(2, 0) / SETS
        spread = jnp.zeros((1, 1), F32)
        for source in range(SETS):
            shift = by_set[2, source, 0:1, :1] - middle
            spread = spread + shift * shift
        variance1 = (set_sum(2, 1) + samples * spread) / count
    direction_dot = norm1 + 2.0 * beta * cross + beta * beta * norm0
    step1 = norm1 / (variance1 + diag_shift * direction_dot)

    for_force = step0 + step1 * (keep + beta)
    for_image = step1 * pull
    scale_ref[...] = jnp.concatenate([wide(for_force), wide(for_image), jnp.zeros((6, 128), F32)], axis=0)
    with jax.named_scope("out"):
        pieces = packed.at[rank, pl.ds(0, LINE - 1)]
        remote(pieces, pieces, spin_send.at[0], spin_recv.at[0], sibling).wait_send()
        for slot in range(3):
            remote(pieces, pieces, pass_send.at[slot], spin_recv.at[0], sibling).wait_send()
        for which in range(5):
            force_copy(which).wait_send()
        for which in range(6):
            blocks = image_core if which == 0 else image_z
            remote(blocks, blocks, image_send.at[which], spin_recv.at[0], sibling).wait_send()


def finish_kernel(image_ref, image_b_ref, force_ref, scale_ref, out_ref, out_b_ref):
    for_force, for_image = scale_ref[0:1, 0:1], scale_ref[1:2, 0:1]
    out_ref[...] = for_force * force_ref[...] - for_image * image_ref[...]
    out_b_ref[...] = for_force * image_b_ref[1:2, :] - for_image * image_b_ref[0:1, :]


def body(groups, shards, spins_packed, weight, hidden_bias, force_w, force_b):
    words, here = spins_packed.shape
    inputs, units = weight.shape
    rows = force_w.shape[0]
    ranks = shards // SETS
    samples, pair = ranks * here, SETS * rows
    parts, pieces = units // PART, units // PIECE
    quarter = here // LINE
    vmem = pl.BlockSpec(memory_space=pltpu.VMEM)
    anywhere = pl.BlockSpec(memory_space=pl.ANY)
    dma = pltpu.SemaphoreType.DMA
    results = pl.pallas_call(
        functools.partial(kernel, groups, shards),
        out_shape=(
            pltpu.VMEM((rows, units), F32), pltpu.VMEM((8, units), F32),
            pltpu.VMEM((rows, units), F32), pltpu.VMEM((8, 128), F32),
        ),
        in_specs=[anywhere] * 5,
        out_specs=(vmem,) * 4,
        scratch_shapes=[
            pltpu.VMEM((ranks, LINE, words, quarter), jnp.int32),
            pltpu.VMEM((inputs, units), BF16),
            pltpu.VMEM((units, inputs), BF16),
            pltpu.VMEM((1, units), F32),
            pltpu.VMEM((units, 128), F32),
            pltpu.VMEM((1, units), F32),
            pltpu.VMEM((inputs, 2 * quarter), BF16),
            pltpu.VMEM((pair + PAD, samples), BF16),
            pltpu.VMEM((units, samples), BF16),
            pltpu.VMEM((parts, 2, 2, 2, rows, PART), F32),
            pltpu.VMEM((pair + PAD, units), BF16),
            pltpu.VMEM((pair + PAD, samples), BF16),
            pltpu.VMEM((parts, pair + PAD, PART), F32),
            pltpu.VMEM((pieces, 2, 2, 2, rows, PIECE), F32),
            pltpu.VMEM((pieces, 2, 2, rows, PIECE), F32),
            pltpu.VMEM((pieces, 2, rows, PIECE), F32),
            pltpu.VMEM((pieces, 2, rows, PIECE), F32),
            pltpu.VMEM((pieces, 2, 2, 2, rows, PIECE), F32),
            pltpu.VMEM((SETS, 1, units), F32),
            pltpu.VMEM((2, groups, 1, samples // 2), F32),
            pltpu.VMEM((2, groups, 1, samples // 2 + EXTRA), F32),
            pltpu.VMEM((2, ranks, 1, samples // 2), F32),
            pltpu.VMEM((2, ranks, 1, samples // 2 + EXTRA), F32),
            pltpu.VMEM((3, SETS, 8, 128), F32),
            pltpu.VMEM((shards, 1, 128), F32),
            pltpu.VMEM((groups, 1, 128), F32),
            dma((5,)),
            dma((1,)),
            dma((ranks,)),
            dma((3,)),
            dma((ranks, LINE)),
            dma((5,)),
            dma((3,)),
            dma((6,)),
            dma((pieces, 5)),
            dma((14,)),
            dma((14,)),
        ],
        compiler_params=pltpu.CompilerParams(
            collective_id=0, has_side_effects=True, vmem_limit_bytes=62 * 1024 * 1024
        ),
    )(spins_packed, weight, hidden_bias.reshape(1, -1), force_w, force_b.reshape(1, -1))
    update_w, update_b = pl.pallas_call(
        finish_kernel,
        out_shape=(jax.ShapeDtypeStruct((rows, units), F32), jax.ShapeDtypeStruct((1, units), F32)),
        in_specs=[vmem] * 4,
        out_specs=(vmem, vmem),
    )(*[pltpu.with_memory_space_constraint(result, pltpu.VMEM) for result in results])
    return update_w, update_b.reshape(-1)


def solution(mesh):
    placed = (P(None, "smp"), P(None, "grp"), P("grp"), P("smp", "grp"), P("grp"))
    return jax.shard_map(
        functools.partial(body, mesh.shape["grp"], mesh.shape["smp"]),
        mesh=mesh, in_specs=placed, out_specs=(P("smp", "grp"), P("grp")), check_vma=False,
    )
```

```python
import functools

import jax
import jax.numpy as jnp
from jax import lax
from jax.experimental import pallas as pl
from jax.experimental.pallas import tpu as pltpu
from jax.sharding import PartitionSpec as P

MESH = pl.DeviceIdType.MESH
F32, BF16 = jnp.float32, jnp.bfloat16
diag_shift = 0.01
SETS = 8
EXTRA = 256
PAD = 16
PART = 256
PIECE = 128
LINE = 4


def total(x):
    return jnp.sum(jnp.sum(x, axis=0, keepdims=True), axis=1, keepdims=True)


def kernel(
    groups, shards,
    packed_in, weight_in, bias_in, force_in, force_b_in,
    image_ref, image_b_ref, own_ref, scale_ref,
    packed, weight, weight_t, bias_ref, bias_t, force_b_ref, tile, spins, hidden, force_all, lhs, scaled, plain,
    image, image_core, image_z, image_x, image_all, image_b, by_group_a, by_group_b, by_rank_a, by_rank_b, by_set, by_shard, by_total,
    load, spin_send, spin_recv, pass_send, pass_recv, force_send, force_recv, image_send, image_recv,
    gather_send, gather_recv,
):
    grp, smp = lax.axis_index("grp"), lax.axis_index("smp")
    words, here = packed_in.shape
    inputs, units = weight.shape
    rows = force_in.shape[0]
    ranks = shards // SETS
    pair = SETS * rows
    samples = ranks * here
    count = samples * SETS
    quarter = here // LINE
    parts = units // PART
    pieces = units // PIECE
    depth = 2 * ranks

    core, z, half = lax.rem(smp, 2), lax.rem(smp // 2, depth), smp // (2 * depth)
    parity, rank = lax.rem(z, 2), z // 2
    member = (core * 2 + parity) * 2 + half
    y, column = lax.rem(grp, LINE), grp // LINE

    def device(half_at, z_at, core_at):
        return {"smp": (half_at * depth + z_at) * 2 + core_at}

    sibling = device(half, z, 1 - core)
    z_partner = device(half, z + 1 - 2 * parity, core)
    x_partner = device(1 - half, z, core)

    def group_device(at):
        return {"grp": at}

    def line_device(at):
        return {"grp": column * LINE + at}

    def rank_device(at):
        return device(half, 2 * at + parity, core)

    def remote(source, target, send, recv, where):
        return pltpu.make_async_remote_copy(
            source, target, send, recv, device_id=where, device_id_type=MESH
        )

    barrier = pltpu.get_barrier_semaphore()
    greeted = [line_device(lax.rem(y + step, LINE)) for step in range(1, LINE)]
    greeted += [group_device((1 - column) * LINE + y), sibling, z_partner, x_partner]
    greeted += [rank_device(lax.rem(rank + step, ranks)) for step in (1, ranks - 1)]
    for where in greeted:
        pl.semaphore_signal(barrier, device_id=where, device_id_type=MESH)

    def cols_of(at):
        return slice(at * PART, (at + 1) * PART)

    def cols_ds(at):
        return pl.ds(pl.multiple_of(at * PART, PART), PART)

    copies = []
    for at in range(LINE):
        copies.append(
            pltpu.make_async_copy(packed_in.at[:, pl.ds(at * quarter, quarter)], packed.at[rank, at], load.at[3])
        )
    for at in range(parts):
        copies.append(
            pltpu.make_async_copy(force_in.at[:, cols_ds(at)], force_all.at[at, core, parity, half], load.at[4])
        )
    later = [
        pltpu.make_async_copy(weight_in, weight, load.at[0]),
        pltpu.make_async_copy(bias_in, bias_ref, load.at[1]),
        pltpu.make_async_copy(force_b_in, force_b_ref, load.at[2]),
    ]
    for copy in copies + later:
        copy.start()
    pltpu.make_async_copy(packed.at[rank], packed.at[rank], load.at[3]).wait()
    blocks = force_all.at[:, core, parity, half]
    pltpu.make_async_copy(blocks, blocks, load.at[4]).wait()

    def turn(at, carry):
        cols = pl.ds(pl.multiple_of(at * 256, 256), 256)
        weight_t[cols, :] = weight[:, cols].T
        bias_t[cols, :] = jnp.broadcast_to(bias_ref[:, cols], (128, 256)).T
        return carry

    after, before, across = lax.rem(rank + 1, ranks), lax.rem(rank + ranks - 1, ranks), lax.rem(rank + 2, ranks)

    def force_copy(which):
        source, recv, where = (
            (force_all.at[:, core, parity, half], 0, z_partner),
            (force_all.at[:, core, parity, half], 1, x_partner),
            (force_all.at[:, core, parity, 1 - half], 0, z_partner),
            (force_all.at[:, core, parity], 2, sibling),
            (force_all.at[:, core, 1 - parity], 2, sibling),
        )[which]
        return remote(source, source, force_send.at[which], force_recv.at[recv], where)

    def force_arrived(which):
        target = (
            force_all.at[:, core, 1 - parity], force_all.at[:, core, parity, 1 - half], force_all.at[:, 1 - core]
        )[which]
        remote(target, target, force_send.at[which], force_recv.at[which], sibling).wait_recv()

    def spin_send_to(step):
        own = packed.at[rank, y]
        return remote(own, own, spin_send.at[0], spin_recv.at[rank], rank_device(lax.rem(rank + step, ranks)))

    def spin_arrived(source):
        target = packed.at[source, y]
        remote(target, target, spin_send.at[0], spin_recv.at[source], sibling).wait_recv()

    def hand_on(source, slot):
        for step in (1, 3, 2):
            piece = packed.at[source, y]
            remote(
                piece, piece, pass_send.at[slot], pass_recv.at[source, y], line_device(lax.rem(y + step, LINE))
            ).start()

    def handed(source, step):
        from_y = lax.rem(y + step, LINE)
        target = packed.at[source, from_y]
        remote(target, target, pass_send.at[0], pass_recv.at[source, from_y], sibling).wait_recv()
        return source, from_y

    masks = jnp.left_shift(1, lax.broadcasted_iota(jnp.int32, (32, quarter), 0))

    def places(tiles):
        return [pl.ds(pl.multiple_of(source * here + at * quarter, quarter), quarter) for source, at in tiles]

    def unpack(tiles):
        cols = places(tiles)
        for which, (source, at) in enumerate(tiles):
            to = slice(which * quarter, (which + 1) * quarter)
            for word in range(words):
                bits = jnp.bitwise_and(jnp.broadcast_to(packed[source, at, word : word + 1, :], (32, quarter)), masks)
                tile[word * 32 : word * 32 + 32, to] = jnp.where(bits != 0, 1.0, -1.0).astype(BF16)
        for to in range(SETS):
            word = (to % 2) * 2 * depth + 4 * rank + 2 * (to // 2 % 2) + to // 4
            from_rows = pl.ds(pl.multiple_of(word * rows, rows), rows)
            for which in range(2):
                spins[to * rows : (to + 1) * rows, cols[which]] = tile[
                    from_rows, which * quarter : (which + 1) * quarter
                ]

    def activate(tiles):
        cols = places(tiles)
        for unit in range(0, units, 1024):
            these = pl.ds(unit, 1024)
            pre = jnp.dot(weight_t[these, :], tile[...], preferred_element_type=F32)
            pre = pre + jnp.concatenate([bias_t[these, :]] * (2 * quarter // 128), axis=1)
            result = jnp.tanh(pre).astype(BF16)
            for which in range(2):
                hidden[these, cols[which]] = result[:, which * quarter : (which + 1) * quarter]

    def hidden_of(*tiles):
        unpack(tiles)
        activate(tiles)

    with jax.named_scope("barrier"):
        pl.semaphore_wait(barrier, len(greeted))
    force_copy(1).start()
    for step in (1, ranks - 1):
        spin_send_to(step).start()
    force_copy(0).start()

    spins[pair:, :] = (lax.broadcasted_iota(jnp.int32, (PAD, samples), 0) == 0).astype(F32).astype(BF16)
    with jax.named_scope("turn"):
        for copy in later:
            copy.wait()
        lax.fori_loop(0, units // 256, turn, 0)
    with jax.named_scope("hidden0"):
        hidden_of((rank, 0), (rank, 1))
        hidden_of((rank, 2), (rank, 3))
    with jax.named_scope("spinab"):
        spin_arrived(before)
        relayed = packed.at[before, y]
        remote(relayed, relayed, spin_send.at[0], spin_recv.at[before], rank_device(after)).start()
        hand_on(before, 0)
        spin_arrived(after)
        hand_on(after, 1)
    with jax.named_scope("hidden1"):
        hidden_of((before, y), (after, y))
    with jax.named_scope("wait"):
        tiles = handed(before, 3), handed(after, 3)
    with jax.named_scope("hidden2"):
        hidden_of(*tiles)
    with jax.named_scope("spinc"):
        spin_arrived(across)
        hand_on(across, 2)
        force_arrived(1)
        force_copy(2).start()
        force_copy(3).start()
        tiles = (across, y), handed(before, 1), handed(after, 1), handed(before, 2)
    with jax.named_scope("hidden3"):
        hidden_of(*tiles[:2])
        hidden_of(*tiles[2:])
    with jax.named_scope("wait"):
        force_arrived(0)
        force_copy(4).start()
        tiles = handed(after, 2), handed(across, 1), handed(across, 3), handed(across, 2)
    with jax.named_scope("hidden4"):
        hidden_of(*tiles[:2])
        hidden_of(*tiles[2:])

    span = samples // 2
    by_group, by_rank = (by_group_a, by_group_b), (by_rank_a, by_rank_b)

    def fill_lhs(at, slots, row):
        width = slots.shape[-1]
        cols = slice(at * width, (at + 1) * width)
        for to in range(SETS):
            lhs[to * rows : (to + 1) * rows, cols] = slots[at, to // 4, to // 2 % 2, to % 2].astype(BF16)
        lhs[pair:, cols] = jnp.concatenate(
            [row[:, cols] / ranks, jnp.zeros((PAD - 1, width), F32)], axis=0
        ).astype(BF16)

    def values_of(which, first, last, side, fresh):
        these, cols = slice(first * PART, last * PART), slice(side * span, (side + 1) * span)
        product = jnp.dot(lhs[:, these], hidden[these, cols], preferred_element_type=F32)
        value = jnp.sum(product[:pair] * spins[:pair, cols].astype(F32), axis=0, keepdims=True) + product[pair : pair + 1]
        mine = by_group[side].at[which, grp, :, :span]
        mine[...] = value if fresh else mine[...] + value

    with jax.named_scope("forcew"):
        force_arrived(2)
        for at in range(parts):
            fill_lhs(at, force_all, force_b_ref)
    other_groups = [group_device(lax.rem(grp + step, groups)) for step in range(1, groups)]
    other_ranks = [rank_device(lax.rem(rank + step, ranks)) for step in range(1, ranks)]
    other_sets = [
        device(half_at, z_at, core_at)
        for core_at in (core, 1 - core)
        for z_at in (z, z + 1 - 2 * parity)
        for half_at in (half, 1 - half)
    ][1:]

    def gather(slots, which, size, me, peers):
        send, recv = gather_send.at[which], gather_recv.at[which]
        for peer in peers:
            remote(slots.at[me], slots.at[me], send, recv, peer).start()
        others = slots.at[pl.ds(0, size - 1)]

        def finish():
            remote(others, others, send, recv, sibling).wait()

        return finish

    def gather_shards():
        send, recv = gather_send.at[12], gather_recv.at[12]
        for far in sorted(range(depth), key=lambda apart: -min(apart, depth - apart)):
            for half_at in (1 - half, half):
                for core_at in (1 - core, core):
                    if far or half_at is not half or core_at is not core:
                        where = device(half_at, lax.rem(z + far, depth), core_at)
                        remote(by_shard.at[smp], by_shard.at[smp], send, recv, where).start()
        others = by_shard.at[pl.ds(0, shards - 1)]

        def finish():
            remote(others, others, send, recv, sibling).wait()

        return finish

    def wide(x, lanes=128):
        return jnp.broadcast_to(x, (1, lanes))

    def send_groups(which, side):
        return gather(by_group[side].at[which], 2 * which + side, groups, grp, other_groups)

    def send_ranks(which, side):
        mine = by_group[side][which, 0]
        for source in range(1, groups):
            mine = mine + by_group[side][which, source]
        by_rank[side][which, rank] = mine
        return gather(by_rank[side].at[which], 4 + 2 * which + side, ranks, rank, other_ranks)

    def sum_ranks(which, side):
        whole = by_rank[side][which, 0]
        for source in range(1, ranks):
            whole = whole + by_rank[side][which, source]
        return whole

    def gather_sets(which, first, second):
        by_set[which, member] = jnp.concatenate([wide(first), wide(second), jnp.zeros((6, 128), F32)], axis=0)
        return gather(by_set.at[which], 8 + which, SETS, member, other_sets)

    def set_sum(which, row):
        value = by_set[which, 0, row : row + 1, :]
        for source in range(1, SETS):
            value = value + by_set[which, source, row : row + 1, :]
        return value[:, :1]

    def own_force(at):
        return force_all[at, core, parity, half]

    force_dot = total(force_b_ref[...] * force_b_ref[...]) / shards
    for at in range(parts):
        force_dot = force_dot + total(own_force(at) * own_force(at))
    def of_hidden(left, at):
        return lax.dot_general(
            left[...], hidden[cols_ds(at), :], (((1,), (1,)), ((), ())), preferred_element_type=F32
        )

    def extras(which, first, second):
        by_group[1][which, grp, :, span:] = jnp.concatenate([wide(first), wide(second)], axis=1)

    def own_sum(side):
        return total(by_group[side][0, grp, :, :span])

    with jax.named_scope("values0"):
        values_of(0, 0, parts, 0, True)
        finish_a = send_groups(0, 0)
        extras(0, force_dot, jnp.zeros((1, 1), F32))
        values_of(0, 0, parts, 1, True)
        finish_b = send_groups(0, 1)
    with jax.named_scope("redg"):
        by_shard[smp] = wide(own_sum(0) + own_sum(1))
        finish_shards = gather_shards()

        def plain_part(at, carry):
            plain[at] = of_hidden(spins, at)
            return carry

        lax.fori_loop(0, 2, plain_part, 0)
        finish_a()
        finish_ranks_a = send_ranks(0, 0)
        finish_b()
        finish_ranks_b = send_ranks(0, 1)
    with jax.named_scope("shards"):
        finish_shards()
        mine = by_shard[0]
        for source in range(1, shards):
            mine = mine + by_shard[source]
        by_total[grp] = mine
        finish_total = gather(by_total, 13, groups, grp, other_groups)
    with jax.named_scope("redr"):
        lax.fori_loop(2, parts, plain_part, 0)
        finish_ranks_a()
        finish_ranks_b()
        sums = [sum_ranks(0, side) for side in range(2)]
        own_dot = sums[1][:, span : span + 1]
        mean_own = (total(sums[0][:, :span]) + total(sums[1][:, :span])) / samples
        centred = [whole[:, :span] - mean_own for whole in sums]
    with jax.named_scope("scaled"):
        for at in range(0, samples, 512):
            weights = centred[at // span][:, at % span : at % span + 512]
            scaled[:pair, at : at + 512] = (spins[:pair, at : at + 512].astype(F32) * weights).astype(BF16)
            scaled[pair:, at : at + 512] = jnp.concatenate(
                [weights, jnp.zeros((PAD - 1, 512), F32)], axis=0
            ).astype(BF16)

    def outer(at):
        return (x_partner, z_partner, half) if at % 2 == 0 else (z_partner, x_partner, parity)

    def pick(ref, at, which):
        return ref.at[:, which] if at % 2 == 0 else ref.at[which]

    def core_copy(at):
        return remote(image.at[at, 1 - core], image_core.at[at], image_send.at[0], image_recv.at[at, 0], sibling)

    def image_copy(at, which):
        far, near, place = outer(at)
        ours = pick(image_all.at[at, core], at, place)
        theirs = pick(image_all.at[at, core], at, 1 - place)
        source, target, where = (
            None,
            (pick(image.at[at, core], at, 1 - place), image_z.at[at], far),
            (pick(image.at[at, core], at, place), image_x.at[at], near),
            (ours, ours, far),
            (ours, ours, sibling),
            (theirs, theirs, sibling),
        )[which]
        return remote(source, target, image_send.at[which], image_recv.at[at, min(which, 4)], where)

    def image_arrived(at, which):
        place = outer(at)[2]
        target = (
            image_core.at[at], image_z.at[at], image_x.at[at],
            pick(image_all.at[at, core], at, 1 - place),
            image_all.at[at, 1 - core],
        )[which]
        remote(target, target, image_send.at[which], image_recv.at[at, which], sibling).wait_recv()

    per = PART // PIECE

    def image_part(at, carry):
        part = of_hidden(scaled, at)
        for to in range(SETS):
            for which in range(per):
                image[per * at + which, to // 4, to // 2 % 2, to % 2] = part[
                    to * rows : (to + 1) * rows, which * PIECE : (which + 1) * PIECE
                ]
        image_b[member, :, cols_ds(at)] = part[pair : pair + 1]
        return carry

    def shifted(at):
        for which in range(per):
            for to in range(SETS):
                block = image.at[per * at + which, to // 4, to // 2 % 2, to % 2]
                block[...] = block[...] + shift * plain[
                    at, to * rows : (to + 1) * rows, which * PIECE : (which + 1) * PIECE
                ]
            core_copy(per * at + which).start()
        image_b[member, :, cols_ds(at)] = image_b[member, :, cols_ds(at)] + shift * plain[at, pair : pair + 1]

    def sum_core(at):
        place = outer(at)[2]
        image_arrived(at, 0)
        theirs = pick(image.at[at, core], at, 1 - place)
        theirs[...] = theirs[...] + pick(image_core.at[at], at, 1 - place)[...]
        image_copy(at, 1).start()
        ours = pick(image.at[at, core], at, place)
        ours[...] = ours[...] + pick(image_core.at[at], at, place)[...]

    def sum_outer(at):
        image_arrived(at, 1)
        ours = pick(image.at[at, core], at, outer(at)[2])
        ours[...] = ours[...] + image_z[at]
        image_copy(at, 2).start()

    def sum_inner(at):
        image_arrived(at, 2)
        place = outer(at)[2]
        pick(image_all.at[at, core], at, place)[...] = pick(image.at[at, core], at, place)[...] + image_x[at]
        image_copy(at, 3).start()
        image_copy(at, 4).start()

    def share(at):
        image_arrived(at, 3)
        image_copy(at, 5).start()

    def image_ready(at):
        image_arrived(at, 4)
        fill_lhs(at, image_all, image_b[0])

    def named(name, step, *at):
        with jax.named_scope(name):
            step(*at)

    with jax.named_scope("image"):
        lax.fori_loop(0, 2, image_part, 0)
    with jax.named_scope("mean"):
        finish_total()
        mean0 = by_total[0]
        for source in range(1, groups):
            mean0 = mean0 + by_total[source]
        shift = mean_own - mean0[:, :1] / count
        shifted(0)
        shifted(1)
        moment = total(centred[0] * centred[0]) + total(centred[1] * centred[1]) + samples * shift * shift
        finish_moment = gather_sets(0, moment, own_dot)

    def image_step(at, carry):
        image_part(at, 0)
        shifted(at)

        @pl.when(at == 2)
        def _():
            for piece in range(2 * per):
                sum_core(piece)

        return carry

    with jax.named_scope("image"):
        lax.fori_loop(2, parts, image_step, 0)
    finish_bias = gather(image_b, 11, SETS, member, other_sets)
    turns = [at ^ 1 for at in range(pieces)]
    for at in range(2 * per, pieces):
        named("core", sum_core, at)
    for at in turns:
        named("outer", sum_outer, at)
    with jax.named_scope("bias"):
        finish_moment()
        finish_bias()
        norm0 = set_sum(0, 1)
        step0 = norm0 / (set_sum(0, 0) / count + diag_shift * norm0)
        keep = 1.0 - diag_shift * step0
        pull = step0 / count
        whole_b = image_b[0]
        for source in range(1, SETS):
            whole_b = whole_b + image_b[source]
        image_b[0] = whole_b
    for at in range(pieces):
        named("inner", sum_inner, at)
    with jax.named_scope("norm"):
        residual_b = keep * force_b_ref[...] - pull * whole_b
        own_norm = total(residual_b * residual_b) / shards
        own_cross = total(residual_b * force_b_ref[...]) / shards
        image_b_ref[0:1, :] = whole_b
        image_b_ref[1:2, :] = force_b_ref[...]
        for at in range(parts):
            own_ref[:, cols_of(at)] = own_force(at)
        for at in range(pieces):
            image_ref[:, at * PIECE : (at + 1) * PIECE] = image_all[at, core, parity, half]
        residual = keep * own_ref[...] - pull * image_ref[...]
        own_norm = own_norm + total(residual * residual)
        own_cross = own_cross + total(residual * own_ref[...])
        finish_norm = gather_sets(1, own_norm, own_cross)
    near, last = turns[: pieces // 2], turns[pieces // 2 :]
    for at in near:
        named("share", share, at)
    for at in near[:2]:
        named("ready", image_ready, at)
    for at in last[:2]:
        named("share", share, at)
    for at in near[2:]:
        named("ready", image_ready, at)
    with jax.named_scope("values1"):
        values_of(1, 0, 2, 0, True)
    for at in last[2:]:
        named("share", share, at)
    with jax.named_scope("values1"):
        values_of(1, 0, 2, 1, True)
    for at in last:
        named("ready", image_ready, at)
    named("fnorm", finish_norm)
    extras(1, set_sum(1, 0), set_sum(1, 1))
    with jax.named_scope("values1"):
        values_of(1, 2, 4, 0, False)
        finish_a = send_groups(1, 0)
        values_of(1, 2, 4, 1, False)
        finish_b = send_groups(1, 1)
    with jax.named_scope("redg"):
        finish_a()
        finish_ranks_a = send_ranks(1, 0)
        finish_b()
        finish_ranks_b = send_ranks(1, 1)
    with jax.named_scope("redr"):
        finish_ranks_a()
        finish_ranks_b()
        sums = [sum_ranks(1, side) for side in range(2)]
        norm1, cross = sums[1][:, span : span + 1], sums[1][:, span + 128 : span + 129]
    beta = norm1 / norm0
    with jax.named_scope("sets"):
        values1 = [(keep + beta) * (centred[side] + shift) - pull * sums[side][:, :span] for side in range(2)]
        mean1 = (total(values1[0]) + total(values1[1])) / samples
        values1 = [value - mean1 for value in values1]
        gather_sets(2, mean1, total(values1[0] * values1[0]) + total(values1[1] * values1[1]))()
        middle = set_sum(2, 0) / SETS
        spread = jnp.zeros((1, 1), F32)
        for source in range(SETS):
            shift = by_set[2, source, 0:1, :1] - middle
            spread = spread + shift * shift
        variance1 = (set_sum(2, 1) + samples * spread) / count
    direction_dot = norm1 + 2.0 * beta * cross + beta * beta * norm0
    step1 = norm1 / (variance1 + diag_shift * direction_dot)

    for_force = step0 + step1 * (keep + beta)
    for_image = step1 * pull
    scale_ref[...] = jnp.concatenate([wide(for_force), wide(for_image), jnp.zeros((6, 128), F32)], axis=0)
    with jax.named_scope("out"):
        pieces = packed.at[rank, pl.ds(0, LINE - 1)]
        remote(pieces, pieces, spin_send.at[0], spin_recv.at[0], sibling).wait_send()
        for slot in range(3):
            remote(pieces, pieces, pass_send.at[slot], spin_recv.at[0], sibling).wait_send()
        for which in range(5):
            force_copy(which).wait_send()
        for which in range(6):
            blocks = image_core if which == 0 else image_z
            remote(blocks, blocks, image_send.at[which], spin_recv.at[0], sibling).wait_send()


def finish_kernel(image_ref, image_b_ref, force_ref, scale_ref, out_ref, out_b_ref):
    for_force, for_image = scale_ref[0:1, 0:1], scale_ref[1:2, 0:1]
    out_ref[...] = for_force * force_ref[...] - for_image * image_ref[...]
    out_b_ref[...] = for_force * image_b_ref[1:2, :] - for_image * image_b_ref[0:1, :]


def body(groups, shards, spins_packed, weight, hidden_bias, force_w, force_b):
    words, here = spins_packed.shape
    inputs, units = weight.shape
    rows = force_w.shape[0]
    ranks = shards // SETS
    samples, pair = ranks * here, SETS * rows
    parts, pieces = units // PART, units // PIECE
    quarter = here // LINE
    vmem = pl.BlockSpec(memory_space=pltpu.VMEM)
    anywhere = pl.BlockSpec(memory_space=pl.ANY)
    dma = pltpu.SemaphoreType.DMA
    results = pl.pallas_call(
        functools.partial(kernel, groups, shards),
        out_shape=(
            pltpu.VMEM((rows, units), F32), pltpu.VMEM((8, units), F32),
            pltpu.VMEM((rows, units), F32), pltpu.VMEM((8, 128), F32),
        ),
        in_specs=[anywhere] * 5,
        out_specs=(vmem,) * 4,
        scratch_shapes=[
            pltpu.VMEM((ranks, LINE, words, quarter), jnp.int32),
            pltpu.VMEM((inputs, units), BF16),
            pltpu.VMEM((units, inputs), BF16),
            pltpu.VMEM((1, units), F32),
            pltpu.VMEM((units, 128), F32),
            pltpu.VMEM((1, units), F32),
            pltpu.VMEM((inputs, 2 * quarter), BF16),
            pltpu.VMEM((pair + PAD, samples), BF16),
            pltpu.VMEM((units, samples), BF16),
            pltpu.VMEM((parts, 2, 2, 2, rows, PART), F32),
            pltpu.VMEM((pair + PAD, units), BF16),
            pltpu.VMEM((pair + PAD, samples), BF16),
            pltpu.VMEM((parts, pair + PAD, PART), F32),
            pltpu.VMEM((pieces, 2, 2, 2, rows, PIECE), F32),
            pltpu.VMEM((pieces, 2, 2, rows, PIECE), F32),
            pltpu.VMEM((pieces, 2, rows, PIECE), F32),
            pltpu.VMEM((pieces, 2, rows, PIECE), F32),
            pltpu.VMEM((pieces, 2, 2, 2, rows, PIECE), F32),
            pltpu.VMEM((SETS, 1, units), F32),
            pltpu.VMEM((2, groups, 1, samples // 2), F32),
            pltpu.VMEM((2, groups, 1, samples // 2 + EXTRA), F32),
            pltpu.VMEM((2, ranks, 1, samples // 2), F32),
            pltpu.VMEM((2, ranks, 1, samples // 2 + EXTRA), F32),
            pltpu.VMEM((3, SETS, 8, 128), F32),
            pltpu.VMEM((shards, 1, 128), F32),
            pltpu.VMEM((groups, 1, 128), F32),
            dma((5,)),
            dma((1,)),
            dma((ranks,)),
            dma((3,)),
            dma((ranks, LINE)),
            dma((5,)),
            dma((3,)),
            dma((6,)),
            dma((pieces, 5)),
            dma((14,)),
            dma((14,)),
        ],
        compiler_params=pltpu.CompilerParams(
            collective_id=0, has_side_effects=True, vmem_limit_bytes=62 * 1024 * 1024
        ),
    )(spins_packed, weight, hidden_bias.reshape(1, -1), force_w, force_b.reshape(1, -1))
    update_w, update_b = pl.pallas_call(
        finish_kernel,
        out_shape=(jax.ShapeDtypeStruct((rows, units), F32), jax.ShapeDtypeStruct((1, units), F32)),
        in_specs=[vmem] * 4,
        out_specs=(vmem, vmem),
    )(*[pltpu.with_memory_space_constraint(result, pltpu.VMEM) for result in results])
    return update_w, update_b.reshape(-1)


def solution(mesh):
    placed = (P(None, "smp"), P(None, "grp"), P("grp"), P("smp", "grp"), P("grp"))
    return jax.shard_map(
        functools.partial(body, mesh.shape["grp"], mesh.shape["smp"]),
        mesh=mesh, in_specs=placed, out_specs=(P("smp", "grp"), P("grp")), check_vma=False,
    )
```
